32 devices in a mesh: rows: 32 (over z, y, x, core).
Axes of the slice: x: 2, y: 2, z: 4, core: 2. Of those that a mesh axis runs over, the one named last changes fastest.
Arguments:
- left: bfloat16 [131072, 512], P('rows'), may hold values from -6 to 6
- right: bfloat16 [131072, 512], P('rows'), may hold values from -6 to 6
- tiles: bfloat16 [2, 64, 128, 128], replicated, may hold values from -0.1875 to 0.1875
- source_blocks: int32 [2, 1024, 16], P(None, 'rows'), may hold values from 0 to 95, as said below
- tile_index: int32 [2, 1024, 16], P(None, 'rows'), may hold values from -1 to 63
- send_blocks: int32 [1024, 2], P('rows'), may hold values from -1 to 31, as said below
Outputs:
- moments: float32 [2, 512, 512], P(None, 'rows')
The draws below stay inside these ranges and needn't reach their ends.
Inputs may be any that keep to these rules, and one draw needn't show every extreme that they name: `source_blocks`: every slot with v >= 32 names a slot of send_blocks that is not -1. Empty slots (tile -1) name an own block. Each provided block is named by some slot of the receiving device. Some device receives 2 blocks from every device, and some device has all of its slots filled. `send_blocks`: slot 0 is never -1; the two blocks that one device provides to another are different.
All inputs are finite; a program needn't handle non-finite values.
Results may differ from the reference program's by a relative error of at most 0.0029.
Values may be sent and summed in bfloat16 or wider, within the bound.
No kernel may reach another device: no remote copies, remote signals or barrier semaphores. Data moves between devices by JAX's collectives and lax.ppermute only.
A program may use at most 192 MiB of HBM per device.

```python
import math
import jax
import jax.numpy as jnp
from jax import lax

ROW_BLK = 128
VEC = 512
BLK_DEV = 32
KSLOT = 16
TILES = 64
CAP = 2
ROWS = 131072
N_ROWS = 32


def joint_plan(key):
    subkeys = [jax.random.fold_in(key, 1000 + number) for number in range(12)]
    hub_device = jax.random.randint(subkeys[0], (), 0, N_ROWS)
    counts = 1 + jax.random.randint(subkeys[1], (N_ROWS, N_ROWS), 0, 2)
    receiver = jnp.arange(N_ROWS)[None, :]
    counts = jnp.where(receiver == hub_device, 2, counts)
    first_block = jax.random.randint(subkeys[2], (N_ROWS, N_ROWS), 0, BLK_DEV)
    second = (first_block + 1 + jax.random.randint(subkeys[3], (N_ROWS, N_ROWS), 0, BLK_DEV - 1)) % BLK_DEV
    send_table = jnp.stack([first_block, jnp.where(counts == 2, second, -1)], axis=-1).reshape(N_ROWS * N_ROWS, CAP)
    total_slots = 2 * BLK_DEV * KSLOT

    def one_order(subkey):
        return jax.random.permutation(subkey, total_slots)
    orders = jax.vmap(one_order)(jax.random.split(subkeys[4], N_ROWS))
    inverse = jnp.argsort(orders, axis=1, stable=True)
    position = jnp.broadcast_to(jnp.arange(total_slots)[None, :], (N_ROWS, total_slots))
    pair_peer = jnp.minimum(position // CAP, N_ROWS - 1)
    pair_slot = position % CAP
    pair_open = pair_slot < jnp.take_along_axis(counts.T, pair_peer, axis=1)
    forced = (position < N_ROWS * CAP) & pair_open
    fill_level = 1 + jax.random.randint(subkeys[5], (N_ROWS,), 0, 8)
    busy_device = jax.random.randint(subkeys[6], (), 0, N_ROWS)
    fill_level = jnp.where(jnp.arange(N_ROWS) == busy_device, 8, fill_level)
    kept_slot = jax.random.randint(subkeys[7], (N_ROWS, total_slots), 0, 8) < fill_level[:, None]
    far_slot = jax.random.randint(subkeys[8], (N_ROWS, total_slots), 0, 2) == 1
    far_peer = jax.random.randint(subkeys[9], (N_ROWS, total_slots), 0, N_ROWS)
    near_block = jax.random.randint(subkeys[10], (N_ROWS, total_slots), 0, BLK_DEV)
    values = jnp.where(forced, BLK_DEV + position, jnp.where(far_slot & kept_slot, BLK_DEV + far_peer * CAP, near_block))
    active = forced | kept_slot
    chosen_tiles = jnp.where(active, jax.random.randint(subkeys[11], (N_ROWS, total_slots), 0, TILES), -1)
    values = jnp.take_along_axis(values, inverse, axis=1)
    chosen_tiles = jnp.take_along_axis(chosen_tiles, inverse, axis=1)
    values = values.reshape(N_ROWS, 2, BLK_DEV, KSLOT).transpose(1, 0, 2, 3).reshape(2, N_ROWS * BLK_DEV, KSLOT)
    chosen_tiles = chosen_tiles.reshape(N_ROWS, 2, BLK_DEV, KSLOT).transpose(1, 0, 2, 3).reshape(2, N_ROWS * BLK_DEV, KSLOT)
    return (values.astype(jnp.int32), chosen_tiles.astype(jnp.int32), send_table.astype(jnp.int32))


def draw_source_blocks(key, part):
    return joint_plan(key)[0]


def draw_tile_index(key, part):
    return joint_plan(key)[1]


def draw_send_blocks(key, part):
    return joint_plan(key)[2]


def raised(result, own_key, source, target, shards_of, factor):
    owner, partner = [(jnp.arange(result.shape[dim]) // (result.shape[dim] // shards_of)).reshape([-1 if axis == dim else 1 for axis in range(result.ndim)]) for dim in (source, target)]
    chosen = jax.random.permutation(own_key, shards_of)[partner]
    strong = (owner == chosen) | (owner == (partner + shards_of // 2) % shards_of)
    return jnp.where(strong, factor * result, result)


def block_scale(own_key, extent, cuts, smallest, largest):
    loudness, own = 1.0, jax.random.fold_in(own_key, 6)
    for dim, blocks in cuts:
        draws = jnp.exp(jax.random.uniform(jax.random.fold_in(own, dim), (blocks,), jnp.float32, smallest / len(cuts), largest / len(cuts)))
        loudness = loudness * jnp.repeat(draws, extent[dim] // blocks).reshape([-1 if axis == dim else 1 for axis in range(len(extent))])
    return loudness


def normal_values(own_key, extent, deviation, most, cuts=(), kind=jnp.bfloat16):
    level = block_scale(own_key, extent, cuts, -0.22, 0.18) if cuts else 1.0
    drawn = jax.random.normal(own_key, extent, jnp.float32) * deviation * level
    return jnp.minimum(jnp.maximum(drawn, -most), most).astype(kind)


def noise_with(own_key, extent, spread, limit, cuts, heavy, held_as=jnp.bfloat16):
    entries = spread * jax.random.normal(own_key, extent, jnp.float32)
    if cuts:
        entries = entries * block_scale(own_key, extent, cuts, -0.22, 0.18)
    return jnp.clip(raised(entries, jax.random.fold_in(own_key, 3), *heavy), -limit, limit).astype(held_as)


def setup_inputs(seed: int = 0) -> dict:
    streams_of = jax.random.split(jax.random.key(seed), 7)
    left = noise_with(streams_of[0], (ROWS, VEC), 1.0, 6.0, ((0, 32),), (0, 1, 32, 2.75))
    right = normal_values(streams_of[1], (ROWS, VEC), 1.0, 6.0, ((0, 32),))
    tiles = normal_values(streams_of[2], (2, TILES, ROW_BLK, ROW_BLK), (ROW_BLK * KSLOT // 2) ** -0.5, 0.1875)
    source_blocks = draw_source_blocks(jax.random.fold_in(streams_of[6], 71), 0)
    tile_index = draw_tile_index(jax.random.fold_in(streams_of[6], 71), 0)
    send_blocks = draw_send_blocks(jax.random.fold_in(streams_of[6], 71), 0)
    return {"left": left, "right": right, "tiles": tiles, "source_blocks": source_blocks, "tile_index": tile_index, "send_blocks": send_blocks}


def resolve(values, send_blocks):
    owner_device = (jnp.arange(values.shape[0], dtype=jnp.int32) // BLK_DEV)[:, None]
    remote = values >= BLK_DEV
    offset = jnp.maximum(values - BLK_DEV, 0)
    peer_device = offset // CAP
    peer_slot = offset % CAP
    provided = send_blocks[peer_device * N_ROWS + owner_device, peer_slot]
    return jnp.where(remote, peer_device * BLK_DEV + provided, owner_device * BLK_DEV + values).astype(jnp.int32)

def reference(left, right, tiles, source_blocks, tile_index, send_blocks):
    total_blocks = BLK_DEV * N_ROWS
    blocks = right.reshape(total_blocks, ROW_BLK, VEC)
    norm_scale = 1.0 / math.sqrt(total_blocks * ROW_BLK)
    group_size = 8
    results = []
    for direction in range(2):
        global_source = resolve(source_blocks[direction], send_blocks)
        tile_table = tiles[direction]

        def one_group(operands):
            group_sources, group_tiles = operands
            live = (group_tiles >= 0)[..., None, None]
            chosen = jnp.where(live, tile_table[jnp.maximum(group_tiles, 0)], jnp.zeros((), jnp.bfloat16))
            picked = blocks[group_sources]
            summed = jnp.einsum('bkij,bkjn->bin', chosen.astype(jnp.float32), picked.astype(jnp.float32))
            return summed.astype(jnp.bfloat16)
        current = lax.map(one_group, (global_source.reshape(-1, group_size, KSLOT), tile_index[direction].reshape(-1, group_size, KSLOT)))
        current = current.reshape(total_blocks * ROW_BLK, VEC)
        gram = lax.dot_general(left, current, (((0,), (0,)), ((), ())), preferred_element_type=jnp.float32)
        results.append(gram * norm_scale)
    return jnp.stack(results)
```

```python
import functools
import math

import jax
import jax.numpy as jnp
import numpy as np
from jax import lax
from jax.experimental import pallas as pl
from jax.experimental.pallas import tpu as pltpu
from jax.sharding import PartitionSpec as P


F32 = jnp.float32
BF16 = jnp.bfloat16
SHIFT = 1024
SMEM = pltpu.SMEM
VMEM = pltpu.VMEM
ANY = pl.ANY


def exchange_order(devices):
    half = devices // 2
    order = []
    for step in range(half):
        order.append(half + step)
        if step + 1 < half:
            order.append(1 + step)
    return order


def exchange_groups(count):
    first, second = (count + 1) // 2, count - max(1, count // 6)
    return [(0, first), (first, second), (second, count)]


def whole(shape, space=VMEM):
    return pl.BlockSpec(shape, lambda *_: (0,) * len(shape), memory_space=space)


def pack_kernel(masks, rank_ref, send_ref, blocks_ref, *rest):
    outs, sems = rest[: len(masks)], rest[len(masks)]
    cap = send_ref.shape[1]
    rank = rank_ref[0]
    copies = []
    for n, mask in enumerate(masks):
        for c in range(cap):
            block = jnp.maximum(send_ref[rank ^ mask, c], 0)
            copy = pltpu.make_async_copy(blocks_ref.at[block], outs[n].at[c], sems.at[n * cap + c])
            copy.start()
            copies.append(copy)
    for copy in copies:
        copy.wait()


def pack(rank, send, blocks, masks):
    cap = send.shape[1]
    return pl.pallas_call(
        functools.partial(pack_kernel, masks),
        out_shape=[jax.ShapeDtypeStruct((cap,) + blocks.shape[1:], BF16)] * len(masks),
        in_specs=[whole((1,), SMEM), whole(send.shape, SMEM), whole(blocks.shape)],
        out_specs=[pl.BlockSpec(memory_space=ANY)] * len(masks),
        scratch_shapes=[pltpu.SemaphoreType.DMA((len(masks) * cap,))],
        name="pack",
    )(rank, send, blocks)


def add_pairs(acc_ref, count, entry, tiles_ref, pool_ref, zero_ref):
    def pair(j, carry):
        e0 = entry(2 * j)
        e1 = entry(jnp.minimum(2 * j + 1, count - 1))
        odd = 2 * j + 1 >= count
        t0 = tiles_ref[e0 // SHIFT]
        t1 = tiles_ref[jnp.where(odd, tiles_ref.shape[0] - 1, e1 // SHIFT)]
        r0 = pool_ref[e0 % SHIFT]
        r1 = pool_ref[e1 % SHIFT]
        acc_ref[...] += jnp.dot(
            jnp.concatenate([t0, t1], axis=1),
            jnp.concatenate([r0, r1], axis=0),
            preferred_element_type=F32,
        )
        return carry

    lax.fori_loop(0, (count + 1) // 2, pair, 0)


def local_kernel(
    phases, rank_ref, where_ref, send_ref, source_ref, tile_ref, blocks_ref, tiles_ref,
    out_ref, lists_ref, counts_ref, mine_ref,
):
    step = pl.program_id(0)
    slots = source_ref.shape[1]
    local = blocks_ref.shape[0]
    cap = send_ref.shape[1]
    rank = rank_ref[0]

    def place(k, counts):
        v = source_ref[step, k]
        t = tile_ref[step, k]
        r = jnp.maximum(v - local, 0)
        spot = where_ref[(r // cap) ^ rank]
        own = jnp.where(v < local, v, jnp.maximum(send_ref[rank, r % cap], 0))
        phase = jnp.where(v < local, 0, spot // SHIFT)
        phase = jnp.where(t < 0, phases, phase)
        block = jnp.where(phase == 0, own, (spot % SHIFT) * cap + r % cap)
        value = jnp.maximum(t, 0) * SHIFT + block
        new = []
        for ph in range(phases):
            hit = phase == ph

            @pl.when(hit)
            def _(ph=ph):
                if ph == 0:
                    mine_ref[counts[ph]] = value
                else:
                    lists_ref[ph - 1, step * slots + counts[ph]] = value

            new.append(counts[ph] + hit.astype(jnp.int32))
        return tuple(new)

    counts = lax.fori_loop(0, slots, place, (jnp.int32(0),) * phases)
    for ph in range(1, phases):
        counts_ref[ph - 1, step] = counts[ph]
    out_ref[...] = jnp.zeros_like(out_ref)
    add_pairs(out_ref.at[0], counts[0], lambda j: mine_ref[j], tiles_ref.at[0], blocks_ref, None)


def local_hops(rank, where, send, source, tile, blocks, tiles, phases):
    steps, slots = source.shape
    per = steps // 2
    rows, vectors = blocks.shape[1:]
    shape = tiles.shape
    return pl.pallas_call(
        functools.partial(local_kernel, phases),
        grid=(steps,),
        out_shape=[
            jax.ShapeDtypeStruct((steps, rows, vectors), F32),
            jax.ShapeDtypeStruct((phases - 1, steps * slots), jnp.int32),
            jax.ShapeDtypeStruct((phases - 1, steps), jnp.int32),
        ],
        in_specs=[
            whole((1,), SMEM), whole(where.shape, SMEM), whole(send.shape, SMEM),
            whole(source.shape, SMEM), whole(tile.shape, SMEM), whole(blocks.shape),
            pl.BlockSpec((1,) + shape[1:], lambda i: (i // per, 0, 0, 0)),
        ],
        out_specs=[
            pl.BlockSpec((1, rows, vectors), lambda i: (i, 0, 0)),
            whole((phases - 1, steps * slots), SMEM),
            whole((phases - 1, steps), SMEM),
        ],
        scratch_shapes=[SMEM((slots,), jnp.int32)],
        compiler_params=pltpu.CompilerParams(dimension_semantics=("arbitrary",)),
        cost_estimate=pl.CostEstimate(flops=20 * 10**9, bytes_accessed=24 * 2**20, transcendentals=0),
        name="local_hops",
    )(rank, where, send, source, tile, blocks, tiles)


def load_pool(arrivals, pool_ref, sems):
    copies = []
    for n, ref in enumerate(arrivals):
        cap = ref.shape[0]
        copy = pltpu.make_async_copy(ref, pool_ref.at[pl.ds(n * cap, cap)], sems.at[n])
        copy.start()
        copies.append(copy)
    for copy in copies:
        copy.wait()


def arrival_kernel(phase, count, slots, lists_ref, counts_ref, tiles_ref, in_ref, *rest):
    arrivals, (out_ref, pool_ref, sems) = rest[:count], rest[count:]
    step = pl.program_id(0)

    @pl.when(step == 0)
    def _():
        load_pool(arrivals, pool_ref, sems)

    out_ref[...] = in_ref[...]
    add_pairs(
        out_ref.at[0], counts_ref[phase - 1, step],
        lambda j: lists_ref[phase - 1, step * slots + j], tiles_ref.at[0], pool_ref, None,
    )


def arrival_hops(phase, lists, counts, tiles, current, arrivals):
    steps, rows, vectors = current.shape
    per = steps // 2
    slots = lists.shape[1] // steps
    cap = arrivals[0].shape[0]
    shape = tiles.shape
    block = pl.BlockSpec((1, rows, vectors), lambda i: (i, 0, 0))
    return pl.pallas_call(
        functools.partial(arrival_kernel, phase, len(arrivals), slots),
        grid=(steps,),
        out_shape=jax.ShapeDtypeStruct(current.shape, F32),
        in_specs=[
            whole(lists.shape, SMEM), whole(counts.shape, SMEM),
            pl.BlockSpec((1,) + shape[1:], lambda i: (i // per, 0, 0, 0)), block,
        ] + [pl.BlockSpec(memory_space=ANY)] * len(arrivals),
        out_specs=block,
        scratch_shapes=[
            VMEM((len(arrivals) * cap, rows, vectors), BF16),
            pltpu.SemaphoreType.DMA((len(arrivals),)),
        ],
        input_output_aliases={3: 0},
        compiler_params=pltpu.CompilerParams(dimension_semantics=("arbitrary",)),
        cost_estimate=pl.CostEstimate(flops=8 * 10**9, bytes_accessed=40 * 2**20, transcendentals=0),
        name=f"arrival_hops_{phase}",
    )(lists, counts, tiles, current, *arrivals)


def gram_kernel(
    phase, count, slots, per, bunch, rank_ref, lists_ref, counts_ref, tiles_ref, in_ref, left_ref,
    *rest,
):
    arrivals, rest = rest[:count], rest[count:]
    outs, (pool_ref, acc_ref, current_ref, sum_ref, sems) = rest[:-5], rest[-5:]
    step = pl.program_id(0)
    rows, vectors = acc_ref.shape

    @pl.when(step == 0)
    def _():
        load_pool(arrivals, pool_ref, sems)
        sum_ref[...] = jnp.zeros_like(sum_ref)

    for d in range(2):
        for g in range(bunch):
            block = d * per + step * bunch + g
            acc_ref[...] = in_ref[d, g]
            add_pairs(
                acc_ref, counts_ref[phase - 1, block],
                lambda j, block=block: lists_ref[phase - 1, block * slots + j],
                tiles_ref.at[d], pool_ref, None,
            )
            current_ref[pl.ds(g * rows, rows), pl.ds(d * vectors, vectors)] = acc_ref[...].astype(BF16)
    sum_ref[...] += jnp.dot(left_ref[...], current_ref[...], preferred_element_type=F32)

    @pl.when(step == pl.num_programs(0) - 1)
    def _():
        if len(outs) == 1:
            outs[0][...] = sum_ref[...]
            return
        send_ref, keep_ref = outs
        core = rank_ref[0] % 2
        pairs, own = send_ref.shape[0], send_ref.shape[1]
        for n in range(pairs):
            keep_ref[n] = sum_ref[pl.ds(pl.multiple_of((2 * n + core) * own, own), own), :]
            send_ref[n] = sum_ref[pl.ds(pl.multiple_of((2 * n + 1 - core) * own, own), own), :].astype(send_ref.dtype)


def gram(phase, rank, lists, counts, tiles, current, left_t, arrivals, devices, sent):
    steps, rows, vectors = current.shape
    per = steps // 2
    slots = lists.shape[1] // steps
    bunch = math.gcd(per, 4)
    cap = arrivals[0].shape[0]
    own = left_t.shape[0] // devices
    current = current.reshape(2, per, rows, vectors)
    if own % 8:
        halves = [jax.ShapeDtypeStruct((left_t.shape[0], 2 * vectors), F32)]
    else:
        half = (devices // 2, own, 2 * vectors)
        halves = [jax.ShapeDtypeStruct(half, sent), jax.ShapeDtypeStruct(half, F32)]
    return pl.pallas_call(
        functools.partial(gram_kernel, phase, len(arrivals), slots, per, bunch),
        grid=(per // bunch,),
        out_shape=halves,
        in_specs=[
            whole((1,), SMEM), whole(lists.shape, SMEM), whole(counts.shape, SMEM), whole(tiles.shape),
            pl.BlockSpec((2, bunch, rows, vectors), lambda i: (0, i, 0, 0)),
            pl.BlockSpec((left_t.shape[0], bunch * rows), lambda i: (0, i)),
        ] + [pl.BlockSpec(memory_space=ANY)] * len(arrivals),
        out_specs=[whole(part.shape) for part in halves],
        scratch_shapes=[
            VMEM((len(arrivals) * cap, rows, vectors), BF16),
            VMEM((rows, vectors), F32),
            VMEM((bunch * rows, 2 * vectors), BF16),
            VMEM((left_t.shape[0], 2 * vectors), F32),
            pltpu.SemaphoreType.DMA((len(arrivals),)),
        ],
        compiler_params=pltpu.CompilerParams(dimension_semantics=("arbitrary",)),
        cost_estimate=pl.CostEstimate(flops=6 * 10**9, bytes_accessed=24 * 2**20, transcendentals=0),
        name="gram",
    )(rank, lists, counts, tiles, current, left_t, *arrivals)


def split_kernel(width, shift, count, final, scale, rank_ref, keep_ref, *rest):
    arrived, outs = rest[:count], rest[count:]
    mine = (rank_ref[0] >> shift) % width
    if final:
        vectors = outs[0].shape[-1]
        total = keep_ref[...]
        for ref in arrived:
            total = total + ref[...].astype(F32)
        total = total * scale
        for d in range(2):
            outs[0][d] = total[:, d * vectors:(d + 1) * vectors]
        return
    for mask in range(width):
        where = mine ^ mask
        if len(keep_ref.shape) == 4:
            part = keep_ref[:, where]
            for ref in arrived:
                part = part + ref[:, where].astype(F32)
        else:
            part = keep_ref[where]
            for ref in arrived:
                part = part + ref[where].astype(F32)
        outs[mask][...] = part.astype(outs[mask].dtype)


def split(rank, keep, arrived, width, shift, sent):
    part = keep.shape[:-3] + keep.shape[-2:]
    return pl.pallas_call(
        functools.partial(split_kernel, width, shift, len(arrived), False, None),
        out_shape=[jax.ShapeDtypeStruct(part, sent if n else F32) for n in range(width)],
        in_specs=[whole((1,), SMEM), whole(keep.shape)] + [whole(a.shape) for a in arrived],
        out_specs=[whole(part)] * width,
        name=f"split_{shift}",
    )(rank, keep, *arrived)


def finish(rank, keep, arrived, scale):
    own, both = keep.shape
    return pl.pallas_call(
        functools.partial(split_kernel, 1, 0, len(arrived), True, scale),
        out_shape=jax.ShapeDtypeStruct((2, own, both // 2), F32),
        in_specs=[whole((1,), SMEM), whole(keep.shape)] + [whole(a.shape) for a in arrived],
        out_specs=whole((2, own, both // 2)),
        name="finish",
    )(rank, keep, *arrived)


def swap(value, mask, devices):
    return lax.ppermute(value, "rows", [(i, i ^ mask) for i in range(devices)])


def body(left, right, tiles, source_blocks, tile_index, send_blocks):
    block_rows = tiles.shape[-1]
    vectors = right.shape[1]
    local = right.shape[0] // block_rows
    devices = lax.axis_size("rows")
    slots = source_blocks.shape[-1]
    scale = 1.0 / math.sqrt(local * block_rows * devices)
    rank = lax.axis_index("rows").astype(jnp.int32).reshape(1)
    blocks = right.reshape(local, block_rows, vectors)
    order = exchange_order(devices)
    groups = exchange_groups(len(order))
    where = np.zeros((devices,), np.int32)
    for phase, (start, stop) in enumerate(groups):
        for n in range(start, stop):
            where[order[n]] = (phase + 1) * SHIFT + n - start

    packed = pack(rank, send_blocks, blocks, order)
    arrived = [swap(value, mask, devices) for value, mask in zip(packed, order)]

    tiles = jnp.concatenate([tiles, jnp.zeros((2, 1) + tiles.shape[2:], tiles.dtype)], axis=1)
    source = source_blocks.reshape(2 * local, slots)
    tile = tile_index.reshape(2 * local, slots)
    current, lists, counts = local_hops(
        rank, jnp.asarray(where), send_blocks, source, tile, blocks, tiles, len(groups) + 1
    )
    left_t = left.T
    for phase, (start, stop) in enumerate(groups[:-1]):
        current = arrival_hops(phase + 1, lists, counts, tiles, current, arrived[start:stop])
    start, stop = groups[-1]
    sums = gram(
        len(groups), rank, lists, counts, tiles, current, left_t, arrived[start:stop], devices, F32
    )
    if len(sums) == 1:
        mine = lax.psum_scatter(sums[0] * scale, "rows", scatter_dimension=0, tiled=True)
        return mine.reshape(mine.shape[0], 2, vectors).transpose(1, 0, 2)
    send, keep = sums
    own = keep.shape[1]
    outer = devices // 8
    got = swap(send, 1, devices)
    parts = split(rank, keep.reshape(outer, 4, own, 2 * vectors),
                  [got.reshape(outer, 4, own, 2 * vectors)], 4, 1, BF16)
    got = [swap(parts[n], n << 1, devices) for n in range(1, 4)]
    parts = split(rank, parts[0], got, outer, 3, F32)
    got = [swap(parts[n], n << 3, devices) for n in range(1, outer)]
    return finish(rank, parts[0], got, scale)


def solution(mesh):
    placed = (
        P("rows", None),
        P("rows", None),
        P(),
        P(None, "rows", None),
        P(None, "rows", None),
        P("rows", None),
    )
    return jax.shard_map(
        body, mesh=mesh, in_specs=placed, out_specs=P(None, "rows", None), check_vma=False
    )
```

```python
import functools
import math

import jax
import jax.numpy as jnp
from jax import lax
from jax.experimental import pallas as pl
from jax.experimental.pallas import tpu as pltpu
from jax.sharding import PartitionSpec as P


F32 = jnp.float32
BF16 = jnp.bfloat16
SHIFT = 1024
SMEM = pltpu.SMEM
VMEM = pltpu.VMEM
ANY = pl.ANY


def exchange_order(devices):
    half = devices // 2
    order = []
    for step in range(half):
        order.append(half + step)
        if step + 1 < half:
            order.append(1 + step)
    return order


def exchange_groups(count):
    first, second = (count + 1) // 2, count - max(1, count // 6)
    return [(0, first), (first, second), (second, count)]


def whole(shape, space=VMEM):
    return pl.BlockSpec(shape, lambda *_: (0,) * len(shape), memory_space=space)


def pack_kernel(masks, after, rank_ref, send_ref, blocks_ref, *rest):
    rest = rest[after:]
    outs, (held_ref, in_sems, out_sems) = rest[: len(masks)], rest[len(masks):]
    cap = send_ref.shape[0]
    rank = rank_ref[0]
    inward, outward = [], []
    for n, mask in enumerate(masks):
        for c in range(cap):
            i = n * cap + c
            block = jnp.maximum(send_ref[c, rank ^ mask], 0)
            copy = pltpu.make_async_copy(blocks_ref.at[block], held_ref.at[i], in_sems.at[i])
            copy.start()
            inward.append(copy)
            outward.append(pltpu.make_async_copy(held_ref.at[i], outs[n].at[c], out_sems.at[i]))
    for one, two in zip(inward, outward):
        one.wait()
        two.start()
    for copy in outward:
        copy.wait()


def pack(rank, send, blocks, masks, after=()):
    cap = send.shape[0]
    count = len(masks) * cap
    return pl.pallas_call(
        functools.partial(pack_kernel, masks, len(after)),
        out_shape=[jax.ShapeDtypeStruct((cap,) + blocks.shape[1:], BF16)] * len(masks),
        in_specs=[whole((1,), SMEM), whole(send.shape, SMEM)]
        + [pl.BlockSpec(memory_space=ANY)] * (1 + len(after)),
        out_specs=[pl.BlockSpec(memory_space=ANY)] * len(masks),
        scratch_shapes=[
            VMEM((count,) + blocks.shape[1:], BF16),
            pltpu.SemaphoreType.DMA((count,)),
            pltpu.SemaphoreType.DMA((count,)),
        ],
        name="pack",
    )(rank, send, blocks, *after)


def slot_lists(rank, send, source, tile, local, devices, starts, spare):
    cap = send.shape[0]
    slots = source.shape[1]
    half = devices // 2
    mine = lax.dynamic_index_in_dim(send, rank[0], 1, keepdims=False)
    away = source >= local
    r = jnp.maximum(source - local, 0)
    c = r % cap
    mask = (r // cap) ^ rank[0]
    spot = jnp.where(mask >= half, 2 * (mask - half), 2 * mask - 1)
    own = source
    for n in range(cap):
        own = jnp.where(away & (c == n), jnp.maximum(mine[n], 0), own)
    phase = jnp.zeros_like(source)
    first = jnp.zeros_like(source)
    far = away & (mask != 0)
    for n, start in enumerate(starts):
        phase = jnp.where(far & (spot >= start), n + 1, phase)
        first = jnp.where(far & (spot >= start), start, first)
    value = tile * SHIFT + jnp.where(far, (spot - first) * cap + c, own)
    phases = jnp.arange(len(starts) + 1, dtype=jnp.int32)[:, None, None]
    hit = (tile >= 0)[None] & (phase[None] == phases)
    k = jnp.arange(slots, dtype=jnp.int32)
    before = (hit[:, :, None, :] & (k[None, :] < k[:, None])).astype(jnp.int32).sum(-1)
    there = hit[:, :, None, :] & (before[:, :, None, :] == k[:, None])
    empty = spare * SHIFT
    lists = jnp.where(there, value[None, :, None, :] - empty, 0).sum(-1) + empty
    return lists.reshape(len(starts) + 1, -1), hit.astype(jnp.int32).sum(-1)


def pair(entry, j, tiles_ref, pool_ref):
    e0, e1 = entry(2 * j), entry(2 * j + 1)
    return jnp.dot(
        jnp.concatenate([tiles_ref[e0 // SHIFT], tiles_ref[e1 // SHIFT]], axis=1),
        jnp.concatenate([pool_ref[e0 % SHIFT], pool_ref[e1 % SHIFT]], axis=0),
        preferred_element_type=F32,
    )


def add_rest(acc_ref, done, count, entry, tiles_ref, pool_ref):
    def one(j, carry):
        acc_ref[...] += pair(entry, j, tiles_ref, pool_ref)
        return carry

    lax.fori_loop(done, (count + 1) // 2, one, 0)


def load_pool(arrivals, pool_ref, sems):
    copies = []
    for n, ref in enumerate(arrivals):
        cap = ref.shape[0]
        copy = pltpu.make_async_copy(ref, pool_ref.at[pl.ds(n * cap, cap)], sems.at[n])
        copy.start()
        copies.append(copy)
    for copy in copies:
        copy.wait()


def hops_kernel(phase, slots, fixed, count, lists_ref, counts_ref, tiles_ref, *rest):
    if phase == 0:
        pool_ref, out_ref = rest
        in_ref = None
    else:
        in_ref, arrivals, (out_ref, pool_ref, sems) = rest[0], rest[1:1 + count], rest[1 + count:]
    step = pl.program_id(0)
    bunch = out_ref.shape[0]
    tiles_ref = tiles_ref.at[0]

    if phase:
        @pl.when(step == 0)
        def _():
            load_pool(arrivals, pool_ref, sems)

    def entry_of(g):
        return lambda j: lists_ref[phase, (step * bunch + g) * slots + j]

    for g in range(bunch):
        for j in range(fixed):
            value = pair(entry_of(g), j, tiles_ref, pool_ref)
            if j:
                out_ref[g] += value
            elif phase:
                out_ref[g] = in_ref[g] + value
            else:
                out_ref[g] = value
    for g in range(bunch):
        add_rest(
            out_ref.at[g], fixed, counts_ref[phase, step * bunch + g], entry_of(g), tiles_ref, pool_ref
        )


def hops(phase, lists, counts, tiles, pool, current, fixed, bunch=4):
    steps = counts.shape[1]
    slots = lists.shape[1] // steps
    bunch = math.gcd(bunch, steps // 2)
    per = steps // 2 // bunch
    shape = tiles.shape
    rows, vectors = (pool if phase == 0 else pool[0]).shape[1:]
    block = pl.BlockSpec((bunch, rows, vectors), lambda i: (i, 0, 0))
    in_specs = [
        whole(lists.shape, SMEM), whole(counts.shape, SMEM),
        pl.BlockSpec((1,) + shape[1:], lambda i: (i // per, 0, 0, 0)),
    ]
    if phase == 0:
        operands, scratch, aliases, count = [pool], [], {}, 0
        in_specs += [whole(pool.shape)]
    else:
        count = len(pool)
        operands, aliases = [current, *pool], {3: 0}
        in_specs += [block] + [pl.BlockSpec(memory_space=ANY)] * count
        scratch = [
            VMEM((count * pool[0].shape[0], rows, vectors), BF16), pltpu.SemaphoreType.DMA((count,)),
        ]
    return pl.pallas_call(
        functools.partial(hops_kernel, phase, slots, fixed, count),
        grid=(steps // bunch,),
        out_shape=jax.ShapeDtypeStruct((steps, rows, vectors), F32),
        in_specs=in_specs,
        out_specs=block,
        scratch_shapes=scratch,
        input_output_aliases=aliases,
        compiler_params=pltpu.CompilerParams(dimension_semantics=("arbitrary",)),
        cost_estimate=pl.CostEstimate(flops=8 * 10**9, bytes_accessed=40 * 2**20, transcendentals=0),
        name=f"hops_{phase}",
    )(lists, counts, tiles, *operands)


def gram_kernel(
    phase, count, slots, fixed, per, bunch, rank_ref, lists_ref, counts_ref, tiles_ref, in_ref,
    left_ref, *rest,
):
    arrivals, rest = rest[:count], rest[count:]
    outs, (pool_ref, acc_ref, current_ref, sum_ref, sems) = rest[:-5], rest[-5:]
    step = pl.program_id(0)
    rows, vectors = acc_ref.shape[2:]

    @pl.when(step == 0)
    def _():
        load_pool(arrivals, pool_ref, sems)
        sum_ref[...] = jnp.zeros_like(sum_ref)

    def entry_of(d, g):
        return lambda j: lists_ref[phase, (d * per + step * bunch + g) * slots + j]

    for d in range(2):
        for g in range(bunch):
            for j in range(fixed):
                value = pair(entry_of(d, g), j, tiles_ref.at[d], pool_ref)
                if j:
                    acc_ref[d, g] += value
                else:
                    acc_ref[d, g] = in_ref[d, g] + value
    for d in range(2):
        for g in range(bunch):
            add_rest(
                acc_ref.at[d, g], fixed, counts_ref[phase, d * per + step * bunch + g],
                entry_of(d, g), tiles_ref.at[d], pool_ref,
            )
    for d in range(2):
        for g in range(bunch):
            current_ref[pl.ds(g * rows, rows), pl.ds(d * vectors, vectors)] = acc_ref[d, g].astype(BF16)
    sum_ref[...] += jnp.dot(left_ref[...], current_ref[...], preferred_element_type=F32)

    @pl.when(step == pl.num_programs(0) - 1)
    def _():
        if len(outs) == 1:
            outs[0][...] = sum_ref[...]
            return
        send_ref, keep_ref = outs
        core = rank_ref[0] % 2
        pairs, own = send_ref.shape[0], send_ref.shape[1]
        for n in range(pairs):
            keep_ref[n] = sum_ref[pl.ds(pl.multiple_of((2 * n + core) * own, own), own), :]
            send_ref[n] = sum_ref[pl.ds(pl.multiple_of((2 * n + 1 - core) * own, own), own), :].astype(send_ref.dtype)


def gram(phase, rank, lists, counts, tiles, current, left_t, arrivals, devices, sent, fixed):
    steps, rows, vectors = current.shape
    per = steps // 2
    slots = lists.shape[1] // steps
    bunch = math.gcd(per, 4)
    cap = arrivals[0].shape[0]
    own = left_t.shape[0] // devices
    current = current.reshape(2, per, rows, vectors)
    if own % 8:
        halves = [jax.ShapeDtypeStruct((left_t.shape[0], 2 * vectors), F32)]
    else:
        half = (devices // 2, own, 2 * vectors)
        halves = [jax.ShapeDtypeStruct(half, sent), jax.ShapeDtypeStruct(half, F32)]
    return pl.pallas_call(
        functools.partial(gram_kernel, phase, len(arrivals), slots, fixed, per, bunch),
        grid=(per // bunch,),
        out_shape=halves,
        in_specs=[
            whole((1,), SMEM), whole(lists.shape, SMEM), whole(counts.shape, SMEM), whole(tiles.shape),
            pl.BlockSpec((2, bunch, rows, vectors), lambda i: (0, i, 0, 0)),
            pl.BlockSpec((left_t.shape[0], bunch * rows), lambda i: (0, i)),
        ] + [pl.BlockSpec(memory_space=ANY)] * len(arrivals),
        out_specs=[whole(part.shape) for part in halves],
        scratch_shapes=[
            VMEM((len(arrivals) * cap, rows, vectors), BF16),
            VMEM((2, bunch, rows, vectors), F32),
            VMEM((bunch * rows, 2 * vectors), BF16),
            VMEM((left_t.shape[0], 2 * vectors), F32),
            pltpu.SemaphoreType.DMA((len(arrivals),)),
        ],
        compiler_params=pltpu.CompilerParams(dimension_semantics=("arbitrary",)),
        cost_estimate=pl.CostEstimate(flops=6 * 10**9, bytes_accessed=24 * 2**20, transcendentals=0),
        name="gram",
    )(rank, lists, counts, tiles, current, left_t, *arrivals)


def split_kernel(width, shift, count, final, scale, rank_ref, keep_ref, *rest):
    arrived, outs = rest[:count], rest[count:]
    mine = (rank_ref[0] >> shift) % width
    if final:
        vectors = outs[0].shape[-1]
        total = keep_ref[...]
        for ref in arrived:
            total = total + ref[...].astype(F32)
        total = total * scale
        for d in range(2):
            outs[0][d] = total[:, d * vectors:(d + 1) * vectors]
        return
    for mask in range(width):
        where = mine ^ mask
        if len(keep_ref.shape) == 4:
            part = keep_ref[:, where]
            for ref in arrived:
                part = part + ref[:, where].astype(F32)
        else:
            part = keep_ref[where]
            for ref in arrived:
                part = part + ref[where].astype(F32)
        outs[mask][...] = part.astype(outs[mask].dtype)


def split(rank, keep, arrived, width, shift, sent):
    part = keep.shape[:-3] + keep.shape[-2:]
    return pl.pallas_call(
        functools.partial(split_kernel, width, shift, len(arrived), False, None),
        out_shape=[jax.ShapeDtypeStruct(part, sent if n else F32) for n in range(width)],
        in_specs=[whole((1,), SMEM), whole(keep.shape)] + [whole(a.shape) for a in arrived],
        out_specs=[whole(part)] * width,
        name=f"split_{shift}",
    )(rank, keep, *arrived)


def finish(rank, keep, arrived, scale):
    own, both = keep.shape
    return pl.pallas_call(
        functools.partial(split_kernel, 1, 0, len(arrived), True, scale),
        out_shape=jax.ShapeDtypeStruct((2, own, both // 2), F32),
        in_specs=[whole((1,), SMEM), whole(keep.shape)] + [whole(a.shape) for a in arrived],
        out_specs=whole((2, own, both // 2)),
        name="finish",
    )(rank, keep, *arrived)


def swap(value, mask, devices):
    return lax.ppermute(value, "rows", [(i, i ^ mask) for i in range(devices)])


def body(left, right, tiles, source_blocks, tile_index, send_blocks):
    block_rows = tiles.shape[-1]
    vectors = right.shape[1]
    local = right.shape[0] // block_rows
    devices = lax.axis_size("rows")
    slots = source_blocks.shape[-1]
    scale = 1.0 / math.sqrt(local * block_rows * devices)
    rank = lax.axis_index("rows").astype(jnp.int32).reshape(1)
    blocks = right.reshape(local, block_rows, vectors)
    order = exchange_order(devices)
    groups = exchange_groups(len(order))
    send = send_blocks.T

    early = min(4, len(order))
    packed = pack(rank, send, blocks, order[:early])
    packed += pack(rank, send, blocks, order[early:], packed[:1])
    arrived = [swap(value, mask, devices) for value, mask in zip(packed, order)]

    lists, counts = slot_lists(
        rank, send, source_blocks.reshape(2 * local, slots), tile_index.reshape(2 * local, slots),
        local, devices, [start for start, _ in groups], tiles.shape[1],
    )
    tiles = jnp.concatenate([tiles, jnp.zeros((2, 1) + tiles.shape[2:], tiles.dtype)], axis=1)
    left_t = left.T
    current = hops(0, lists, counts, tiles, blocks, None, 4)
    for n, (start, stop) in enumerate(groups[:-1]):
        current = hops(n + 1, lists, counts, tiles, arrived[start:stop], current, 2)
    start, stop = groups[-1]
    sums = gram(
        len(groups), rank, lists, counts, tiles, current, left_t, arrived[start:stop], devices, F32, 1
    )
    if len(sums) == 1:
        mine = lax.psum_scatter(sums[0] * scale, "rows", scatter_dimension=0, tiled=True)
        return mine.reshape(mine.shape[0], 2, vectors).transpose(1, 0, 2)
    send, keep = sums
    own = keep.shape[1]
    outer = devices // 8
    got = swap(send, 1, devices)
    parts = split(rank, keep.reshape(outer, 4, own, 2 * vectors),
                  [got.reshape(outer, 4, own, 2 * vectors)], 4, 1, BF16)
    got = [swap(parts[n], n << 1, devices) for n in range(1, 4)]
    parts = split(rank, parts[0], got, outer, 3, F32)
    got = [swap(parts[n], n << 3, devices) for n in range(1, outer)]
    return finish(rank, parts[0], got, scale)


def solution(mesh):
    placed = (
        P("rows", None),
        P("rows", None),
        P(),
        P(None, "rows", None),
        P(None, "rows", None),
        P("rows", None),
    )
    return jax.shard_map(
        body, mesh=mesh, in_specs=placed, out_specs=P(None, "rows", None), check_vma=False
    )
```

```python
import functools
import math

import jax
import jax.numpy as jnp
from jax import lax
from jax.experimental import pallas as pl
from jax.experimental.pallas import tpu as pltpu
from jax.sharding import PartitionSpec as P


F32 = jnp.float32
BF16 = jnp.bfloat16
SHIFT = 1024
ROOM = 8 * 2**20
SMEM = pltpu.SMEM
VMEM = pltpu.VMEM
HBM = pltpu.HBM


def exchange_order(devices):
    half = devices // 2
    order = []
    for step in range(half):
        order.append(half + step)
        if step + 1 < half:
            order.append(1 + step)
    return order


def exchange_groups(count):
    first, second = (count + 1) // 2, count - max(1, count // 6)
    return [(0, first), (first, second), (second, count)]


def in_hbm(value):
    return pltpu.with_memory_space_constraint(value, HBM)


def in_vmem(value):
    return pltpu.with_memory_space_constraint(value, VMEM)


def whole(shape, space=VMEM):
    return pl.BlockSpec(shape, lambda *_: (0,) * len(shape), memory_space=space)


def pack_kernel(masks, after, rank_ref, send_ref, blocks_ref, *rest):
    rest = rest[after:]
    outs, (held_ref, in_sems, out_sems) = rest[: len(masks)], rest[len(masks):]
    cap = send_ref.shape[0]
    rank = rank_ref[0]
    inward, outward = [], []
    for n, mask in enumerate(masks):
        for c in range(cap):
            i = n * cap + c
            block = jnp.maximum(send_ref[c, rank ^ mask], 0)
            copy = pltpu.make_async_copy(blocks_ref.at[block], held_ref.at[i], in_sems.at[i])
            copy.start()
            inward.append(copy)
            outward.append(pltpu.make_async_copy(held_ref.at[i], outs[n].at[c], out_sems.at[i]))
    for one, two in zip(inward, outward):
        one.wait()
        two.start()
    for copy in outward:
        copy.wait()


def pack(rank, send, blocks, masks, after=()):
    cap = send.shape[0]
    count = len(masks) * cap
    return pl.pallas_call(
        functools.partial(pack_kernel, masks, len(after)),
        out_shape=[jax.ShapeDtypeStruct((cap,) + blocks.shape[1:], BF16)] * len(masks),
        in_specs=[whole((1,), SMEM), whole(send.shape, SMEM)]
        + [pl.BlockSpec(memory_space=HBM)] * (1 + len(after)),
        out_specs=[pl.BlockSpec(memory_space=HBM)] * len(masks),
        scratch_shapes=[
            VMEM((count,) + blocks.shape[1:], BF16),
            pltpu.SemaphoreType.DMA((count,)),
            pltpu.SemaphoreType.DMA((count,)),
        ],
        name="pack",
    )(rank, send, blocks, *after)


def slot_lists(rank, send, source, tile, local, devices, starts, spare):
    cap = send.shape[0]
    slots = source.shape[1]
    half = devices // 2
    mine = lax.dynamic_index_in_dim(send, rank[0], 1, keepdims=False)
    away = source >= local
    r = jnp.maximum(source - local, 0)
    c = r % cap
    mask = (r // cap) ^ rank[0]
    spot = jnp.where(mask >= half, 2 * (mask - half), 2 * mask - 1)
    own = source
    for n in range(cap):
        own = jnp.where(away & (c == n), jnp.maximum(mine[n], 0), own)
    phase = jnp.zeros_like(source)
    first = jnp.zeros_like(source)
    far = away & (mask != 0)
    for n, start in enumerate(starts):
        phase = jnp.where(far & (spot >= start), n + 1, phase)
        first = jnp.where(far & (spot >= start), start, first)
    value = tile * SHIFT + jnp.where(far, (spot - first) * cap + c, own)
    phases = jnp.arange(len(starts) + 1, dtype=jnp.int32)[:, None, None]
    hit = (tile >= 0)[None] & (phase[None] == phases)
    k = jnp.arange(slots, dtype=jnp.int32)
    before = (hit[:, :, None, :] & (k[None, :] < k[:, None])).astype(jnp.int32).sum(-1)
    there = hit[:, :, None, :] & (before[:, :, None, :] == k[:, None])
    empty = spare * SHIFT
    lists = jnp.where(there, value[None, :, None, :] - empty, 0).sum(-1) + empty
    return lists.reshape(len(starts) + 1, -1), hit.astype(jnp.int32).sum(-1)


def pair(entry, j, tiles_ref, pool_ref):
    e0, e1 = entry(2 * j), entry(2 * j + 1)
    return jnp.dot(
        jnp.concatenate([tiles_ref[e0 // SHIFT], tiles_ref[e1 // SHIFT]], axis=1),
        jnp.concatenate([pool_ref[e0 % SHIFT], pool_ref[e1 % SHIFT]], axis=0),
        preferred_element_type=F32,
    )


def add_rest(acc_ref, done, count, entry, tiles_ref, pool_ref):
    def one(j, carry):
        acc_ref[...] += pair(entry, j, tiles_ref, pool_ref)
        return carry

    lax.fori_loop(done, (count + 1) // 2, one, 0)


def pool_loads(arrivals, pool_ref, sems):
    cap = arrivals[0].shape[0]
    return [
        pltpu.make_async_copy(ref, pool_ref.at[pl.ds(n * cap, cap)], sems.at[n])
        for n, ref in enumerate(arrivals)
    ]


def in_chunks(from_ref, to_ref, sems):
    size = from_ref.shape[0] // sems.shape[0]
    return lambda i: pltpu.make_async_copy(
        from_ref.at[pl.ds(i * size, size)], to_ref.at[pl.ds(i * size, size)], sems.at[i]
    )


def hops_kernel(phase, slots, fixed, count, lists_ref, counts_ref, tiles_ref, *rest):
    if phase == 0:
        pool_ref, out_ref, held_ref, out_sems = rest
    else:
        in_ref, arrivals = rest[0], rest[1:1 + count]
        out_ref, held_ref, out_sems, pool_ref, in_sems, sems = rest[1 + count:]
    chunks = out_sems.shape[0]
    steps = held_ref.shape[0]
    bunch = steps // chunks
    outward = in_chunks(held_ref, out_ref, out_sems)
    if phase:
        inward = in_chunks(in_ref, held_ref, in_sems)
        loads = pool_loads(arrivals, pool_ref, sems)
        for copy in loads:
            copy.start()
        for i in range(chunks):
            inward(i).start()
        for copy in loads:
            copy.wait()

    def some(step, carry):
        tiles = tiles_ref.at[2 * step // chunks]
        if phase:
            inward(step).wait()
        for g in range(bunch):
            block = step * bunch + g
            entry = lambda j, block=block: lists_ref[phase, block * slots + j]
            for j in range(fixed):
                value = pair(entry, j, tiles, pool_ref)
                if j or phase:
                    held_ref[block] += value
                else:
                    held_ref[block] = value
        for g in range(bunch):
            block = step * bunch + g
            entry = lambda j, block=block: lists_ref[phase, block * slots + j]
            add_rest(held_ref.at[block], fixed, counts_ref[phase, block], entry, tiles, pool_ref)
        outward(step).start()
        return carry

    lax.fori_loop(0, chunks, some, 0)
    for i in range(chunks):
        outward(i).wait()


def hops(phase, lists, counts, tiles, pool, current, fixed, bunch=4):
    steps = counts.shape[1]
    slots = lists.shape[1] // steps
    chunks = steps // math.gcd(bunch, steps // 2)
    rows, vectors = (pool if phase == 0 else pool[0]).shape[1:]
    dma = pltpu.SemaphoreType.DMA
    in_specs = [pl.BlockSpec(memory_space=SMEM)] * 2 + [pl.BlockSpec(memory_space=VMEM)]
    scratch = [VMEM((steps, rows, vectors), F32), dma((chunks,))]
    if phase == 0:
        operands, aliases, count, held = [pool], {}, 0, [pool]
        in_specs += [pl.BlockSpec(memory_space=VMEM)]
    else:
        count, held = len(pool), pool
        operands, aliases = [in_hbm(current), *map(in_hbm, pool)], {3: 0}
        in_specs += [pl.BlockSpec(memory_space=HBM)] * (1 + count)
        scratch += [VMEM((count * pool[0].shape[0], rows, vectors), BF16), dma((chunks,)), dma((count,))]
    room = ROOM + 4 * steps * rows * vectors + sum(2 * a.size for a in held)
    return pl.pallas_call(
        functools.partial(hops_kernel, phase, slots, fixed, count),
        out_shape=HBM((steps, rows, vectors), F32),
        in_specs=in_specs,
        out_specs=pl.BlockSpec(memory_space=HBM),
        scratch_shapes=scratch,
        input_output_aliases=aliases,
        compiler_params=pltpu.CompilerParams(vmem_limit_bytes=room),
        cost_estimate=pl.CostEstimate(flops=8 * 10**9, bytes_accessed=40 * 2**20, transcendentals=0),
        name=f"hops_{phase}",
    )(lists, counts, tiles, *operands)


def gram_kernel(
    phase, count, slots, fixed, rank_ref, lists_ref, counts_ref, tiles_ref, in_ref, left_ref, *rest
):
    arrivals, rest = rest[:count], rest[count:]
    outs, (pool_ref, held_ref, current_ref, sum_ref, in_sems, sems) = rest[:-6], rest[-6:]
    steps, rows, vectors = held_ref.shape
    per = steps // 2
    chunks = in_sems.shape[0] // 2
    bunch = per // chunks
    inward = in_chunks(in_ref, held_ref, in_sems)
    loads = pool_loads(arrivals, pool_ref, sems)
    for copy in loads:
        copy.start()
    for i in range(chunks):
        for d in range(2):
            inward(d * chunks + i).start()
    for copy in loads:
        copy.wait()

    def some(step, carry):
        spots = [(d, g, d * per + step * bunch + g) for d in range(2) for g in range(bunch)]
        for d in range(2):
            inward(d * chunks + step).wait()
        for d, g, block in spots:
            entry = lambda j, block=block: lists_ref[phase, block * slots + j]
            for j in range(fixed):
                held_ref[block] += pair(entry, j, tiles_ref.at[d], pool_ref)
        for d, g, block in spots:
            entry = lambda j, block=block: lists_ref[phase, block * slots + j]
            add_rest(
                held_ref.at[block], fixed, counts_ref[phase, block], entry, tiles_ref.at[d], pool_ref
            )
        for d, g, block in spots:
            current_ref[pl.ds(g * rows, rows), pl.ds(d * vectors, vectors)] = held_ref[block].astype(BF16)
        part = jnp.dot(left_ref[step], current_ref[...], preferred_element_type=F32)

        @pl.when(step == 0)
        def _():
            sum_ref[...] = part

        @pl.when(step > 0)
        def _():
            sum_ref[...] += part

        return carry

    lax.fori_loop(0, chunks, some, 0)
    if len(outs) == 1:
        outs[0][...] = sum_ref[...]
        return
    send_ref, keep_ref = outs
    core = rank_ref[0] % 2
    pairs, own = send_ref.shape[0], send_ref.shape[1]
    for n in range(pairs):
        keep_ref[n] = sum_ref[pl.ds(pl.multiple_of((2 * n + core) * own, own), own), :]
        send_ref[n] = sum_ref[pl.ds(pl.multiple_of((2 * n + 1 - core) * own, own), own), :].astype(send_ref.dtype)


def gram(phase, rank, lists, counts, tiles, current, left_t, arrivals, devices, sent, fixed):
    steps, rows, vectors = current.shape
    slots = lists.shape[1] // steps
    chunks = left_t.shape[0]
    cap = arrivals[0].shape[0]
    columns = left_t.shape[1]
    own = columns // devices
    block = pl.BlockSpec(memory_space=VMEM)
    dma = pltpu.SemaphoreType.DMA
    if own % 8:
        halves = [jax.ShapeDtypeStruct((columns, 2 * vectors), F32)]
    else:
        half = (devices // 2, own, 2 * vectors)
        halves = [jax.ShapeDtypeStruct(half, sent), jax.ShapeDtypeStruct(half, F32)]
    room = 2 * ROOM + 4 * current.size + sum(2 * a.size for a in arrivals)
    return pl.pallas_call(
        functools.partial(gram_kernel, phase, len(arrivals), slots, fixed),
        out_shape=halves,
        in_specs=[pl.BlockSpec(memory_space=SMEM)] * 3
        + [block, pl.BlockSpec(memory_space=HBM), block]
        + [pl.BlockSpec(memory_space=HBM)] * len(arrivals),
        out_specs=[block] * len(halves),
        scratch_shapes=[
            VMEM((len(arrivals) * cap, rows, vectors), BF16),
            VMEM((steps, rows, vectors), F32),
            VMEM((left_t.shape[2], 2 * vectors), BF16),
            VMEM((columns, 2 * vectors), F32),
            dma((2 * chunks,)),
            dma((len(arrivals),)),
        ],
        compiler_params=pltpu.CompilerParams(vmem_limit_bytes=room),
        cost_estimate=pl.CostEstimate(flops=6 * 10**9, bytes_accessed=24 * 2**20, transcendentals=0),
        name="gram",
    )(rank, lists, counts, tiles, in_hbm(current), in_vmem(left_t), *map(in_hbm, arrivals))


def split_kernel(width, shift, count, final, scale, rank_ref, keep_ref, *rest):
    arrived, outs = rest[:count], rest[count:]
    mine = (rank_ref[0] >> shift) % width
    if final:
        vectors = outs[0].shape[-1]
        total = keep_ref[...]
        for ref in arrived:
            total = total + ref[...].astype(F32)
        total = total * scale
        for d in range(2):
            outs[0][d] = total[:, d * vectors:(d + 1) * vectors]
        return
    for mask in range(width):
        where = mine ^ mask
        if len(keep_ref.shape) == 4:
            part = keep_ref[:, where]
            for ref in arrived:
                part = part + ref[:, where].astype(F32)
        else:
            part = keep_ref[where]
            for ref in arrived:
                part = part + ref[where].astype(F32)
        outs[mask][...] = part.astype(outs[mask].dtype)


def split(rank, keep, arrived, width, shift, sent):
    part = keep.shape[:-3] + keep.shape[-2:]
    return pl.pallas_call(
        functools.partial(split_kernel, width, shift, len(arrived), False, None),
        out_shape=[jax.ShapeDtypeStruct(part, sent if n else F32) for n in range(width)],
        in_specs=[pl.BlockSpec(memory_space=SMEM)] + [pl.BlockSpec(memory_space=VMEM)] * (1 + len(arrived)),
        out_specs=[pl.BlockSpec(memory_space=VMEM)] * width,
        name=f"split_{shift}",
    )(rank, *map(in_vmem, (keep, *arrived)))


def finish(rank, keep, arrived, scale):
    own, both = keep.shape
    return pl.pallas_call(
        functools.partial(split_kernel, 1, 0, len(arrived), True, scale),
        out_shape=jax.ShapeDtypeStruct((2, own, both // 2), F32),
        in_specs=[pl.BlockSpec(memory_space=SMEM)] + [pl.BlockSpec(memory_space=VMEM)] * (1 + len(arrived)),
        out_specs=pl.BlockSpec(memory_space=VMEM),
        name="finish",
    )(rank, *map(in_vmem, (keep, *arrived)))


def swap(value, mask, devices):
    return lax.ppermute(value, "rows", [(i, i ^ mask) for i in range(devices)])


def body(left, right, tiles, source_blocks, tile_index, send_blocks):
    block_rows = tiles.shape[-1]
    vectors = right.shape[1]
    local = right.shape[0] // block_rows
    devices = lax.axis_size("rows")
    slots = source_blocks.shape[-1]
    scale = 1.0 / math.sqrt(local * block_rows * devices)
    rank = lax.axis_index("rows").astype(jnp.int32).reshape(1)
    blocks = right.reshape(local, block_rows, vectors)
    order = exchange_order(devices)
    groups = exchange_groups(len(order))
    send = send_blocks.T

    early = min(4, len(order))
    packed = pack(rank, send, blocks, order[:early])
    packed += pack(rank, send, blocks, order[early:], packed[:1])
    arrived = [swap(value, mask, devices) for value, mask in zip(packed, order)]

    lists, counts = slot_lists(
        rank, send, source_blocks.reshape(2 * local, slots), tile_index.reshape(2 * local, slots),
        local, devices, [start for start, _ in groups], tiles.shape[1],
    )
    tiles = jnp.concatenate([tiles, jnp.zeros((2, 1) + tiles.shape[2:], tiles.dtype)], axis=1)
    bunch = math.gcd(local, 4) * block_rows
    left_t = left.reshape(-1, bunch, vectors).transpose(0, 2, 1)
    tiles = in_vmem(tiles)
    current = hops(0, lists, counts, tiles, blocks, None, 4)
    for n, (start, stop) in enumerate(groups[:-1]):
        current = hops(n + 1, lists, counts, tiles, arrived[start:stop], current, 2)
    start, stop = groups[-1]
    sums = gram(
        len(groups), rank, lists, counts, tiles, current, left_t, arrived[start:stop], devices, F32, 1
    )
    if len(sums) == 1:
        mine = lax.psum_scatter(sums[0] * scale, "rows", scatter_dimension=0, tiled=True)
        return mine.reshape(mine.shape[0], 2, vectors).transpose(1, 0, 2)
    send, keep = sums
    own = keep.shape[1]
    outer = devices // 8
    got = swap(send, 1, devices)
    parts = split(rank, keep.reshape(outer, 4, own, 2 * vectors),
                  [got.reshape(outer, 4, own, 2 * vectors)], 4, 1, BF16)
    got = [swap(parts[n], n << 1, devices) for n in range(1, 4)]
    parts = split(rank, parts[0], got, outer, 3, F32)
    got = [swap(parts[n], n << 3, devices) for n in range(1, outer)]
    return finish(rank, parts[0], got, scale)


def solution(mesh):
    placed = (
        P("rows", None),
        P("rows", None),
        P(),
        P(None, "rows", None),
        P(None, "rows", None),
        P("rows", None),
    )
    return jax.shard_map(
        body, mesh=mesh, in_specs=placed, out_specs=P(None, "rows", None), check_vma=False
    )
```

```python
import functools
import math

import jax
import jax.numpy as jnp
from jax import lax
from jax.experimental import pallas as pl
from jax.experimental.pallas import tpu as pltpu
from jax.sharding import PartitionSpec as P


F32 = jnp.float32
BF16 = jnp.bfloat16
SHIFT = 1024
ROOM = 8 * 2**20
EARLY = 3
AHEAD = 6
SMEM = pltpu.SMEM
VMEM = pltpu.VMEM
HBM = pltpu.HBM


def exchange_order(devices):
    half = devices // 2
    far, near = list(range(half, devices)), list(range(1, half))
    order, far = far[:EARLY], far[EARLY:]
    while far or near:
        order += near[:1] + far[:1]
        near, far = near[1:], far[1:]
    return order


def exchange_groups(count):
    first, second = (count + 1) // 2, count - max(1, count // 5)
    return [(0, first), (first, second), (second, count)]


def in_hbm(value):
    return pltpu.with_memory_space_constraint(value, HBM)


def in_vmem(value):
    return pltpu.with_memory_space_constraint(value, VMEM)


def whole(shape, space=VMEM):
    return pl.BlockSpec(shape, lambda *_: (0,) * len(shape), memory_space=space)


def pack_kernel(masks, after, rank_ref, send_ref, blocks_ref, *rest):
    rest = rest[after:]
    outs, (held_ref, in_sems, out_sems) = rest[: len(masks)], rest[len(masks):]
    cap = send_ref.shape[0]
    rank = rank_ref[0]
    inward, outward = [], []
    for n, mask in enumerate(masks):
        for c in range(cap):
            i = n * cap + c
            block = jnp.maximum(send_ref[c, rank ^ mask], 0)
            copy = pltpu.make_async_copy(blocks_ref.at[block], held_ref.at[i], in_sems.at[i])
            copy.start()
            inward.append(copy)
            outward.append(pltpu.make_async_copy(held_ref.at[i], outs[n].at[c], out_sems.at[i]))
    for one, two in zip(inward, outward):
        one.wait()
        two.start()
    for copy in outward:
        copy.wait()


def pack(rank, send, blocks, masks, after=()):
    cap = send.shape[0]
    count = len(masks) * cap
    return pl.pallas_call(
        functools.partial(pack_kernel, masks, len(after)),
        out_shape=[jax.ShapeDtypeStruct((cap,) + blocks.shape[1:], BF16)] * len(masks),
        in_specs=[whole((1,), SMEM), whole(send.shape, SMEM)]
        + [pl.BlockSpec(memory_space=HBM)] * (1 + len(after)),
        out_specs=[pl.BlockSpec(memory_space=HBM)] * len(masks),
        scratch_shapes=[
            VMEM((count,) + blocks.shape[1:], BF16),
            pltpu.SemaphoreType.DMA((count,)),
            pltpu.SemaphoreType.DMA((count,)),
        ],
        name="pack",
    )(rank, send, blocks, *after)


def slot_lists(rank, send, source, tile, local, order, starts, spare):
    cap = send.shape[0]
    slots = source.shape[1]
    mine = lax.dynamic_index_in_dim(send, rank[0], 1, keepdims=False)
    away = source >= local
    r = jnp.maximum(source - local, 0)
    c = r % cap
    mask = (r // cap) ^ rank[0]
    spot = jnp.where(
        mask[..., None] == jnp.array(order, jnp.int32), jnp.arange(len(order), dtype=jnp.int32), 0
    ).sum(-1)
    own = source
    for n in range(cap):
        own = jnp.where(away & (c == n), jnp.maximum(mine[n], 0), own)
    phase = jnp.zeros_like(source)
    first = jnp.zeros_like(source)
    far = away & (mask != 0)
    for n, start in enumerate(starts):
        phase = jnp.where(far & (spot >= start), n + 1, phase)
        first = jnp.where(far & (spot >= start), start, first)
    value = tile * SHIFT + jnp.where(far, (spot - first) * cap + c, own)
    phases = jnp.arange(len(starts) + 1, dtype=jnp.int32)[:, None, None]
    hit = (tile >= 0)[None] & (phase[None] == phases)
    k = jnp.arange(slots, dtype=jnp.int32)
    before = (hit[:, :, None, :] & (k[None, :] < k[:, None])).astype(jnp.int32).sum(-1)
    there = hit[:, :, None, :] & (before[:, :, None, :] == k[:, None])
    empty = spare * SHIFT
    lists = jnp.where(there, value[None, :, None, :] - empty, 0).sum(-1) + empty
    return lists.reshape(len(starts) + 1, -1), hit.astype(jnp.int32).sum(-1)


def pair(entry, j, tiles_ref, pool_ref):
    e0, e1 = entry(2 * j), entry(2 * j + 1)
    return jnp.dot(
        jnp.concatenate([tiles_ref[e0 // SHIFT], tiles_ref[e1 // SHIFT]], axis=1),
        jnp.concatenate([pool_ref[e0 % SHIFT], pool_ref[e1 % SHIFT]], axis=0),
        preferred_element_type=F32,
    )


def add_rest(acc_ref, done, count, entry, tiles_ref, pool_ref):
    def one(j, carry):
        acc_ref[...] += pair(entry, j, tiles_ref, pool_ref)
        return carry

    lax.fori_loop(done, (count + 1) // 2, one, 0)


def pool_loads(arrivals, pool_ref, sems):
    cap = arrivals[0].shape[0]
    return [
        pltpu.make_async_copy(ref, pool_ref.at[pl.ds(n * cap, cap)], sems.at[n])
        for n, ref in enumerate(arrivals)
    ]


def in_chunks(from_ref, to_ref, sems):
    size = from_ref.shape[0] // sems.shape[0]
    return lambda i: pltpu.make_async_copy(
        from_ref.at[pl.ds(i * size, size)], to_ref.at[pl.ds(i * size, size)], sems.at[i]
    )


def hops_kernel(phase, slots, fixed, count, lists_ref, counts_ref, tiles_ref, *rest):
    if phase == 0:
        pool_ref, out_ref, held_ref, out_sems = rest
    else:
        in_ref, arrivals = rest[0], rest[1:1 + count]
        out_ref, held_ref, out_sems, pool_ref, in_sems, sems = rest[1 + count:]
    chunks = out_sems.shape[0]
    steps = held_ref.shape[0]
    bunch = steps // chunks
    outward = in_chunks(held_ref, out_ref, out_sems)
    if phase:
        inward = in_chunks(in_ref, held_ref, in_sems)
        loads = pool_loads(arrivals, pool_ref, sems)
        for copy in loads:
            copy.start()
        ahead = min(AHEAD, chunks)
        for i in range(ahead):
            inward(i).start()
        for copy in loads:
            copy.wait()

    def some(step, carry):
        tiles = tiles_ref.at[2 * step // chunks]
        if phase:
            @pl.when(step + ahead < chunks)
            def _():
                inward(step + ahead).start()

            inward(step).wait()
        for g in range(bunch):
            block = step * bunch + g
            entry = lambda j, block=block: lists_ref[phase, block * slots + j]
            for j in range(fixed):
                value = pair(entry, j, tiles, pool_ref)
                if j or phase:
                    held_ref[block] += value
                else:
                    held_ref[block] = value
        for g in range(bunch):
            block = step * bunch + g
            entry = lambda j, block=block: lists_ref[phase, block * slots + j]
            add_rest(held_ref.at[block], fixed, counts_ref[phase, block], entry, tiles, pool_ref)
        outward(step).start()
        return carry

    lax.fori_loop(0, chunks, some, 0)
    for i in range(chunks):
        outward(i).wait()


def hops(phase, lists, counts, tiles, pool, current, fixed, bunch=4):
    steps = counts.shape[1]
    slots = lists.shape[1] // steps
    chunks = steps // math.gcd(bunch, steps // 2)
    rows, vectors = (pool if phase == 0 else pool[0]).shape[1:]
    dma = pltpu.SemaphoreType.DMA
    in_specs = [pl.BlockSpec(memory_space=SMEM)] * 2 + [pl.BlockSpec(memory_space=VMEM)]
    scratch = [VMEM((steps, rows, vectors), F32), dma((chunks,))]
    if phase == 0:
        operands, aliases, count, held = [pool], {}, 0, [pool]
        in_specs += [pl.BlockSpec(memory_space=VMEM)]
    else:
        count, held = len(pool), pool
        operands, aliases = [in_hbm(current), *map(in_hbm, pool)], {3: 0}
        in_specs += [pl.BlockSpec(memory_space=HBM)] * (1 + count)
        scratch += [VMEM((count * pool[0].shape[0], rows, vectors), BF16), dma((chunks,)), dma((count,))]
    room = ROOM + 4 * steps * rows * vectors + sum(2 * a.size for a in held)
    return pl.pallas_call(
        functools.partial(hops_kernel, phase, slots, fixed, count),
        out_shape=HBM((steps, rows, vectors), F32),
        in_specs=in_specs,
        out_specs=pl.BlockSpec(memory_space=HBM),
        scratch_shapes=scratch,
        input_output_aliases=aliases,
        compiler_params=pltpu.CompilerParams(vmem_limit_bytes=room),
        cost_estimate=pl.CostEstimate(flops=8 * 10**9, bytes_accessed=40 * 2**20, transcendentals=0),
    )(lists, counts, tiles, *operands)


def gram_kernel(
    phase, count, slots, fixed, rank_ref, lists_ref, counts_ref, tiles_ref, in_ref, left_ref, *rest
):
    arrivals, rest = rest[:count], rest[count:]
    outs, (pool_ref, held_ref, current_ref, sum_ref, in_sems, sems) = rest[:-6], rest[-6:]
    steps, rows, vectors = held_ref.shape
    per = steps // 2
    chunks = in_sems.shape[0] // 2
    bunch = per // chunks
    inward = in_chunks(in_ref, held_ref, in_sems)
    loads = pool_loads(arrivals, pool_ref, sems)
    for copy in loads:
        copy.start()
    ahead = min(AHEAD // 2, chunks)
    for i in range(ahead):
        for d in range(2):
            inward(d * chunks + i).start()
    for copy in loads:
        copy.wait()

    def some(step, carry):
        spots = [(d, g, d * per + step * bunch + g) for d in range(2) for g in range(bunch)]

        @pl.when(step + ahead < chunks)
        def _():
            for d in range(2):
                inward(d * chunks + step + ahead).start()

        for d in range(2):
            inward(d * chunks + step).wait()
        for d, g, block in spots:
            entry = lambda j, block=block: lists_ref[phase, block * slots + j]
            for j in range(fixed):
                held_ref[block] += pair(entry, j, tiles_ref.at[d], pool_ref)
        for d, g, block in spots:
            entry = lambda j, block=block: lists_ref[phase, block * slots + j]
            add_rest(
                held_ref.at[block], fixed, counts_ref[phase, block], entry, tiles_ref.at[d], pool_ref
            )
        for d, g, block in spots:
            current_ref[pl.ds(g * rows, rows), pl.ds(d * vectors, vectors)] = held_ref[block].astype(BF16)
        part = jnp.dot(left_ref[step], current_ref[...], preferred_element_type=F32)

        @pl.when(step == 0)
        def _():
            sum_ref[...] = part

        @pl.when(step > 0)
        def _():
            sum_ref[...] += part

        return carry

    lax.fori_loop(0, chunks, some, 0)
    if len(outs) == 1:
        outs[0][...] = sum_ref[...]
        return
    send_ref, keep_ref = outs
    core = rank_ref[0] % 2
    outer, inner, own = send_ref.shape[:3]
    for n in range(outer * inner):
        keep_ref[n // inner, n % inner] = sum_ref[pl.ds(pl.multiple_of((2 * n + core) * own, own), own), :]
        send_ref[n // inner, n % inner] = sum_ref[pl.ds(pl.multiple_of((2 * n + 1 - core) * own, own), own), :].astype(send_ref.dtype)


def gram(phase, rank, lists, counts, tiles, current, left_t, arrivals, devices, sent, fixed):
    steps, rows, vectors = current.shape
    slots = lists.shape[1] // steps
    chunks = left_t.shape[0]
    cap = arrivals[0].shape[0]
    columns = left_t.shape[1]
    own = columns // devices
    block = pl.BlockSpec(memory_space=VMEM)
    dma = pltpu.SemaphoreType.DMA
    if own % 8:
        halves = [jax.ShapeDtypeStruct((columns, 2 * vectors), F32)]
    else:
        half = (devices // 8, 4, own, 2 * vectors)
        halves = [VMEM(half, sent), VMEM(half, F32)]
    room = 2 * ROOM + 4 * current.size + sum(2 * a.size for a in arrivals)
    return pl.pallas_call(
        functools.partial(gram_kernel, phase, len(arrivals), slots, fixed),
        out_shape=halves,
        in_specs=[pl.BlockSpec(memory_space=SMEM)] * 3
        + [block, pl.BlockSpec(memory_space=HBM), block]
        + [pl.BlockSpec(memory_space=HBM)] * len(arrivals),
        out_specs=[block] * len(halves),
        scratch_shapes=[
            VMEM((len(arrivals) * cap, rows, vectors), BF16),
            VMEM((steps, rows, vectors), F32),
            VMEM((left_t.shape[2], 2 * vectors), BF16),
            VMEM((columns, 2 * vectors), F32),
            dma((2 * chunks,)),
            dma((len(arrivals),)),
        ],
        compiler_params=pltpu.CompilerParams(vmem_limit_bytes=room),
        cost_estimate=pl.CostEstimate(flops=6 * 10**9, bytes_accessed=24 * 2**20, transcendentals=0),
        name="gram",
    )(rank, lists, counts, tiles, in_hbm(current), in_vmem(left_t), *map(in_hbm, arrivals))


def split_kernel(width, shift, count, final, scale, rank_ref, keep_ref, *rest):
    arrived, outs = rest[:count], rest[count:]
    mine = (rank_ref[0] >> shift) % width
    if final:
        vectors = outs[0].shape[-1]
        total = keep_ref[...]
        for ref in arrived:
            total = total + ref[...].astype(F32)
        total = total * scale
        for d in range(2):
            outs[0][d] = total[:, d * vectors:(d + 1) * vectors]
        return
    for mask in range(width):
        where = mine ^ mask
        if len(keep_ref.shape) == 4:
            part = keep_ref[:, where]
            for ref in arrived:
                part = part + ref[:, where].astype(F32)
        else:
            part = keep_ref[where]
            for ref in arrived:
                part = part + ref[where].astype(F32)
        outs[mask][...] = part.astype(outs[mask].dtype)


def split(rank, keep, arrived, width, shift, sent):
    part = keep.shape[:-3] + keep.shape[-2:]
    return pl.pallas_call(
        functools.partial(split_kernel, width, shift, len(arrived), False, None),
        out_shape=[VMEM(part, sent if n else F32) for n in range(width)],
        in_specs=[pl.BlockSpec(memory_space=SMEM)] + [pl.BlockSpec(memory_space=VMEM)] * (1 + len(arrived)),
        out_specs=[pl.BlockSpec(memory_space=VMEM)] * width,
        compiler_params=pltpu.CompilerParams(vmem_limit_bytes=ROOM),
    )(rank, *map(in_vmem, (keep, *arrived)))


def finish(rank, keep, arrived, scale):
    own, both = keep.shape
    return pl.pallas_call(
        functools.partial(split_kernel, 1, 0, len(arrived), True, scale),
        out_shape=jax.ShapeDtypeStruct((2, own, both // 2), F32),
        in_specs=[pl.BlockSpec(memory_space=SMEM)] + [pl.BlockSpec(memory_space=VMEM)] * (1 + len(arrived)),
        out_specs=pl.BlockSpec(memory_space=VMEM),
        compiler_params=pltpu.CompilerParams(vmem_limit_bytes=ROOM),
        name="finish",
    )(rank, *map(in_vmem, (keep, *arrived)))


def swap(value, mask, devices):
    return lax.ppermute(value, "rows", [(i, i ^ mask) for i in range(devices)])


def body(left, right, tiles, source_blocks, tile_index, send_blocks):
    block_rows = tiles.shape[-1]
    vectors = right.shape[1]
    local = right.shape[0] // block_rows
    devices = lax.axis_size("rows")
    slots = source_blocks.shape[-1]
    scale = 1.0 / math.sqrt(local * block_rows * devices)
    rank = lax.axis_index("rows").astype(jnp.int32).reshape(1)
    blocks = right.reshape(local, block_rows, vectors)
    order = exchange_order(devices)
    groups = exchange_groups(len(order))
    send = send_blocks.T

    early = min(EARLY, len(order))
    packed = pack(rank, send, blocks, order[:early])
    packed += pack(rank, send, blocks, order[early:], packed[:1])
    arrived = []
    for n, mask in enumerate(order):
        arrived.append(swap(packed[n], mask, devices))

    lists, counts = slot_lists(
        rank, send, source_blocks.reshape(2 * local, slots), tile_index.reshape(2 * local, slots),
        local, order, [start for start, _ in groups], tiles.shape[1],
    )
    tiles = jnp.concatenate([tiles, jnp.zeros((2, 1) + tiles.shape[2:], tiles.dtype)], axis=1)
    bunch = math.gcd(local, 4) * block_rows
    left_t = left.reshape(-1, bunch, vectors).transpose(0, 2, 1)
    tiles = in_vmem(tiles)
    current = hops(0, lists, counts, tiles, blocks, None, 4)
    for n, (start, stop) in enumerate(groups[:-1]):
        current = hops(n + 1, lists, counts, tiles, arrived[start:stop], current, 2)
    start, stop = groups[-1]
    sums = gram(
        len(groups), rank, lists, counts, tiles, current, left_t, arrived[start:stop], devices, F32, 1
    )
    if len(sums) == 1:
        mine = lax.psum_scatter(sums[0] * scale, "rows", scatter_dimension=0, tiled=True)
        return mine.reshape(mine.shape[0], 2, vectors).transpose(1, 0, 2)
    send, keep = sums
    outer = devices // 8
    got = swap(send, 1, devices)
    parts = split(rank, keep, [got], 4, 1, BF16)
    got = [swap(parts[n], n << 1, devices) for n in range(1, 4)]
    parts = split(rank, parts[0], got, outer, 3, F32)
    got = [swap(parts[n], n << 3, devices) for n in range(1, outer)]
    return finish(rank, parts[0], got, scale)


def solution(mesh):
    placed = (
        P("rows", None),
        P("rows", None),
        P(),
        P(None, "rows", None),
        P(None, "rows", None),
        P("rows", None),
    )

    return jax.shard_map(body, mesh=mesh, in_specs=placed, out_specs=P(None, "rows", None), check_vma=False)
```

```python
import functools
import math

import jax
import jax.numpy as jnp
from jax import lax
from jax.experimental import pallas as pl
from jax.experimental.pallas import tpu as pltpu
from jax.sharding import PartitionSpec as P


F32 = jnp.float32
BF16 = jnp.bfloat16
SHIFT = 1024
ROOM = 8 * 2**20
EARLY = 3
AHEAD = 6
SMEM = pltpu.SMEM
VMEM = pltpu.VMEM
HBM = pltpu.HBM


def exchange_order(devices):
    half = devices // 2
    far, near = list(range(half, devices)), list(range(1, half))
    order, far = far[:EARLY], far[EARLY:]
    while far or near:
        order += near[:1] + far[:1]
        near, far = near[1:], far[1:]
    return order


def exchange_groups(devices):
    half = devices // 2
    far, near = list(range(half, devices)), list(range(1, half))
    last = half - max(1, half // 8)
    first = half * 5 // 8
    return [near + far[:first], far[first:last], far[last:]]


def in_hbm(value):
    return pltpu.with_memory_space_constraint(value, HBM)


def in_vmem(value):
    return pltpu.with_memory_space_constraint(value, VMEM)


def whole(shape, space=VMEM):
    return pl.BlockSpec(shape, lambda *_: (0,) * len(shape), memory_space=space)


def pack_kernel(masks, after, rank_ref, send_ref, blocks_ref, *rest):
    rest = rest[after:]
    outs, (held_ref, in_sems, out_sems) = rest[: len(masks)], rest[len(masks):]
    cap = send_ref.shape[0]
    rank = rank_ref[0]
    inward, outward = [], []
    for n, mask in enumerate(masks):
        for c in range(cap):
            i = n * cap + c
            block = jnp.maximum(send_ref[c, rank ^ mask], 0)
            copy = pltpu.make_async_copy(blocks_ref.at[block], held_ref.at[i], in_sems.at[i])
            copy.start()
            inward.append(copy)
            outward.append(pltpu.make_async_copy(held_ref.at[i], outs[n].at[c], out_sems.at[i]))
    for one, two in zip(inward, outward):
        one.wait()
        two.start()
    for copy in outward:
        copy.wait()


def pack(rank, send, blocks, masks, after=()):
    cap = send.shape[0]
    count = len(masks) * cap
    return pl.pallas_call(
        functools.partial(pack_kernel, masks, len(after)),
        out_shape=[jax.ShapeDtypeStruct((cap,) + blocks.shape[1:], BF16)] * len(masks),
        in_specs=[whole((1,), SMEM), whole(send.shape, SMEM)]
        + [pl.BlockSpec(memory_space=HBM)] * (1 + len(after)),
        out_specs=[pl.BlockSpec(memory_space=HBM)] * len(masks),
        scratch_shapes=[
            VMEM((count,) + blocks.shape[1:], BF16),
            pltpu.SemaphoreType.DMA((count,)),
            pltpu.SemaphoreType.DMA((count,)),
        ],
        name="pack",
    )(rank, send, blocks, *after)


def slot_lists(rank, send, source, tile, local, order, starts, spare):
    cap = send.shape[0]
    slots = source.shape[1]
    mine = lax.dynamic_index_in_dim(send, rank[0], 1, keepdims=False)
    away = source >= local
    r = jnp.maximum(source - local, 0)
    c = r % cap
    mask = (r // cap) ^ rank[0]
    spot = jnp.where(
        mask[..., None] == jnp.array(order, jnp.int32), jnp.arange(len(order), dtype=jnp.int32), 0
    ).sum(-1)
    own = source
    for n in range(cap):
        own = jnp.where(away & (c == n), jnp.maximum(mine[n], 0), own)
    phase = jnp.zeros_like(source)
    first = jnp.zeros_like(source)
    far = away & (mask != 0)
    for n, start in enumerate(starts):
        phase = jnp.where(far & (spot >= start), n + 1, phase)
        first = jnp.where(far & (spot >= start), start, first)
    value = tile * SHIFT + jnp.where(far, (spot - first) * cap + c, own)
    phases = jnp.arange(len(starts) + 1, dtype=jnp.int32)[:, None, None]
    hit = (tile >= 0)[None] & (phase[None] == phases)
    k = jnp.arange(slots, dtype=jnp.int32)
    before = (hit[:, :, None, :] & (k[None, :] < k[:, None])).astype(jnp.int32).sum(-1)
    there = hit[:, :, None, :] & (before[:, :, None, :] == k[:, None])
    empty = spare * SHIFT
    lists = jnp.where(there, value[None, :, None, :] - empty, 0).sum(-1) + empty
    return lists.reshape(len(starts) + 1, -1), hit.astype(jnp.int32).sum(-1)


def pair(entry, j, tiles_ref, pool_ref):
    e0, e1 = entry(2 * j), entry(2 * j + 1)
    return jnp.dot(
        jnp.concatenate([tiles_ref[e0 // SHIFT], tiles_ref[e1 // SHIFT]], axis=1),
        jnp.concatenate([pool_ref[e0 % SHIFT], pool_ref[e1 % SHIFT]], axis=0),
        preferred_element_type=F32,
    )


def add_rest(acc_ref, done, count, entry, tiles_ref, pool_ref):
    def one(j, carry):
        acc_ref[...] += pair(entry, j, tiles_ref, pool_ref)
        return carry

    lax.fori_loop(done, (count + 1) // 2, one, 0)


def pool_loads(arrivals, pool_ref, sems):
    cap = arrivals[0].shape[0]
    return [
        pltpu.make_async_copy(ref, pool_ref.at[pl.ds(n * cap, cap)], sems.at[n])
        for n, ref in enumerate(arrivals)
    ]


def in_chunks(from_ref, to_ref, sems):
    size = from_ref.shape[0] // sems.shape[0]
    return lambda i: pltpu.make_async_copy(
        from_ref.at[pl.ds(i * size, size)], to_ref.at[pl.ds(i * size, size)], sems.at[i]
    )


def hops_kernel(phase, slots, fixed, count, lists_ref, counts_ref, tiles_ref, *rest):
    if phase == 0:
        pool_ref, out_ref, held_ref, out_sems = rest
    else:
        in_ref, arrivals = rest[0], rest[1:1 + count]
        out_ref, held_ref, out_sems, pool_ref, in_sems, sems = rest[1 + count:]
    chunks = out_sems.shape[0]
    steps = held_ref.shape[0]
    bunch = steps // chunks
    outward = in_chunks(held_ref, out_ref, out_sems)
    if phase:
        inward = in_chunks(in_ref, held_ref, in_sems)
        loads = pool_loads(arrivals, pool_ref, sems)
        for copy in loads:
            copy.start()
        ahead = min(AHEAD, chunks)
        for i in range(ahead):
            inward(i).start()
        for copy in loads:
            copy.wait()

    def some(step, carry):
        tiles = tiles_ref.at[2 * step // chunks]
        if phase:
            @pl.when(step + ahead < chunks)
            def _():
                inward(step + ahead).start()

            inward(step).wait()
        for g in range(bunch):
            block = step * bunch + g
            entry = lambda j, block=block: lists_ref[phase, block * slots + j]
            for j in range(fixed):
                value = pair(entry, j, tiles, pool_ref)
                if j or phase:
                    held_ref[block] += value
                else:
                    held_ref[block] = value
        for g in range(bunch):
            block = step * bunch + g
            entry = lambda j, block=block: lists_ref[phase, block * slots + j]
            add_rest(held_ref.at[block], fixed, counts_ref[phase, block], entry, tiles, pool_ref)
        outward(step).start()
        return carry

    lax.fori_loop(0, chunks, some, 0)
    for i in range(chunks):
        outward(i).wait()


def hops(phase, lists, counts, tiles, pool, current, fixed, bunch=4):
    steps = counts.shape[1]
    slots = lists.shape[1] // steps
    chunks = steps // math.gcd(bunch, steps // 2)
    rows, vectors = (pool if phase == 0 else pool[0]).shape[1:]
    dma = pltpu.SemaphoreType.DMA
    in_specs = [pl.BlockSpec(memory_space=SMEM)] * 2 + [pl.BlockSpec(memory_space=VMEM)]
    scratch = [VMEM((steps, rows, vectors), F32), dma((chunks,))]
    if phase == 0:
        operands, aliases, count, held = [pool], {}, 0, [pool]
        in_specs += [pl.BlockSpec(memory_space=VMEM)]
    else:
        count, held = len(pool), pool
        operands, aliases = [in_hbm(current), *map(in_hbm, pool)], {3: 0}
        in_specs += [pl.BlockSpec(memory_space=HBM)] * (1 + count)
        scratch += [VMEM((count * pool[0].shape[0], rows, vectors), BF16), dma((chunks,)), dma((count,))]
    room = ROOM + 4 * steps * rows * vectors + sum(2 * a.size for a in held)
    return pl.pallas_call(
        functools.partial(hops_kernel, phase, slots, fixed, count),
        out_shape=HBM((steps, rows, vectors), F32),
        in_specs=in_specs,
        out_specs=pl.BlockSpec(memory_space=HBM),
        scratch_shapes=scratch,
        input_output_aliases=aliases,
        compiler_params=pltpu.CompilerParams(vmem_limit_bytes=room),
        cost_estimate=pl.CostEstimate(flops=8 * 10**9, bytes_accessed=40 * 2**20, transcendentals=0),
    )(lists, counts, tiles, *operands)


def gram_kernel(
    phase, count, slots, fixed, rank_ref, lists_ref, counts_ref, tiles_ref, in_ref, left_ref, *rest
):
    arrivals, rest = rest[:count], rest[count:]
    outs, (pool_ref, held_ref, current_ref, sum_ref, in_sems, sems) = rest[:-6], rest[-6:]
    steps, rows, vectors = held_ref.shape
    per = steps // 2
    chunks = in_sems.shape[0] // 2
    bunch = per // chunks
    inward = in_chunks(in_ref, held_ref, in_sems)
    loads = pool_loads(arrivals, pool_ref, sems)
    for copy in loads:
        copy.start()
    ahead = min(2, chunks)
    for i in range(ahead):
        for d in range(2):
            inward(d * chunks + i).start()
    sum_ref[...] = jnp.zeros_like(sum_ref)
    for copy in loads:
        copy.wait()

    def some(step, carry):
        spots = [(d, g, d * per + step * bunch + g) for d in range(2) for g in range(bunch)]

        @pl.when(step + ahead < chunks)
        def _():
            for d in range(2):
                inward(d * chunks + step + ahead).start()

        for d in range(2):
            inward(d * chunks + step).wait()
        for d, g, block in spots:
            entry = lambda j, block=block: lists_ref[phase, block * slots + j]
            for j in range(fixed):
                held_ref[block] += pair(entry, j, tiles_ref.at[d], pool_ref)
        for d, g, block in spots:
            entry = lambda j, block=block: lists_ref[phase, block * slots + j]
            add_rest(
                held_ref.at[block], fixed, counts_ref[phase, block], entry, tiles_ref.at[d], pool_ref
            )
        for d, g, block in spots:
            current_ref[pl.ds(g * rows, rows), pl.ds(d * vectors, vectors)] = held_ref[block].astype(BF16)
        sum_ref[...] += jnp.dot(left_ref[step], current_ref[...], preferred_element_type=F32)
        return carry

    lax.fori_loop(0, chunks, some, 0)
    if len(outs) == 1:
        outs[0][...] = sum_ref[...]
        return
    send_ref, keep_ref = outs
    core = rank_ref[0] % 2
    outer, inner, own = send_ref.shape[:3]
    for n in range(outer * inner):
        keep_ref[n // inner, n % inner] = sum_ref[pl.ds(pl.multiple_of((2 * n + core) * own, own), own), :]
        send_ref[n // inner, n % inner] = sum_ref[pl.ds(pl.multiple_of((2 * n + 1 - core) * own, own), own), :].astype(send_ref.dtype)


def gram(phase, rank, lists, counts, tiles, current, left_t, arrivals, devices, sent, fixed):
    steps, rows, vectors = current.shape
    slots = lists.shape[1] // steps
    chunks = left_t.shape[0]
    cap = arrivals[0].shape[0]
    columns = left_t.shape[1]
    own = columns // devices
    block = pl.BlockSpec(memory_space=VMEM)
    dma = pltpu.SemaphoreType.DMA
    if own % 8:
        halves = [jax.ShapeDtypeStruct((columns, 2 * vectors), F32)]
    else:
        half = (devices // 8, 4, own, 2 * vectors)
        halves = [VMEM(half, sent), VMEM(half, F32)]
    room = 2 * ROOM + 4 * current.size + sum(2 * a.size for a in arrivals)
    return pl.pallas_call(
        functools.partial(gram_kernel, phase, len(arrivals), slots, fixed),
        out_shape=halves,
        in_specs=[pl.BlockSpec(memory_space=SMEM)] * 3
        + [block, pl.BlockSpec(memory_space=HBM), block]
        + [pl.BlockSpec(memory_space=HBM)] * len(arrivals),
        out_specs=[block] * len(halves),
        scratch_shapes=[
            VMEM((len(arrivals) * cap, rows, vectors), BF16),
            VMEM((steps, rows, vectors), F32),
            VMEM((left_t.shape[2], 2 * vectors), BF16),
            VMEM((columns, 2 * vectors), F32),
            dma((2 * chunks,)),
            dma((len(arrivals),)),
        ],
        compiler_params=pltpu.CompilerParams(vmem_limit_bytes=room),
        cost_estimate=pl.CostEstimate(flops=6 * 10**9, bytes_accessed=24 * 2**20, transcendentals=0),
        name="gram",
    )(rank, lists, counts, tiles, in_hbm(current), in_vmem(left_t), *map(in_hbm, arrivals))


def split_kernel(width, shift, count, final, scale, rank_ref, keep_ref, *rest):
    arrived, outs = rest[:count], rest[count:]
    mine = (rank_ref[0] >> shift) % width
    if final:
        vectors = outs[0].shape[-1]
        total = keep_ref[...]
        for ref in arrived:
            total = total + ref[...].astype(F32)
        total = total * scale
        for d in range(2):
            outs[0][d] = total[:, d * vectors:(d + 1) * vectors]
        return
    for mask in range(width):
        where = mine ^ mask
        if len(keep_ref.shape) == 4:
            part = keep_ref[:, where]
            for ref in arrived:
                part = part + ref[:, where].astype(F32)
        else:
            part = keep_ref[where]
            for ref in arrived:
                part = part + ref[where].astype(F32)
        outs[mask][...] = part.astype(outs[mask].dtype)


def split(rank, keep, arrived, width, shift, sent):
    part = keep.shape[:-3] + keep.shape[-2:]
    return pl.pallas_call(
        functools.partial(split_kernel, width, shift, len(arrived), False, None),
        out_shape=[VMEM(part, sent if n else F32) for n in range(width)],
        in_specs=[pl.BlockSpec(memory_space=SMEM)] + [pl.BlockSpec(memory_space=VMEM)] * (1 + len(arrived)),
        out_specs=[pl.BlockSpec(memory_space=VMEM)] * width,
        compiler_params=pltpu.CompilerParams(vmem_limit_bytes=ROOM),
    )(rank, *map(in_vmem, (keep, *arrived)))


def finish(rank, keep, arrived, scale):
    own, both = keep.shape
    return pl.pallas_call(
        functools.partial(split_kernel, 1, 0, len(arrived), True, scale),
        out_shape=jax.ShapeDtypeStruct((2, own, both // 2), F32),
        in_specs=[pl.BlockSpec(memory_space=SMEM)] + [pl.BlockSpec(memory_space=VMEM)] * (1 + len(arrived)),
        out_specs=pl.BlockSpec(memory_space=VMEM),
        compiler_params=pltpu.CompilerParams(vmem_limit_bytes=ROOM),
        name="finish",
    )(rank, *map(in_vmem, (keep, *arrived)))


def swap(value, mask, devices):
    return lax.ppermute(value, "rows", [(i, i ^ mask) for i in range(devices)])


def body(left, right, tiles, source_blocks, tile_index, send_blocks):
    block_rows = tiles.shape[-1]
    vectors = right.shape[1]
    local = right.shape[0] // block_rows
    devices = lax.axis_size("rows")
    slots = source_blocks.shape[-1]
    scale = 1.0 / math.sqrt(local * block_rows * devices)
    rank = lax.axis_index("rows").astype(jnp.int32).reshape(1)
    blocks = right.reshape(local, block_rows, vectors)
    order = exchange_order(devices)
    groups = exchange_groups(devices)
    send = send_blocks.T

    early = min(EARLY, len(order))
    packed = pack(rank, send, blocks, order[:early])
    packed += pack(rank, send, blocks, order[early:], packed[:1])
    arrived = {}
    for n, mask in enumerate(order):
        arrived[mask] = swap(packed[n], mask, devices)

    starts = [sum(map(len, groups[:n])) for n in range(len(groups))]
    lists, counts = slot_lists(
        rank, send, source_blocks.reshape(2 * local, slots), tile_index.reshape(2 * local, slots),
        local, sum(groups, []), starts, tiles.shape[1],
    )
    tiles = jnp.concatenate([tiles, jnp.zeros((2, 1) + tiles.shape[2:], tiles.dtype)], axis=1)
    bunch = math.gcd(local, 8) * block_rows
    left_t = left.reshape(-1, bunch, vectors).transpose(0, 2, 1)
    tiles = in_vmem(tiles)
    current = hops(0, lists, counts, tiles, blocks, None, 4)
    for n, group in enumerate(groups[:-1]):
        current = hops(
            n + 1, lists, counts, tiles, [arrived[mask] for mask in group], current, 2 if n else 4
        )
    sums = gram(
        len(groups), rank, lists, counts, tiles, current, left_t,
        [arrived[mask] for mask in groups[-1]], devices, F32, 1,
    )
    if len(sums) == 1:
        mine = lax.psum_scatter(sums[0] * scale, "rows", scatter_dimension=0, tiled=True)
        return mine.reshape(mine.shape[0], 2, vectors).transpose(1, 0, 2)
    send, keep = sums
    outer = devices // 8
    got = swap(send, 1, devices)
    parts = split(rank, keep, [got], 4, 1, BF16)
    got = [swap(parts[n], n << 1, devices) for n in range(1, 4)]
    parts = split(rank, parts[0], got, outer, 3, F32)
    got = [swap(parts[n], n << 3, devices) for n in range(1, outer)]
    return finish(rank, parts[0], got, scale)


def solution(mesh):
    placed = (
        P("rows", None),
        P("rows", None),
        P(),
        P(None, "rows", None),
        P(None, "rows", None),
        P("rows", None),
    )

    return jax.shard_map(body, mesh=mesh, in_specs=placed, out_specs=P(None, "rows", None), check_vma=False)
```

```python
import functools
import math

import jax
import jax.numpy as jnp
from jax import lax
from jax.experimental import pallas as pl
from jax.experimental.pallas import tpu as pltpu
from jax.sharding import PartitionSpec as P


F32 = jnp.float32
BF16 = jnp.bfloat16
SHIFT = 1024
ROOM = 8 * 2**20
LATE = 13
MOST = 40
EARLY = 3
SMEM = pltpu.SMEM
VMEM = pltpu.VMEM
HBM = pltpu.HBM


def exchange_order(devices):
    half = devices // 2
    far, near = list(range(half, devices)), list(range(1, half))
    order, far = far[:EARLY], far[EARLY:]
    while far or near:
        order += near[:1] + far[:1]
        near, far = near[1:], far[1:]
    return order


def exchange_groups(count):
    early = count - min(LATE, count // 2)
    parts = -(-early // MOST)
    cuts = [early * n // parts for n in range(parts + 1)]
    return list(zip(cuts, cuts[1:] + [count]))


def in_hbm(value):
    return pltpu.with_memory_space_constraint(value, HBM)


def in_vmem(value):
    return pltpu.with_memory_space_constraint(value, VMEM)


def whole(shape, space=VMEM):
    return pl.BlockSpec(shape, lambda *_: (0,) * len(shape), memory_space=space)


def pack_kernel(masks, after, rank_ref, send_ref, blocks_ref, *rest):
    rest = rest[after:]
    outs, (held_ref, in_sems, out_sems) = rest[: len(masks)], rest[len(masks):]
    cap = send_ref.shape[0]
    rank = rank_ref[0]
    inward, outward = [], []
    for n, mask in enumerate(masks):
        for c in range(cap):
            i = n * cap + c
            block = jnp.maximum(send_ref[c, rank ^ mask], 0)
            copy = pltpu.make_async_copy(blocks_ref.at[block], held_ref.at[i], in_sems.at[i])
            copy.start()
            inward.append(copy)
            outward.append(pltpu.make_async_copy(held_ref.at[i], outs[n].at[c], out_sems.at[i]))
    for one, two in zip(inward, outward):
        one.wait()
        two.start()
    for copy in outward:
        copy.wait()


def pack(rank, send, blocks, masks, after=()):
    cap = send.shape[0]
    count = len(masks) * cap
    return pl.pallas_call(
        functools.partial(pack_kernel, masks, len(after)),
        out_shape=[jax.ShapeDtypeStruct((cap,) + blocks.shape[1:], BF16)] * len(masks),
        in_specs=[whole((1,), SMEM), whole(send.shape, SMEM)]
        + [pl.BlockSpec(memory_space=HBM)] * (1 + len(after)),
        out_specs=[pl.BlockSpec(memory_space=HBM)] * len(masks),
        scratch_shapes=[
            VMEM((count,) + blocks.shape[1:], BF16),
            pltpu.SemaphoreType.DMA((count,)),
            pltpu.SemaphoreType.DMA((count,)),
        ],
        name="pack",
    )(rank, send, blocks, *after)


def slot_lists(rank, send, source, tile, local, order, starts, spare):
    cap = send.shape[0]
    slots = source.shape[1]
    mine = lax.dynamic_index_in_dim(send, rank[0], 1, keepdims=False)
    away = source >= local
    r = jnp.maximum(source - local, 0)
    c = r % cap
    mask = (r // cap) ^ rank[0]
    spot = jnp.where(
        mask[..., None] == jnp.array(order, jnp.int32), jnp.arange(len(order), dtype=jnp.int32), 0
    ).sum(-1)
    own = source
    for n in range(cap):
        own = jnp.where(away & (c == n), jnp.maximum(mine[n], 0), own)
    phase = jnp.zeros_like(source)
    first = jnp.zeros_like(source)
    far = away & (mask != 0)
    for n, start in enumerate(starts):
        phase = jnp.where(far & (spot >= start), n + 1, phase)
        first = jnp.where(far & (spot >= start), start, first)
    value = tile * SHIFT + jnp.where(far, (spot - first) * cap + c, own)
    phases = jnp.arange(len(starts) + 1, dtype=jnp.int32)[:, None, None]
    hit = (tile >= 0)[None] & (phase[None] == phases)
    k = jnp.arange(slots, dtype=jnp.int32)
    before = (hit[:, :, None, :] & (k[None, :] < k[:, None])).astype(jnp.int32).sum(-1)
    there = hit[:, :, None, :] & (before[:, :, None, :] == k[:, None])
    empty = spare * SHIFT
    lists = jnp.where(there, value[None, :, None, :] - empty, 0).sum(-1) + empty
    return lists.reshape(len(starts) + 1, -1), hit.astype(jnp.int32).sum(-1)


def pair(entry, j, tiles_ref, pool_ref):
    e0, e1 = entry(2 * j), entry(2 * j + 1)
    return jnp.dot(
        jnp.concatenate([tiles_ref[e0 // SHIFT], tiles_ref[e1 // SHIFT]], axis=1),
        jnp.concatenate([pool_ref[e0 % SHIFT], pool_ref[e1 % SHIFT]], axis=0),
        preferred_element_type=F32,
    )


def add_rest(acc_ref, done, count, entry, tiles_ref, pool_ref):
    def one(j, carry):
        acc_ref[...] += pair(entry, j, tiles_ref, pool_ref)
        return carry

    lax.fori_loop(done, (count + 1) // 2, one, 0)


def pool_loads(arrivals, pool_ref, sems):
    cap = arrivals[0].shape[0]
    return [
        pltpu.make_async_copy(ref, pool_ref.at[pl.ds(n * cap, cap)], sems.at[n])
        for n, ref in enumerate(arrivals)
    ]


def in_chunks(from_ref, to_ref, sems):
    size = from_ref.shape[0] // sems.shape[0]
    return lambda i: pltpu.make_async_copy(
        from_ref.at[pl.ds(i * size, size)], to_ref.at[pl.ds(i * size, size)], sems.at[i]
    )


def hops_kernel(slots, fixed, lists_ref, counts_ref, tiles_ref, pool_ref, out_ref, held_ref, out_sems):
    chunks = out_sems.shape[0]
    bunch = held_ref.shape[0] // chunks
    outward = in_chunks(held_ref, out_ref, out_sems)

    def some(step, carry):
        tiles = tiles_ref.at[2 * step // chunks]
        for g in range(bunch):
            block = step * bunch + g
            entry = lambda j, block=block: lists_ref[0, block * slots + j]
            for j in range(fixed):
                value = pair(entry, j, tiles, pool_ref)
                if j:
                    held_ref[block] += value
                else:
                    held_ref[block] = value
        for g in range(bunch):
            block = step * bunch + g
            entry = lambda j, block=block: lists_ref[0, block * slots + j]
            add_rest(held_ref.at[block], fixed, counts_ref[0, block], entry, tiles, pool_ref)
        outward(step).start()
        return carry

    lax.fori_loop(0, chunks, some, 0)
    for i in range(chunks):
        outward(i).wait()


def hops(lists, counts, tiles, pool, fixed, bunch=4):
    steps = counts.shape[1]
    slots = lists.shape[1] // steps
    chunks = steps // math.gcd(bunch, steps // 2)
    rows, vectors = pool.shape[1:]
    block = pl.BlockSpec(memory_space=VMEM)
    return pl.pallas_call(
        functools.partial(hops_kernel, slots, fixed),
        out_shape=HBM((steps, rows, vectors), F32),
        in_specs=[pl.BlockSpec(memory_space=SMEM)] * 2 + [block] * 2,
        out_specs=pl.BlockSpec(memory_space=HBM),
        scratch_shapes=[VMEM((steps, rows, vectors), F32), pltpu.SemaphoreType.DMA((chunks,))],
        compiler_params=pltpu.CompilerParams(
            vmem_limit_bytes=ROOM + 4 * steps * rows * vectors + 2 * pool.size
        ),
        cost_estimate=pl.CostEstimate(flops=8 * 10**9, bytes_accessed=40 * 2**20, transcendentals=0),
        name="hops",
    )(lists, counts, tiles, pool)


def adjoint_kernel(phase, slots, count, lists_ref, counts_ref, tiles_ref, left_ref, out_ref, sum_ref):
    local, rows = left_ref.shape[:2]
    for s in range(2 * count):
        sum_ref[s] = jnp.zeros_like(sum_ref[s])

    def one_block(block, carry):
        d = block // local
        tiles = tiles_ref.at[d]

        def two(j, carry):
            e0 = lists_ref[phase, block * slots + 2 * j]
            e1 = lists_ref[phase, block * slots + 2 * j + 1]
            value = lax.dot_general(
                jnp.concatenate([tiles[e0 // SHIFT], tiles[e1 // SHIFT]], axis=1),
                left_ref[block % local], (((0,), (0,)), ((), ())), preferred_element_type=F32,
            )
            sum_ref[d * count + e0 % SHIFT] += value[:rows]
            sum_ref[d * count + e1 % SHIFT] += value[rows:]
            return carry

        return lax.fori_loop(0, (counts_ref[phase, block] + 1) // 2, two, carry)

    lax.fori_loop(0, 2 * local, one_block, 0)
    for d in range(2):
        for s in range(count):
            out_ref[d, :, s * rows:(s + 1) * rows] = sum_ref[d * count + s].astype(BF16).T


def adjoint(phase, lists, counts, tiles, left, count):
    slots = lists.shape[1] // counts.shape[1]
    rows, vectors = left.shape[1:]
    block = pl.BlockSpec(memory_space=VMEM)
    size = 2 * count * rows * vectors
    return pl.pallas_call(
        functools.partial(adjoint_kernel, phase, slots, count),
        out_shape=jax.ShapeDtypeStruct((2, vectors, count * rows), BF16),
        in_specs=[pl.BlockSpec(memory_space=SMEM)] * 2 + [block] * 2,
        out_specs=block,
        scratch_shapes=[VMEM((2 * count, rows, vectors), F32)],
        compiler_params=pltpu.CompilerParams(vmem_limit_bytes=ROOM + 6 * size + 2 * left.size),
        cost_estimate=pl.CostEstimate(flops=8 * 10**9, bytes_accessed=16 * 2**20, transcendentals=0),
        name="adjoint",
    )(lists, counts, tiles, left)


def gram_kernel(
    phase, count, slots, fixed, more, lists_ref, counts_ref, tiles_ref, in_ref, left_ref, *rest
):
    arrivals, (sum_ref, pool_ref, held_ref, high_ref, low_ref, in_sems, sems) = rest[:count], rest[count:]
    steps, rows, vectors = held_ref.shape
    per = steps // 2
    chunks = in_sems.shape[0] // 2
    bunch = per // chunks
    inward = None if more else in_chunks(in_ref, held_ref, in_sems)
    loads = pool_loads(arrivals, pool_ref, sems)
    for copy in loads:
        copy.start()
    ahead = min(2, chunks)
    if more:
        sum_ref[...] = in_ref[...]
    else:
        for i in range(ahead):
            for d in range(2):
                inward(d * chunks + i).start()
        sum_ref[...] = jnp.zeros_like(sum_ref)
    for copy in loads:
        copy.wait()

    def some(step, carry):
        spots = [(d, g, d * per + step * bunch + g) for d in range(2) for g in range(bunch)]

        if not more:
            @pl.when(step + ahead < chunks)
            def _():
                for d in range(2):
                    inward(d * chunks + step + ahead).start()

            for d in range(2):
                inward(d * chunks + step).wait()
        for d, g, block in spots:
            entry = lambda j, block=block: lists_ref[phase, block * slots + j]
            if more:
                held_ref[block] = jnp.zeros_like(held_ref[block])
            for j in range(fixed):
                held_ref[block] += pair(entry, j, tiles_ref.at[d], pool_ref)
        for d, g, block in spots:
            entry = lambda j, block=block: lists_ref[phase, block * slots + j]
            add_rest(
                held_ref.at[block], fixed, counts_ref[phase, block], entry, tiles_ref.at[d], pool_ref
            )
        for d, g, block in spots:
            value = held_ref[block]
            high = value.astype(BF16)
            spot = (pl.ds(g * rows, rows), pl.ds(d * vectors, vectors))
            high_ref[spot] = high
            low_ref[spot] = (value - high.astype(F32)).astype(BF16)
        sum_ref[...] += jnp.dot(left_ref[step], high_ref[...], preferred_element_type=F32)
        sum_ref[...] += jnp.dot(left_ref[step], low_ref[...], preferred_element_type=F32)
        return carry

    lax.fori_loop(0, chunks, some, 0)


def gram(phase, lists, counts, tiles, current, left_t, arrivals, fixed):
    steps = counts.shape[1]
    more = current.ndim == 2
    rows, vectors = arrivals[0].shape[1:]
    slots = lists.shape[1] // steps
    chunks, columns, depth = left_t.shape
    cap = arrivals[0].shape[0]
    block = pl.BlockSpec(memory_space=VMEM)
    dma = pltpu.SemaphoreType.DMA
    room = 2 * ROOM + 4 * steps * rows * vectors + sum(2 * a.size for a in arrivals)
    return pl.pallas_call(
        functools.partial(gram_kernel, phase, len(arrivals), slots, fixed, more),
        out_shape=jax.ShapeDtypeStruct((columns, 2 * vectors), F32),
        in_specs=[pl.BlockSpec(memory_space=SMEM)] * 2
        + [block, block if more else pl.BlockSpec(memory_space=HBM), block]
        + [pl.BlockSpec(memory_space=HBM)] * len(arrivals),
        out_specs=block,
        scratch_shapes=[
            VMEM((len(arrivals) * cap, rows, vectors), BF16),
            VMEM((steps, rows, vectors), F32),
            VMEM((depth, 2 * vectors), BF16),
            VMEM((depth, 2 * vectors), BF16),
            dma((2 * chunks,)),
            dma((len(arrivals),)),
        ],
        compiler_params=pltpu.CompilerParams(vmem_limit_bytes=room),
        cost_estimate=pl.CostEstimate(flops=12 * 10**9, bytes_accessed=24 * 2**20, transcendentals=0),
        name="gram",
    )(lists, counts, tiles, current if more else in_hbm(current), in_vmem(left_t), *map(in_hbm, arrivals))


def late_kernel(count, rank_ref, in_ref, adjoint_ref, *rest):
    arrivals, rest = rest[:count], rest[count:]
    outs, (sum_ref, pool_ref, sems) = rest[:-3], rest[-3:]
    blocks, rows, vectors = pool_ref.shape
    loads = pool_loads(arrivals, pool_ref, sems)
    for copy in loads:
        copy.start()
    for copy in loads:
        copy.wait()
    pool = pool_ref[...].reshape(blocks * rows, vectors)
    for d in range(2):
        side = (slice(None), slice(d * vectors, (d + 1) * vectors))
        sum_ref[side] = in_ref[side] + jnp.dot(adjoint_ref[d], pool, preferred_element_type=F32)
    if len(outs) == 1:
        outs[0][...] = sum_ref[...]
        return
    send_ref, keep_ref = outs
    core = rank_ref[0] % 2
    outer, inner, own = send_ref.shape[:3]
    for n in range(outer * inner):
        keep_ref[n // inner, n % inner] = sum_ref[pl.ds(pl.multiple_of((2 * n + core) * own, own), own), :]
        send_ref[n // inner, n % inner] = sum_ref[
            pl.ds(pl.multiple_of((2 * n + 1 - core) * own, own), own), :
        ].astype(send_ref.dtype)


def late(rank, sums, adjoint, arrivals, devices, sent):
    columns, both = sums.shape
    own = columns // devices
    cap, rows, vectors = arrivals[0].shape
    block = pl.BlockSpec(memory_space=VMEM)
    if own % 8:
        halves = [jax.ShapeDtypeStruct(sums.shape, F32)]
    else:
        half = (devices // 8, 4, own, both)
        halves = [VMEM(half, sent), VMEM(half, F32)]
    return pl.pallas_call(
        functools.partial(late_kernel, len(arrivals)),
        out_shape=halves,
        in_specs=[pl.BlockSpec(memory_space=SMEM), block, block]
        + [pl.BlockSpec(memory_space=HBM)] * len(arrivals),
        out_specs=[block] * len(halves),
        scratch_shapes=[
            VMEM(sums.shape, F32),
            VMEM((len(arrivals) * cap, rows, vectors), BF16),
            pltpu.SemaphoreType.DMA((len(arrivals),)),
        ],
        compiler_params=pltpu.CompilerParams(
            vmem_limit_bytes=2 * ROOM + sum(2 * a.size for a in arrivals)
        ),
        cost_estimate=pl.CostEstimate(flops=4 * 10**9, bytes_accessed=12 * 2**20, transcendentals=0),
        name="late",
    )(rank, in_vmem(sums), in_vmem(adjoint), *map(in_hbm, arrivals))


def split_kernel(width, shift, count, final, scale, rank_ref, keep_ref, *rest):
    arrived, outs = rest[:count], rest[count:]
    mine = (rank_ref[0] >> shift) % width
    if final:
        vectors = outs[0].shape[-1]
        total = keep_ref[...]
        for ref in arrived:
            total = total + ref[...].astype(F32)
        total = total * scale
        for d in range(2):
            outs[0][d] = total[:, d * vectors:(d + 1) * vectors]
        return
    for mask in range(width):
        where = mine ^ mask
        if len(keep_ref.shape) == 4:
            part = keep_ref[:, where]
            for ref in arrived:
                part = part + ref[:, where].astype(F32)
        else:
            part = keep_ref[where]
            for ref in arrived:
                part = part + ref[where].astype(F32)
        outs[mask][...] = part.astype(outs[mask].dtype)


def split(rank, keep, arrived, width, shift, sent):
    part = keep.shape[:-3] + keep.shape[-2:]
    return pl.pallas_call(
        functools.partial(split_kernel, width, shift, len(arrived), False, None),
        out_shape=[VMEM(part, sent if n else F32) for n in range(width)],
        in_specs=[pl.BlockSpec(memory_space=SMEM)] + [pl.BlockSpec(memory_space=VMEM)] * (1 + len(arrived)),
        out_specs=[pl.BlockSpec(memory_space=VMEM)] * width,
        compiler_params=pltpu.CompilerParams(vmem_limit_bytes=ROOM),
    )(rank, *map(in_vmem, (keep, *arrived)))


def finish(rank, keep, arrived, scale):
    own, both = keep.shape
    return pl.pallas_call(
        functools.partial(split_kernel, 1, 0, len(arrived), True, scale),
        out_shape=jax.ShapeDtypeStruct((2, own, both // 2), F32),
        in_specs=[pl.BlockSpec(memory_space=SMEM)] + [pl.BlockSpec(memory_space=VMEM)] * (1 + len(arrived)),
        out_specs=pl.BlockSpec(memory_space=VMEM),
        compiler_params=pltpu.CompilerParams(vmem_limit_bytes=ROOM),
        name="finish",
    )(rank, *map(in_vmem, (keep, *arrived)))


def swap(value, mask, devices):
    return lax.ppermute(value, "rows", [(i, i ^ mask) for i in range(devices)])


def body(left, right, tiles, source_blocks, tile_index, send_blocks):
    block_rows = tiles.shape[-1]
    vectors = right.shape[1]
    local = right.shape[0] // block_rows
    devices = lax.axis_size("rows")
    slots = source_blocks.shape[-1]
    scale = 1.0 / math.sqrt(local * block_rows * devices)
    rank = lax.axis_index("rows").astype(jnp.int32).reshape(1)
    blocks = right.reshape(local, block_rows, vectors)
    order = exchange_order(devices)
    groups = exchange_groups(len(order))
    send = send_blocks.T

    early = min(EARLY, len(order))
    packed = pack(rank, send, blocks, order[:early])
    packed += pack(rank, send, blocks, order[early:], packed[:1])
    arrived = []
    for n, mask in enumerate(order):
        arrived.append(swap(packed[n], mask, devices))

    lists, counts = slot_lists(
        rank, send, source_blocks.reshape(2 * local, slots), tile_index.reshape(2 * local, slots),
        local, order, [start for start, _ in groups], tiles.shape[1],
    )
    tiles = jnp.concatenate([tiles, jnp.zeros((2, 1) + tiles.shape[2:], tiles.dtype)], axis=1)
    bunch = math.gcd(local, 8) * block_rows
    left_t = left.reshape(-1, bunch, vectors).transpose(0, 2, 1)
    tiles = in_vmem(tiles)
    sums = hops(lists, counts, tiles, blocks, 4)
    start, stop = groups[-1]
    met = adjoint(
        len(groups), lists, counts, tiles, left.reshape(blocks.shape), (stop - start) * send.shape[0]
    )
    for n, (first, last) in enumerate(groups[:-1]):
        sums = gram(n + 1, lists, counts, tiles, sums, left_t, arrived[first:last], 3)
    sums = late(rank, sums, met, arrived[start:stop], devices, F32)
    if len(sums) == 1:
        mine = lax.psum_scatter(sums[0] * scale, "rows", scatter_dimension=0, tiled=True)
        return mine.reshape(mine.shape[0], 2, vectors).transpose(1, 0, 2)
    send, keep = sums
    outer = devices // 8
    got = swap(send, 1, devices)
    parts = split(rank, keep, [got], 4, 1, BF16)
    got = [swap(parts[n], n << 1, devices) for n in range(1, 4)]
    parts = split(rank, parts[0], got, outer, 3, F32)
    got = [swap(parts[n], n << 3, devices) for n in range(1, outer)]
    return finish(rank, parts[0], got, scale)


def solution(mesh):
    placed = (
        P("rows", None),
        P("rows", None),
        P(),
        P(None, "rows", None),
        P(None, "rows", None),
        P("rows", None),
    )

    return jax.shard_map(body, mesh=mesh, in_specs=placed, out_specs=P(None, "rows", None), check_vma=False)
```

```python
import functools
import math

import jax
import jax.numpy as jnp
from jax import lax
from jax.experimental import pallas as pl
from jax.experimental.pallas import tpu as pltpu
from jax.sharding import PartitionSpec as P


F32 = jnp.float32
BF16 = jnp.bfloat16
SHIFT = 1024
ROOM = 8 * 2**20
LATE = 13
MOST = 40
EARLY = 3
SMEM = pltpu.SMEM
VMEM = pltpu.VMEM
HBM = pltpu.HBM


def exchange_order(devices):
    half = devices // 2
    far, near = list(range(half, devices)), list(range(1, half))
    order, far = far[:EARLY], far[EARLY:]
    while far or near:
        order += near[:1] + far[:1]
        near, far = near[1:], far[1:]
    return order


def exchange_groups(count):
    early = count - min(LATE, count // 2)
    parts = -(-early // MOST)
    cuts = [early * n // parts for n in range(parts + 1)]
    return list(zip(cuts, cuts[1:] + [count]))


def in_hbm(value):
    return pltpu.with_memory_space_constraint(value, HBM)


def in_vmem(value):
    return pltpu.with_memory_space_constraint(value, VMEM)


def whole(shape, space=VMEM):
    return pl.BlockSpec(shape, lambda *_: (0,) * len(shape), memory_space=space)


def first_kernel(masks, rank_ref, send_ref, blocks_ref, *rest):
    outs, sems = rest[: len(masks)], rest[len(masks)]
    cap = send_ref.shape[0]
    copies = []
    for n, mask in enumerate(masks):
        for c in range(cap):
            block = jnp.maximum(send_ref[c, rank_ref[0] ^ mask], 0)
            copy = pltpu.make_async_copy(blocks_ref.at[block], outs[n].at[c], sems.at[n * cap + c])
            copy.start()
            copies.append(copy)
    for copy in copies:
        copy.wait()


def first_pack(rank, send, blocks, masks):
    cap = send.shape[0]
    return pl.pallas_call(
        functools.partial(first_kernel, masks),
        out_shape=[VMEM((cap,) + blocks.shape[1:], BF16)] * len(masks),
        in_specs=[pl.BlockSpec(memory_space=SMEM)] * 2 + [pl.BlockSpec(memory_space=HBM)],
        out_specs=[pl.BlockSpec(memory_space=VMEM)] * len(masks),
        scratch_shapes=[pltpu.SemaphoreType.DMA((len(masks) * cap,))],
        compiler_params=pltpu.CompilerParams(vmem_limit_bytes=ROOM),
        name="first_pack",
    )(rank, send, in_hbm(blocks))


def pack_kernel(masks, after, rank_ref, send_ref, blocks_ref, *rest):
    rest = rest[after:]
    outs, (held_ref, in_sems, out_sems) = rest[: len(masks)], rest[len(masks):]
    cap = send_ref.shape[0]
    rank = rank_ref[0]
    inward, outward = [], []
    for n, mask in enumerate(masks):
        for c in range(cap):
            i = n * cap + c
            block = jnp.maximum(send_ref[c, rank ^ mask], 0)
            copy = pltpu.make_async_copy(blocks_ref.at[block], held_ref.at[i], in_sems.at[i])
            copy.start()
            inward.append(copy)
            outward.append(pltpu.make_async_copy(held_ref.at[i], outs[n].at[c], out_sems.at[i]))
    for one, two in zip(inward, outward):
        one.wait()
        two.start()
    for copy in outward:
        copy.wait()


def pack(rank, send, blocks, masks, after=()):
    cap = send.shape[0]
    count = len(masks) * cap
    return pl.pallas_call(
        functools.partial(pack_kernel, masks, len(after)),
        out_shape=[jax.ShapeDtypeStruct((cap,) + blocks.shape[1:], BF16)] * len(masks),
        in_specs=[whole((1,), SMEM), whole(send.shape, SMEM)]
        + [pl.BlockSpec(memory_space=HBM)] * (1 + len(after)),
        out_specs=[pl.BlockSpec(memory_space=HBM)] * len(masks),
        scratch_shapes=[
            VMEM((count,) + blocks.shape[1:], BF16),
            pltpu.SemaphoreType.DMA((count,)),
            pltpu.SemaphoreType.DMA((count,)),
        ],
        compiler_params=pltpu.CompilerParams(vmem_limit_bytes=ROOM + 2 * count * blocks[0].size),
        name="pack",
    )(rank, send, in_hbm(blocks), *after)


def slot_lists(rank, send, source, tile, local, order, starts, spare):
    cap = send.shape[0]
    slots = source.shape[1]
    mine = lax.dynamic_index_in_dim(send, rank[0], 1, keepdims=False)
    away = source >= local
    r = jnp.maximum(source - local, 0)
    c = r % cap
    mask = (r // cap) ^ rank[0]
    spot = jnp.where(
        mask[..., None] == jnp.array(order, jnp.int32), jnp.arange(len(order), dtype=jnp.int32), 0
    ).sum(-1)
    own = source
    for n in range(cap):
        own = jnp.where(away & (c == n), jnp.maximum(mine[n], 0), own)
    phase = jnp.zeros_like(source)
    first = jnp.zeros_like(source)
    far = away & (mask != 0)
    for n, start in enumerate(starts):
        phase = jnp.where(far & (spot >= start), n + 1, phase)
        first = jnp.where(far & (spot >= start), start, first)
    value = tile * SHIFT + jnp.where(far, (spot - first) * cap + c, own)
    phases = jnp.arange(len(starts) + 1, dtype=jnp.int32)[:, None, None]
    hit = (tile >= 0)[None] & (phase[None] == phases)
    k = jnp.arange(slots, dtype=jnp.int32)
    before = (hit[:, :, None, :] & (k[None, :] < k[:, None])).astype(jnp.int32).sum(-1)
    there = hit[:, :, None, :] & (before[:, :, None, :] == k[:, None])
    empty = spare * SHIFT
    lists = jnp.where(there, value[None, :, None, :] - empty, 0).sum(-1) + empty
    return lists.reshape(len(starts) + 1, -1), hit.astype(jnp.int32).sum(-1)


def pair(entry, j, tiles_ref, pool_ref):
    e0, e1 = entry(2 * j), entry(2 * j + 1)
    return jnp.dot(
        jnp.concatenate([tiles_ref[e0 // SHIFT], tiles_ref[e1 // SHIFT]], axis=1),
        jnp.concatenate([pool_ref[e0 % SHIFT], pool_ref[e1 % SHIFT]], axis=0),
        preferred_element_type=F32,
    )


def add_rest(acc_ref, done, count, entry, tiles_ref, pool_ref):
    def one(j, carry):
        acc_ref[...] += pair(entry, j, tiles_ref, pool_ref)
        return carry

    lax.fori_loop(done, (count + 1) // 2, one, 0)


def pool_loads(arrivals, pool_ref, sems):
    cap = arrivals[0].shape[0]
    return [
        pltpu.make_async_copy(ref, pool_ref.at[pl.ds(n * cap, cap)], sems.at[n])
        for n, ref in enumerate(arrivals)
    ]


def in_chunks(from_ref, to_ref, sems):
    size = from_ref.shape[0] // sems.shape[0]
    return lambda i: pltpu.make_async_copy(
        from_ref.at[pl.ds(i * size, size)], to_ref.at[pl.ds(i * size, size)], sems.at[i]
    )


def hops_kernel(slots, fixed, lists_ref, counts_ref, tiles_ref, pool_ref, out_ref, held_ref, out_sems):
    chunks = out_sems.shape[0]
    bunch = held_ref.shape[0] // chunks
    outward = in_chunks(held_ref, out_ref, out_sems)

    def some(step, carry):
        tiles = tiles_ref.at[2 * step // chunks]
        for g in range(bunch):
            block = step * bunch + g
            entry = lambda j, block=block: lists_ref[0, block * slots + j]
            for j in range(fixed):
                value = pair(entry, j, tiles, pool_ref)
                if j:
                    held_ref[block] += value
                else:
                    held_ref[block] = value
        for g in range(bunch):
            block = step * bunch + g
            entry = lambda j, block=block: lists_ref[0, block * slots + j]
            add_rest(held_ref.at[block], fixed, counts_ref[0, block], entry, tiles, pool_ref)
        outward(step).start()
        return carry

    lax.fori_loop(0, chunks, some, 0)
    for i in range(chunks):
        outward(i).wait()


def hops(lists, counts, tiles, pool, fixed, bunch=4):
    steps = counts.shape[1]
    slots = lists.shape[1] // steps
    chunks = steps // math.gcd(bunch, steps // 2)
    rows, vectors = pool.shape[1:]
    block = pl.BlockSpec(memory_space=VMEM)
    return pl.pallas_call(
        functools.partial(hops_kernel, slots, fixed),
        out_shape=HBM((steps, rows, vectors), F32),
        in_specs=[pl.BlockSpec(memory_space=SMEM)] * 2 + [block] * 2,
        out_specs=pl.BlockSpec(memory_space=HBM),
        scratch_shapes=[VMEM((steps, rows, vectors), F32), pltpu.SemaphoreType.DMA((chunks,))],
        compiler_params=pltpu.CompilerParams(
            vmem_limit_bytes=ROOM + 4 * steps * rows * vectors + 2 * pool.size
        ),
        cost_estimate=pl.CostEstimate(flops=8 * 10**9, bytes_accessed=40 * 2**20, transcendentals=0),
        name="hops",
    )(lists, counts, tiles, pool)


def adjoint_kernel(phase, slots, count, lists_ref, counts_ref, tiles_ref, left_ref, *rest):
    outs, sum_ref = rest[:-1], rest[-1]
    local, rows = left_ref.shape[:2]
    for s in range(2 * count):
        sum_ref[s] = jnp.zeros_like(sum_ref[s])

    def one_block(block, carry):
        d = block // local
        tiles = tiles_ref.at[d]

        def two(j, carry):
            e0 = lists_ref[phase, block * slots + 2 * j]
            e1 = lists_ref[phase, block * slots + 2 * j + 1]
            value = lax.dot_general(
                jnp.concatenate([tiles[e0 // SHIFT], tiles[e1 // SHIFT]], axis=1),
                left_ref[block % local], (((0,), (0,)), ((), ())), preferred_element_type=F32,
            )
            sum_ref[d * count + e0 % SHIFT] += value[:rows]
            sum_ref[d * count + e1 % SHIFT] += value[rows:]
            return carry

        return lax.fori_loop(0, (counts_ref[phase, block] + 1) // 2, two, carry)

    lax.fori_loop(0, 2 * local, one_block, 0)
    first = 0
    for out_ref in outs:
        size = out_ref.shape[2] // rows
        for d in range(2):
            for s in range(size):
                value = sum_ref[d * count + first + s]
                out_ref[d, :, s * rows:(s + 1) * rows] = value.astype(BF16).T
        first += size


def adjoint(phase, lists, counts, tiles, left, sizes):
    count = sum(sizes)
    slots = lists.shape[1] // counts.shape[1]
    rows, vectors = left.shape[1:]
    block = pl.BlockSpec(memory_space=VMEM)
    size = 2 * count * rows * vectors
    return pl.pallas_call(
        functools.partial(adjoint_kernel, phase, slots, count),
        out_shape=[jax.ShapeDtypeStruct((2, vectors, n * rows), BF16) for n in sizes],
        in_specs=[pl.BlockSpec(memory_space=SMEM)] * 2 + [block] * 2,
        out_specs=[block] * len(sizes),
        scratch_shapes=[VMEM((2 * count, rows, vectors), F32)],
        compiler_params=pltpu.CompilerParams(vmem_limit_bytes=ROOM + 6 * size + 2 * left.size),
        cost_estimate=pl.CostEstimate(flops=8 * 10**9, bytes_accessed=16 * 2**20, transcendentals=0),
        name="adjoint",
    )(lists, counts, tiles, left)


def gram_kernel(
    phase, count, slots, fixed, more, final, lists_ref, counts_ref, tiles_ref, in_ref, left_ref, *rest
):
    whole_sum = not more and phase + 1 == final
    arrivals, (sum_ref, pool_ref, held_ref, high_ref, low_ref, in_sems, sems) = rest[:count], rest[count:]
    steps, rows, vectors = held_ref.shape
    per = steps // 2
    chunks = in_sems.shape[0] // 2
    bunch = per // chunks
    inward = None if more else in_chunks(in_ref, held_ref, in_sems)
    loads = pool_loads(arrivals, pool_ref, sems)
    for copy in loads:
        copy.start()
    ahead = min(2, chunks)
    if more:
        sum_ref[...] = in_ref[...]
    else:
        for i in range(ahead):
            for d in range(2):
                inward(d * chunks + i).start()
        sum_ref[...] = jnp.zeros_like(sum_ref)
    for copy in loads:
        copy.wait()

    def some(step, carry):
        spots = [(d, g, d * per + step * bunch + g) for d in range(2) for g in range(bunch)]

        if not more:
            @pl.when(step + ahead < chunks)
            def _():
                for d in range(2):
                    inward(d * chunks + step + ahead).start()

            for d in range(2):
                inward(d * chunks + step).wait()
        for d, g, block in spots:
            entry = lambda j, block=block: lists_ref[phase, block * slots + j]
            if more:
                held_ref[block] = jnp.zeros_like(held_ref[block])
            for j in range(fixed):
                held_ref[block] += pair(entry, j, tiles_ref.at[d], pool_ref)
        for d, g, block in spots:
            entry = lambda j, block=block: lists_ref[phase, block * slots + j]
            add_rest(
                held_ref.at[block], fixed, counts_ref[phase, block], entry, tiles_ref.at[d], pool_ref
            )
        for d, g, block in spots:
            value = held_ref[block]
            high = value.astype(BF16)
            spot = (pl.ds(g * rows, rows), pl.ds(d * vectors, vectors))
            high_ref[spot] = high
            low = (value - high.astype(F32)).astype(BF16)
            open_block = counts_ref[final, block] > 0 if whole_sum else True
            low_ref[spot] = jnp.where(open_block, low, jnp.zeros_like(low))
        sum_ref[...] += jnp.dot(left_ref[step], high_ref[...], preferred_element_type=F32)
        sum_ref[...] += jnp.dot(left_ref[step], low_ref[...], preferred_element_type=F32)
        return carry

    lax.fori_loop(0, chunks, some, 0)


def gram(phase, lists, counts, tiles, current, left_t, arrivals, fixed):
    steps = counts.shape[1]
    more = current.ndim == 2
    rows, vectors = arrivals[0].shape[1:]
    slots = lists.shape[1] // steps
    chunks, columns, depth = left_t.shape
    cap = arrivals[0].shape[0]
    block = pl.BlockSpec(memory_space=VMEM)
    dma = pltpu.SemaphoreType.DMA
    room = 2 * ROOM + 4 * steps * rows * vectors + sum(2 * a.size for a in arrivals)
    return pl.pallas_call(
        functools.partial(gram_kernel, phase, len(arrivals), slots, fixed, more, counts.shape[0] - 1),
        out_shape=jax.ShapeDtypeStruct((columns, 2 * vectors), F32),
        in_specs=[pl.BlockSpec(memory_space=SMEM)] * 2
        + [block, block if more else pl.BlockSpec(memory_space=HBM), block]
        + [pl.BlockSpec(memory_space=HBM)] * len(arrivals),
        out_specs=block,
        scratch_shapes=[
            VMEM((len(arrivals) * cap, rows, vectors), BF16),
            VMEM((steps, rows, vectors), F32),
            VMEM((depth, 2 * vectors), BF16),
            VMEM((depth, 2 * vectors), BF16),
            dma((2 * chunks,)),
            dma((len(arrivals),)),
        ],
        compiler_params=pltpu.CompilerParams(vmem_limit_bytes=room),
        cost_estimate=pl.CostEstimate(flops=12 * 10**9, bytes_accessed=24 * 2**20, transcendentals=0),
        name="gram",
    )(lists, counts, tiles, current if more else in_hbm(current), in_vmem(left_t), *map(in_hbm, arrivals))


def late_kernel(count, rank_ref, in_ref, adjoint_ref, *rest):
    arrivals, rest = rest[:count], rest[count:]
    outs, (sum_ref, pool_ref, sems) = rest[:-3], rest[-3:]
    blocks, rows, vectors = pool_ref.shape
    loads = pool_loads(arrivals, pool_ref, sems)
    for copy in loads:
        copy.start()
    for copy in loads:
        copy.wait()
    pool = pool_ref[...].reshape(blocks * rows, vectors)
    for d in range(2):
        side = (slice(None), slice(d * vectors, (d + 1) * vectors))
        sum_ref[side] = in_ref[side] + jnp.dot(adjoint_ref[d], pool, preferred_element_type=F32)
    if len(outs) == 1:
        outs[0][...] = sum_ref[...]
        return
    send_ref, keep_ref = outs
    core = rank_ref[0] % 2
    outer, inner, own = send_ref.shape[:3]
    for n in range(outer * inner):
        keep_ref[n // inner, n % inner] = sum_ref[pl.ds(pl.multiple_of((2 * n + core) * own, own), own), :]
        send_ref[n // inner, n % inner] = sum_ref[
            pl.ds(pl.multiple_of((2 * n + 1 - core) * own, own), own), :
        ].astype(send_ref.dtype)


def late(rank, sums, adjoint, arrivals, devices, sent, last):
    columns, both = sums.shape
    own = columns // devices
    cap, rows, vectors = arrivals[0].shape
    block = pl.BlockSpec(memory_space=VMEM)
    if not last or own % 8:
        halves = [VMEM(sums.shape, F32)]
    else:
        half = (devices // 8, 4, own, both)
        halves = [VMEM(half, sent), VMEM(half, F32)]
    return pl.pallas_call(
        functools.partial(late_kernel, len(arrivals)),
        out_shape=halves,
        in_specs=[pl.BlockSpec(memory_space=SMEM), block, block]
        + [pl.BlockSpec(memory_space=HBM)] * len(arrivals),
        out_specs=[block] * len(halves),
        scratch_shapes=[
            VMEM(sums.shape, F32),
            VMEM((len(arrivals) * cap, rows, vectors), BF16),
            pltpu.SemaphoreType.DMA((len(arrivals),)),
        ],
        compiler_params=pltpu.CompilerParams(
            vmem_limit_bytes=2 * ROOM + sum(2 * a.size for a in arrivals)
        ),
        cost_estimate=pl.CostEstimate(flops=4 * 10**9, bytes_accessed=12 * 2**20, transcendentals=0),
        name="late",
    )(rank, in_vmem(sums), in_vmem(adjoint), *map(in_hbm, arrivals))


def split_kernel(width, shift, count, final, scale, rank_ref, keep_ref, *rest):
    arrived, outs = rest[:count], rest[count:]
    mine = (rank_ref[0] >> shift) % width
    if final:
        vectors = outs[0].shape[-1]
        total = keep_ref[...]
        for ref in arrived:
            total = total + ref[...].astype(F32)
        total = total * scale
        for d in range(2):
            outs[0][d] = total[:, d * vectors:(d + 1) * vectors]
        return
    for mask in range(width):
        where = mine ^ mask
        if len(keep_ref.shape) == 4:
            part = keep_ref[:, where]
            for ref in arrived:
                part = part + ref[:, where].astype(F32)
        else:
            part = keep_ref[where]
            for ref in arrived:
                part = part + ref[where].astype(F32)
        outs[mask][...] = part.astype(outs[mask].dtype)


def split(rank, keep, arrived, width, shift, sent):
    part = keep.shape[:-3] + keep.shape[-2:]
    return pl.pallas_call(
        functools.partial(split_kernel, width, shift, len(arrived), False, None),
        out_shape=[VMEM(part, sent if n else F32) for n in range(width)],
        in_specs=[pl.BlockSpec(memory_space=SMEM)] + [pl.BlockSpec(memory_space=VMEM)] * (1 + len(arrived)),
        out_specs=[pl.BlockSpec(memory_space=VMEM)] * width,
        compiler_params=pltpu.CompilerParams(vmem_limit_bytes=ROOM),
    )(rank, *map(in_vmem, (keep, *arrived)))


def finish(rank, keep, arrived, scale):
    own, both = keep.shape
    return pl.pallas_call(
        functools.partial(split_kernel, 1, 0, len(arrived), True, scale),
        out_shape=jax.ShapeDtypeStruct((2, own, both // 2), F32),
        in_specs=[pl.BlockSpec(memory_space=SMEM)] + [pl.BlockSpec(memory_space=VMEM)] * (1 + len(arrived)),
        out_specs=pl.BlockSpec(memory_space=VMEM),
        compiler_params=pltpu.CompilerParams(vmem_limit_bytes=ROOM),
        name="finish",
    )(rank, *map(in_vmem, (keep, *arrived)))


def swap(value, mask, devices):
    return lax.ppermute(value, "rows", [(i, i ^ mask) for i in range(devices)])


def body(left, right, tiles, source_blocks, tile_index, send_blocks):
    block_rows = tiles.shape[-1]
    vectors = right.shape[1]
    local = right.shape[0] // block_rows
    devices = lax.axis_size("rows")
    slots = source_blocks.shape[-1]
    scale = 1.0 / math.sqrt(local * block_rows * devices)
    rank = lax.axis_index("rows").astype(jnp.int32).reshape(1)
    blocks = right.reshape(local, block_rows, vectors)
    order = exchange_order(devices)
    groups = exchange_groups(len(order))
    send = send_blocks.T

    early = min(EARLY, len(order))
    packed = first_pack(rank, send, blocks, order[:early])
    packed += pack(rank, send, blocks, order[early:])
    arrived = []
    for n, mask in enumerate(order):
        arrived.append(swap(packed[n], mask, devices))

    lists, counts = slot_lists(
        rank, send, source_blocks.reshape(2 * local, slots), tile_index.reshape(2 * local, slots),
        local, order, [start for start, _ in groups], tiles.shape[1],
    )
    tiles = jnp.concatenate([tiles, jnp.zeros((2, 1) + tiles.shape[2:], tiles.dtype)], axis=1)
    bunch = math.gcd(local, 8) * block_rows
    left_t = left.reshape(-1, bunch, vectors).transpose(0, 2, 1)
    tiles = in_vmem(tiles)
    sums = hops(lists, counts, tiles, blocks, 4)
    start, stop = groups[-1]
    cut = stop - (stop - start) * 2 // 5
    cap = send.shape[0]
    met = adjoint(
        len(groups), lists, counts, tiles, left.reshape(blocks.shape),
        [(cut - start) * cap, (stop - cut) * cap],
    )
    for n, (first, last) in enumerate(groups[:-1]):
        sums = gram(n + 1, lists, counts, tiles, sums, left_t, arrived[first:last], 3)
    sums, = late(rank, sums, met[0], arrived[start:cut], devices, F32, False)
    sums = late(rank, sums, met[1], arrived[cut:stop], devices, F32, True)
    if len(sums) == 1:
        mine = lax.psum_scatter(sums[0] * scale, "rows", scatter_dimension=0, tiled=True)
        return mine.reshape(mine.shape[0], 2, vectors).transpose(1, 0, 2)
    send, keep = sums
    outer = devices // 8
    got = swap(send, 1, devices)
    parts = split(rank, keep, [got], 4, 1, BF16)
    got = [swap(parts[n], n << 1, devices) for n in range(1, 4)]
    parts = split(rank, parts[0], got, outer, 3, F32)
    got = [swap(parts[n], n << 3, devices) for n in range(1, outer)]
    return finish(rank, parts[0], got, scale)


def solution(mesh):
    placed = (
        P("rows", None),
        P("rows", None),
        P(),
        P(None, "rows", None),
        P(None, "rows", None),
        P("rows", None),
    )

    return jax.shard_map(body, mesh=mesh, in_specs=placed, out_specs=P(None, "rows", None), check_vma=False)
```

```python
import functools
import math

import jax
import jax.numpy as jnp
from jax import lax
from jax.experimental import pallas as pl
from jax.experimental.pallas import tpu as pltpu
from jax.sharding import PartitionSpec as P


F32 = jnp.float32
BF16 = jnp.bfloat16
SHIFT = 1024
ROOM = 8 * 2**20
LATE = 13
MOST = 40
EARLY = 3
SMEM = pltpu.SMEM
VMEM = pltpu.VMEM
HBM = pltpu.HBM


def exchange_order(devices):
    half = devices // 2
    far, near = list(range(half, devices)), list(range(1, half))
    order, far = far[:EARLY], far[EARLY:]
    while far or near:
        order += near[:1] + far[:1]
        near, far = near[1:], far[1:]
    return order


def exchange_groups(count):
    early = count - min(LATE, count // 2)
    parts = -(-early // MOST)
    cuts = [early * n // parts for n in range(parts + 1)]
    return list(zip(cuts, cuts[1:] + [count]))


def in_hbm(value):
    return pltpu.with_memory_space_constraint(value, HBM)


def in_vmem(value):
    return pltpu.with_memory_space_constraint(value, VMEM)


def whole(shape, space=VMEM):
    return pl.BlockSpec(shape, lambda *_: (0,) * len(shape), memory_space=space)


def first_kernel(masks, rank_ref, send_ref, blocks_ref, *rest):
    outs, sems = rest[: len(masks)], rest[len(masks)]
    cap = send_ref.shape[0]
    copies = []
    for n, mask in enumerate(masks):
        for c in range(cap):
            block = jnp.maximum(send_ref[c, rank_ref[0] ^ mask], 0)
            copy = pltpu.make_async_copy(blocks_ref.at[block], outs[n].at[c], sems.at[n * cap + c])
            copy.start()
            copies.append(copy)
    for copy in copies:
        copy.wait()


def first_pack(rank, send, blocks, masks):
    cap = send.shape[0]
    return pl.pallas_call(
        functools.partial(first_kernel, masks),
        out_shape=[VMEM((cap,) + blocks.shape[1:], BF16)] * len(masks),
        in_specs=[pl.BlockSpec(memory_space=SMEM)] * 2 + [pl.BlockSpec(memory_space=HBM)],
        out_specs=[pl.BlockSpec(memory_space=VMEM)] * len(masks),
        scratch_shapes=[pltpu.SemaphoreType.DMA((len(masks) * cap,))],
        compiler_params=pltpu.CompilerParams(vmem_limit_bytes=ROOM),
        name="first_pack",
    )(rank, in_hbm(send), in_hbm(blocks))


def pack_kernel(masks, after, rank_ref, send_ref, blocks_ref, *rest):
    rest = rest[after:]
    outs, (held_ref, in_sems, out_sems) = rest[: len(masks)], rest[len(masks):]
    cap = send_ref.shape[0]
    rank = rank_ref[0]
    inward, outward = [], []
    for n, mask in enumerate(masks):
        for c in range(cap):
            i = n * cap + c
            block = jnp.maximum(send_ref[c, rank ^ mask], 0)
            copy = pltpu.make_async_copy(blocks_ref.at[block], held_ref.at[i], in_sems.at[i])
            copy.start()
            inward.append(copy)
            outward.append(pltpu.make_async_copy(held_ref.at[i], outs[n].at[c], out_sems.at[i]))
    for one, two in zip(inward, outward):
        one.wait()
        two.start()
    for copy in outward:
        copy.wait()


def pack(rank, send, blocks, masks, after=()):
    cap = send.shape[0]
    count = len(masks) * cap
    return pl.pallas_call(
        functools.partial(pack_kernel, masks, len(after)),
        out_shape=[jax.ShapeDtypeStruct((cap,) + blocks.shape[1:], BF16)] * len(masks),
        in_specs=[whole((1,), SMEM), whole(send.shape, SMEM)]
        + [pl.BlockSpec(memory_space=HBM)] * (1 + len(after)),
        out_specs=[pl.BlockSpec(memory_space=HBM)] * len(masks),
        scratch_shapes=[
            VMEM((count,) + blocks.shape[1:], BF16),
            pltpu.SemaphoreType.DMA((count,)),
            pltpu.SemaphoreType.DMA((count,)),
        ],
        compiler_params=pltpu.CompilerParams(vmem_limit_bytes=ROOM + 2 * count * blocks[0].size),
        name="pack",
    )(rank, send, in_hbm(blocks), *after)


def slot_lists(rank, send, source, tile, local, order, starts, spare):
    cap = send.shape[0]
    slots = source.shape[1]
    mine = lax.dynamic_index_in_dim(send, rank[0], 1, keepdims=False)
    away = source >= local
    r = jnp.maximum(source - local, 0)
    c = r % cap
    mask = (r // cap) ^ rank[0]
    spot = jnp.where(
        mask[..., None] == jnp.array(order, jnp.int32), jnp.arange(len(order), dtype=jnp.int32), 0
    ).sum(-1)
    own = source
    for n in range(cap):
        own = jnp.where(away & (c == n), jnp.maximum(mine[n], 0), own)
    phase = jnp.zeros_like(source)
    first = jnp.zeros_like(source)
    far = away & (mask != 0)
    for n, start in enumerate(starts):
        phase = jnp.where(far & (spot >= start), n + 1, phase)
        first = jnp.where(far & (spot >= start), start, first)
    value = tile * SHIFT + jnp.where(far, (spot - first) * cap + c, own)
    phases = jnp.arange(len(starts) + 1, dtype=jnp.int32)[:, None, None]
    hit = (tile >= 0)[None] & (phase[None] == phases)
    k = jnp.arange(slots, dtype=jnp.int32)
    before = (hit[:, :, None, :] & (k[None, :] < k[:, None])).astype(jnp.int32).sum(-1)
    there = hit[:, :, None, :] & (before[:, :, None, :] == k[:, None])
    empty = spare * SHIFT
    lists = jnp.where(there, value[None, :, None, :] - empty, 0).sum(-1) + empty
    return lists.reshape(len(starts) + 1, -1), hit.astype(jnp.int32).sum(-1)


def pair(entry, j, tiles_ref, pool_ref):
    e0, e1 = entry(2 * j), entry(2 * j + 1)
    return jnp.dot(
        jnp.concatenate([tiles_ref[e0 // SHIFT], tiles_ref[e1 // SHIFT]], axis=1),
        jnp.concatenate([pool_ref[e0 % SHIFT], pool_ref[e1 % SHIFT]], axis=0),
        preferred_element_type=F32,
    )


def add_rest(acc_ref, done, count, entry, tiles_ref, pool_ref):
    def one(j, carry):
        acc_ref[...] += pair(entry, j, tiles_ref, pool_ref)
        return carry

    lax.fori_loop(done, (count + 1) // 2, one, 0)


def pool_loads(arrivals, pool_ref, sems):
    cap = arrivals[0].shape[0]
    return [
        pltpu.make_async_copy(ref, pool_ref.at[pl.ds(n * cap, cap)], sems.at[n])
        for n, ref in enumerate(arrivals)
    ]


def in_chunks(from_ref, to_ref, sems):
    size = from_ref.shape[0] // sems.shape[0]
    return lambda i: pltpu.make_async_copy(
        from_ref.at[pl.ds(i * size, size)], to_ref.at[pl.ds(i * size, size)], sems.at[i]
    )


def hops_kernel(slots, fixed, lists_ref, counts_ref, tiles_ref, pool_ref, out_ref, held_ref, out_sems):
    chunks = out_sems.shape[0]
    bunch = held_ref.shape[0] // chunks
    outward = in_chunks(held_ref, out_ref, out_sems)

    def some(step, carry):
        tiles = tiles_ref.at[2 * step // chunks]
        for g in range(bunch):
            block = step * bunch + g
            entry = lambda j, block=block: lists_ref[0, block * slots + j]
            for j in range(fixed):
                value = pair(entry, j, tiles, pool_ref)
                if j:
                    held_ref[block] += value
                else:
                    held_ref[block] = value
        for g in range(bunch):
            block = step * bunch + g
            entry = lambda j, block=block: lists_ref[0, block * slots + j]
            add_rest(held_ref.at[block], fixed, counts_ref[0, block], entry, tiles, pool_ref)
        outward(step).start()
        return carry

    lax.fori_loop(0, chunks, some, 0)
    for i in range(chunks):
        outward(i).wait()


def hops(lists, counts, tiles, pool, fixed, bunch=4):
    steps = counts.shape[1]
    slots = lists.shape[1] // steps
    chunks = steps // math.gcd(bunch, steps // 2)
    rows, vectors = pool.shape[1:]
    block = pl.BlockSpec(memory_space=VMEM)
    return pl.pallas_call(
        functools.partial(hops_kernel, slots, fixed),
        out_shape=HBM((steps, rows, vectors), F32),
        in_specs=[pl.BlockSpec(memory_space=SMEM)] * 2 + [block] * 2,
        out_specs=pl.BlockSpec(memory_space=HBM),
        scratch_shapes=[VMEM((steps, rows, vectors), F32), pltpu.SemaphoreType.DMA((chunks,))],
        compiler_params=pltpu.CompilerParams(
            vmem_limit_bytes=ROOM + 4 * steps * rows * vectors + 2 * pool.size
        ),
        cost_estimate=pl.CostEstimate(flops=8 * 10**9, bytes_accessed=40 * 2**20, transcendentals=0),
        name="hops",
    )(lists, counts, tiles, pool)


def adjoint_kernel(phase, slots, count, lists_ref, counts_ref, tiles_ref, left_ref, *rest):
    outs, sum_ref = rest[:-1], rest[-1]
    local, rows = left_ref.shape[:2]
    for s in range(2 * count):
        sum_ref[s] = jnp.zeros_like(sum_ref[s])

    def one_block(block, carry):
        d = block // local
        tiles = tiles_ref.at[d]

        def two(j, carry):
            e0 = lists_ref[phase, block * slots + 2 * j]
            e1 = lists_ref[phase, block * slots + 2 * j + 1]
            value = lax.dot_general(
                jnp.concatenate([tiles[e0 // SHIFT], tiles[e1 // SHIFT]], axis=1),
                left_ref[block % local], (((0,), (0,)), ((), ())), preferred_element_type=F32,
            )
            sum_ref[d * count + e0 % SHIFT] += value[:rows]
            sum_ref[d * count + e1 % SHIFT] += value[rows:]
            return carry

        return lax.fori_loop(0, (counts_ref[phase, block] + 1) // 2, two, carry)

    lax.fori_loop(0, 2 * local, one_block, 0)
    first = 0
    for out_ref in outs:
        size = out_ref.shape[2] // rows
        for d in range(2):
            for s in range(size):
                value = sum_ref[d * count + first + s]
                out_ref[d, :, s * rows:(s + 1) * rows] = value.astype(BF16).T
        first += size


def adjoint(phase, lists, counts, tiles, left, sizes):
    count = sum(sizes)
    slots = lists.shape[1] // counts.shape[1]
    rows, vectors = left.shape[1:]
    block = pl.BlockSpec(memory_space=VMEM)
    size = 2 * count * rows * vectors
    return pl.pallas_call(
        functools.partial(adjoint_kernel, phase, slots, count),
        out_shape=[jax.ShapeDtypeStruct((2, vectors, n * rows), BF16) for n in sizes],
        in_specs=[pl.BlockSpec(memory_space=SMEM)] * 2 + [block] * 2,
        out_specs=[block] * len(sizes),
        scratch_shapes=[VMEM((2 * count, rows, vectors), F32)],
        compiler_params=pltpu.CompilerParams(vmem_limit_bytes=ROOM + 6 * size + 2 * left.size),
        cost_estimate=pl.CostEstimate(flops=8 * 10**9, bytes_accessed=16 * 2**20, transcendentals=0),
        name="adjoint",
    )(lists, counts, tiles, left)


def gram_kernel(
    phase, count, slots, fixed, more, final, lists_ref, counts_ref, tiles_ref, in_ref, left_ref, *rest
):
    whole_sum = not more and phase + 1 == final
    arrivals, (sum_ref, pool_ref, held_ref, high_ref, low_ref, in_sems, sems) = rest[:count], rest[count:]
    steps, rows, vectors = held_ref.shape
    per = steps // 2
    chunks = in_sems.shape[0] // 2
    bunch = per // chunks
    inward = None if more else in_chunks(in_ref, held_ref, in_sems)
    loads = pool_loads(arrivals, pool_ref, sems)
    for copy in loads:
        copy.start()
    ahead = min(2, chunks)
    if more:
        sum_ref[...] = in_ref[...]
    else:
        for i in range(ahead):
            for d in range(2):
                inward(d * chunks + i).start()
        sum_ref[...] = jnp.zeros_like(sum_ref)
    for copy in loads:
        copy.wait()

    def some(step, carry):
        spots = [(d, g, d * per + step * bunch + g) for d in range(2) for g in range(bunch)]

        if not more:
            @pl.when(step + ahead < chunks)
            def _():
                for d in range(2):
                    inward(d * chunks + step + ahead).start()

            for d in range(2):
                inward(d * chunks + step).wait()
        for d, g, block in spots:
            entry = lambda j, block=block: lists_ref[phase, block * slots + j]
            if more:
                held_ref[block] = jnp.zeros_like(held_ref[block])
            for j in range(fixed):
                held_ref[block] += pair(entry, j, tiles_ref.at[d], pool_ref)
        for d, g, block in spots:
            entry = lambda j, block=block: lists_ref[phase, block * slots + j]
            add_rest(
                held_ref.at[block], fixed, counts_ref[phase, block], entry, tiles_ref.at[d], pool_ref
            )
        for d, g, block in spots:
            value = held_ref[block]
            high = value.astype(BF16)
            spot = (pl.ds(g * rows, rows), pl.ds(d * vectors, vectors))
            high_ref[spot] = high
            low = (value - high.astype(F32)).astype(BF16)
            open_block = counts_ref[final, block] > 0 if whole_sum else True
            low_ref[spot] = jnp.where(open_block, low, jnp.zeros_like(low))
        sum_ref[...] += jnp.dot(left_ref[step], high_ref[...], preferred_element_type=F32)
        sum_ref[...] += jnp.dot(left_ref[step], low_ref[...], preferred_element_type=F32)
        return carry

    lax.fori_loop(0, chunks, some, 0)


def gram(phase, lists, counts, tiles, current, left_t, arrivals, fixed):
    steps = counts.shape[1]
    more = current.ndim == 2
    rows, vectors = arrivals[0].shape[1:]
    slots = lists.shape[1] // steps
    chunks, columns, depth = left_t.shape
    cap = arrivals[0].shape[0]
    block = pl.BlockSpec(memory_space=VMEM)
    dma = pltpu.SemaphoreType.DMA
    room = 2 * ROOM + 4 * steps * rows * vectors + sum(2 * a.size for a in arrivals)
    return pl.pallas_call(
        functools.partial(gram_kernel, phase, len(arrivals), slots, fixed, more, counts.shape[0] - 1),
        out_shape=jax.ShapeDtypeStruct((columns, 2 * vectors), F32),
        in_specs=[pl.BlockSpec(memory_space=SMEM)] * 2
        + [block, block if more else pl.BlockSpec(memory_space=HBM), block]
        + [pl.BlockSpec(memory_space=HBM)] * len(arrivals),
        out_specs=block,
        scratch_shapes=[
            VMEM((len(arrivals) * cap, rows, vectors), BF16),
            VMEM((steps, rows, vectors), F32),
            VMEM((depth, 2 * vectors), BF16),
            VMEM((depth, 2 * vectors), BF16),
            dma((2 * chunks,)),
            dma((len(arrivals),)),
        ],
        compiler_params=pltpu.CompilerParams(vmem_limit_bytes=room),
        cost_estimate=pl.CostEstimate(flops=12 * 10**9, bytes_accessed=24 * 2**20, transcendentals=0),
        name="gram",
    )(lists, counts, tiles, current if more else in_hbm(current), in_vmem(left_t), *map(in_hbm, arrivals))


def late_kernel(count, rank_ref, in_ref, adjoint_ref, *rest):
    arrivals, rest = rest[:count], rest[count:]
    outs, (sum_ref, pool_ref, sems) = rest[:-3], rest[-3:]
    blocks, rows, vectors = pool_ref.shape
    loads = pool_loads(arrivals, pool_ref, sems)
    for copy in loads:
        copy.start()
    for copy in loads:
        copy.wait()
    pool = pool_ref[...].reshape(blocks * rows, vectors)
    for d in range(2):
        side = (slice(None), slice(d * vectors, (d + 1) * vectors))
        sum_ref[side] = in_ref[side] + jnp.dot(adjoint_ref[d], pool, preferred_element_type=F32)
    if len(outs) == 1:
        outs[0][...] = sum_ref[...]
        return
    send_ref, keep_ref = outs
    core = rank_ref[0] % 2
    outer, inner, own = send_ref.shape[:3]
    for n in range(outer * inner):
        keep_ref[n // inner, n % inner] = sum_ref[pl.ds(pl.multiple_of((2 * n + core) * own, own), own), :]
        send_ref[n // inner, n % inner] = sum_ref[
            pl.ds(pl.multiple_of((2 * n + 1 - core) * own, own), own), :
        ].astype(send_ref.dtype)


def late(rank, sums, adjoint, arrivals, devices, sent, last):
    columns, both = sums.shape
    own = columns // devices
    cap, rows, vectors = arrivals[0].shape
    block = pl.BlockSpec(memory_space=VMEM)
    if not last or own % 8:
        halves = [VMEM(sums.shape, F32)]
    else:
        half = (devices // 8, 4, own, both)
        halves = [VMEM(half, sent), VMEM(half, F32)]
    return pl.pallas_call(
        functools.partial(late_kernel, len(arrivals)),
        out_shape=halves,
        in_specs=[pl.BlockSpec(memory_space=SMEM), block, block]
        + [pl.BlockSpec(memory_space=HBM)] * len(arrivals),
        out_specs=[block] * len(halves),
        scratch_shapes=[
            VMEM(sums.shape, F32),
            VMEM((len(arrivals) * cap, rows, vectors), BF16),
            pltpu.SemaphoreType.DMA((len(arrivals),)),
        ],
        compiler_params=pltpu.CompilerParams(
            vmem_limit_bytes=2 * ROOM + sum(2 * a.size for a in arrivals)
        ),
        cost_estimate=pl.CostEstimate(flops=4 * 10**9, bytes_accessed=12 * 2**20, transcendentals=0),
        name="late",
    )(rank, in_vmem(sums), in_vmem(adjoint), *map(in_hbm, arrivals))


def split_kernel(width, shift, count, final, scale, rank_ref, keep_ref, *rest):
    arrived, outs = rest[:count], rest[count:]
    mine = (rank_ref[0] >> shift) % width
    if final:
        vectors = outs[0].shape[-1]
        total = keep_ref[...]
        for ref in arrived:
            total = total + ref[...].astype(F32)
        total = total * scale
        for d in range(2):
            outs[0][d] = total[:, d * vectors:(d + 1) * vectors]
        return
    for mask in range(width):
        where = mine ^ mask
        if len(keep_ref.shape) == 4:
            part = keep_ref[:, where]
            for ref in arrived:
                part = part + ref[:, where].astype(F32)
        else:
            part = keep_ref[where]
            for ref in arrived:
                part = part + ref[where].astype(F32)
        outs[mask][...] = part.astype(outs[mask].dtype)


def split(rank, keep, arrived, width, shift, sent):
    part = keep.shape[:-3] + keep.shape[-2:]
    return pl.pallas_call(
        functools.partial(split_kernel, width, shift, len(arrived), False, None),
        out_shape=[VMEM(part, sent if n else F32) for n in range(width)],
        in_specs=[pl.BlockSpec(memory_space=SMEM)] + [pl.BlockSpec(memory_space=VMEM)] * (1 + len(arrived)),
        out_specs=[pl.BlockSpec(memory_space=VMEM)] * width,
        compiler_params=pltpu.CompilerParams(vmem_limit_bytes=ROOM),
    )(rank, *map(in_vmem, (keep, *arrived)))


def finish(rank, keep, arrived, scale):
    own, both = keep.shape
    return pl.pallas_call(
        functools.partial(split_kernel, 1, 0, len(arrived), True, scale),
        out_shape=jax.ShapeDtypeStruct((2, own, both // 2), F32),
        in_specs=[pl.BlockSpec(memory_space=SMEM)] + [pl.BlockSpec(memory_space=VMEM)] * (1 + len(arrived)),
        out_specs=pl.BlockSpec(memory_space=VMEM),
        compiler_params=pltpu.CompilerParams(vmem_limit_bytes=ROOM),
        name="finish",
    )(rank, *map(in_vmem, (keep, *arrived)))


def swap(value, mask, devices):
    return lax.ppermute(value, "rows", [(i, i ^ mask) for i in range(devices)])


def body(left, right, tiles, source_blocks, tile_index, send_blocks):
    block_rows = tiles.shape[-1]
    vectors = right.shape[1]
    local = right.shape[0] // block_rows
    devices = lax.axis_size("rows")
    slots = source_blocks.shape[-1]
    scale = 1.0 / math.sqrt(local * block_rows * devices)
    rank = lax.axis_index("rows").astype(jnp.int32).reshape(1)
    blocks = right.reshape(local, block_rows, vectors)
    order = exchange_order(devices)
    groups = exchange_groups(len(order))
    send = send_blocks.T

    early = min(EARLY, len(order))
    packed = first_pack(rank, send, blocks, order[:early])
    packed += pack(rank, send, blocks, order[early:])
    arrived = []
    for n, mask in enumerate(order):
        arrived.append(swap(packed[n], mask, devices))

    lists, counts = slot_lists(
        rank, send, source_blocks.reshape(2 * local, slots), tile_index.reshape(2 * local, slots),
        local, order, [start for start, _ in groups], tiles.shape[1],
    )
    tiles = jnp.concatenate([tiles, jnp.zeros((2, 1) + tiles.shape[2:], tiles.dtype)], axis=1)
    bunch = math.gcd(local, 8) * block_rows
    left_t = left.reshape(-1, bunch, vectors).transpose(0, 2, 1)
    tiles = in_vmem(tiles)
    sums = hops(lists, counts, tiles, blocks, 4)
    start, stop = groups[-1]
    cut = stop - (stop - start) * 2 // 5
    cap = send.shape[0]
    met = adjoint(
        len(groups), lists, counts, tiles, left.reshape(blocks.shape),
        [(cut - start) * cap, (stop - cut) * cap],
    )
    for n, (first, last) in enumerate(groups[:-1]):
        sums = gram(n + 1, lists, counts, tiles, sums, left_t, arrived[first:last], 3)
    sums, = late(rank, sums, met[0], arrived[start:cut], devices, F32, False)
    sums = late(rank, sums, met[1], arrived[cut:stop], devices, F32, True)
    if len(sums) == 1:
        mine = lax.psum_scatter(sums[0] * scale, "rows", scatter_dimension=0, tiled=True)
        return mine.reshape(mine.shape[0], 2, vectors).transpose(1, 0, 2)
    send, keep = sums
    outer = devices // 8
    got = swap(send, 1, devices)
    parts = split(rank, keep, [got], 4, 1, BF16)
    got = [swap(parts[n], n << 1, devices) for n in (3, 1, 2)]
    parts = split(rank, parts[0], got, outer, 3, F32)
    far_first = sorted(range(1, outer), key=lambda n: (n < outer // 2, n))
    got = [swap(parts[n], n << 3, devices) for n in far_first]
    return finish(rank, parts[0], got, scale)


def solution(mesh):
    placed = (
        P("rows", None),
        P("rows", None),
        P(),
        P(None, "rows", None),
        P(None, "rows", None),
        P("rows", None),
    )

    return jax.shard_map(body, mesh=mesh, in_specs=placed, out_specs=P(None, "rows", None), check_vma=False)
```

```python
import functools
import math

import jax
import jax.numpy as jnp
from jax import lax
from jax.experimental import pallas as pl
from jax.experimental.pallas import tpu as pltpu
from jax.sharding import PartitionSpec as P


F32 = jnp.float32
BF16 = jnp.bfloat16
SHIFT = 1024
ROOM = 8 * 2**20
LATE = 13
MOST = 40
EARLY = 3
SMEM = pltpu.SMEM
VMEM = pltpu.VMEM
HBM = pltpu.HBM


def exchange_order(devices):
    half = devices // 2
    far, near = list(range(half, devices)), list(range(1, half))
    order, far = far[:EARLY], far[EARLY:]
    while far or near:
        order += near[:1] + far[:1]
        near, far = near[1:], far[1:]
    return order


def exchange_groups(count):
    early = count - min(LATE, count // 2)
    parts = -(-early // MOST)
    cuts = [early * n // parts for n in range(parts + 1)]
    return list(zip(cuts, cuts[1:] + [count]))


def in_hbm(value):
    return pltpu.with_memory_space_constraint(value, HBM)


def in_vmem(value):
    return pltpu.with_memory_space_constraint(value, VMEM)


def whole(shape, space=VMEM):
    return pl.BlockSpec(shape, lambda *_: (0,) * len(shape), memory_space=space)


def first_kernel(masks, rank_ref, send_ref, blocks_ref, *rest):
    outs, sems = rest[: len(masks)], rest[len(masks)]
    cap = send_ref.shape[0]
    copies = []
    for n, mask in enumerate(masks):
        for c in range(cap):
            block = jnp.maximum(send_ref[c, rank_ref[0] ^ mask], 0)
            copy = pltpu.make_async_copy(blocks_ref.at[block], outs[n].at[c], sems.at[n * cap + c])
            copy.start()
            copies.append(copy)
    for copy in copies:
        copy.wait()


def first_pack(rank, send, blocks, masks):
    cap = send.shape[0]
    return pl.pallas_call(
        functools.partial(first_kernel, masks),
        out_shape=[VMEM((cap,) + blocks.shape[1:], BF16)] * len(masks),
        in_specs=[pl.BlockSpec(memory_space=SMEM)] * 2 + [pl.BlockSpec(memory_space=HBM)],
        out_specs=[pl.BlockSpec(memory_space=VMEM)] * len(masks),
        scratch_shapes=[pltpu.SemaphoreType.DMA((len(masks) * cap,))],
        compiler_params=pltpu.CompilerParams(vmem_limit_bytes=ROOM),
        name="first_pack",
    )(rank, in_hbm(send), in_hbm(blocks))


def pack_kernel(masks, after, rank_ref, send_ref, blocks_ref, *rest):
    rest = rest[after:]
    outs, (held_ref, in_sems, out_sems) = rest[: len(masks)], rest[len(masks):]
    cap = send_ref.shape[0]
    rank = rank_ref[0]
    inward, outward = [], []
    for n, mask in enumerate(masks):
        for c in range(cap):
            i = n * cap + c
            block = jnp.maximum(send_ref[c, rank ^ mask], 0)
            copy = pltpu.make_async_copy(blocks_ref.at[block], held_ref.at[i], in_sems.at[i])
            copy.start()
            inward.append(copy)
            outward.append(pltpu.make_async_copy(held_ref.at[i], outs[n].at[c], out_sems.at[i]))
    for one, two in zip(inward, outward):
        one.wait()
        two.start()
    for copy in outward:
        copy.wait()


def pack(rank, send, blocks, masks, after=()):
    cap = send.shape[0]
    count = len(masks) * cap
    return pl.pallas_call(
        functools.partial(pack_kernel, masks, len(after)),
        out_shape=[jax.ShapeDtypeStruct((cap,) + blocks.shape[1:], BF16)] * len(masks),
        in_specs=[whole((1,), SMEM), whole(send.shape, SMEM)]
        + [pl.BlockSpec(memory_space=HBM)] * (1 + len(after)),
        out_specs=[pl.BlockSpec(memory_space=HBM)] * len(masks),
        scratch_shapes=[
            VMEM((count,) + blocks.shape[1:], BF16),
            pltpu.SemaphoreType.DMA((count,)),
            pltpu.SemaphoreType.DMA((count,)),
        ],
        compiler_params=pltpu.CompilerParams(vmem_limit_bytes=ROOM + 2 * count * blocks[0].size),
        name="pack",
    )(rank, send, in_hbm(blocks), *after)


def slot_lists(rank, send, source, tile, local, order, starts, spare):
    cap = send.shape[0]
    slots = source.shape[1]
    mine = lax.dynamic_index_in_dim(send, rank[0], 1, keepdims=False)
    away = source >= local
    r = jnp.maximum(source - local, 0)
    c = r % cap
    mask = (r // cap) ^ rank[0]
    spot = jnp.where(
        mask[..., None] == jnp.array(order, jnp.int32), jnp.arange(len(order), dtype=jnp.int32), 0
    ).sum(-1)
    own = source
    for n in range(cap):
        own = jnp.where(away & (c == n), jnp.maximum(mine[n], 0), own)
    phase = jnp.zeros_like(source)
    first = jnp.zeros_like(source)
    far = away & (mask != 0)
    for n, start in enumerate(starts):
        phase = jnp.where(far & (spot >= start), n + 1, phase)
        first = jnp.where(far & (spot >= start), start, first)
    value = tile * SHIFT + jnp.where(far, (spot - first) * cap + c, own)
    phases = jnp.arange(len(starts) + 1, dtype=jnp.int32)[:, None, None]
    hit = (tile >= 0)[None] & (phase[None] == phases)
    k = jnp.arange(slots, dtype=jnp.int32)
    before = (hit[:, :, None, :] & (k[None, :] < k[:, None])).astype(jnp.int32).sum(-1)
    there = hit[:, :, None, :] & (before[:, :, None, :] == k[:, None])
    empty = spare * SHIFT
    lists = jnp.where(there, value[None, :, None, :] - empty, 0).sum(-1) + empty
    return lists.reshape(len(starts) + 1, -1), hit.astype(jnp.int32).sum(-1)


def pair(entry, j, tiles_ref, pool_ref):
    e0, e1 = entry(2 * j), entry(2 * j + 1)
    return jnp.dot(
        jnp.concatenate([tiles_ref[e0 // SHIFT], tiles_ref[e1 // SHIFT]], axis=1),
        jnp.concatenate([pool_ref[e0 % SHIFT], pool_ref[e1 % SHIFT]], axis=0),
        preferred_element_type=F32,
    )


def add_rest(acc_ref, done, count, entry, tiles_ref, pool_ref):
    def one(j, carry):
        acc_ref[...] += pair(entry, j, tiles_ref, pool_ref)
        return carry

    lax.fori_loop(done, (count + 1) // 2, one, 0)


def pool_loads(arrivals, pool_ref, sems):
    cap = arrivals[0].shape[0]
    return [
        pltpu.make_async_copy(ref, pool_ref.at[pl.ds(n * cap, cap)], sems.at[n])
        for n, ref in enumerate(arrivals)
    ]


def in_chunks(from_ref, to_ref, sems):
    size = from_ref.shape[0] // sems.shape[0]
    return lambda i: pltpu.make_async_copy(
        from_ref.at[pl.ds(i * size, size)], to_ref.at[pl.ds(i * size, size)], sems.at[i]
    )


def hops_kernel(slots, fixed, lists_ref, counts_ref, tiles_ref, pool_ref, out_ref, held_ref, out_sems):
    chunks = out_sems.shape[0]
    bunch = held_ref.shape[0] // chunks
    outward = in_chunks(held_ref, out_ref, out_sems)

    def some(step, carry):
        tiles = tiles_ref.at[2 * step // chunks]
        for g in range(bunch):
            block = step * bunch + g
            entry = lambda j, block=block: lists_ref[0, block * slots + j]
            for j in range(fixed):
                value = pair(entry, j, tiles, pool_ref)
                if j:
                    held_ref[block] += value
                else:
                    held_ref[block] = value
        for g in range(bunch):
            block = step * bunch + g
            entry = lambda j, block=block: lists_ref[0, block * slots + j]
            add_rest(held_ref.at[block], fixed, counts_ref[0, block], entry, tiles, pool_ref)
        outward(step).start()
        return carry

    lax.fori_loop(0, chunks, some, 0)
    for i in range(chunks):
        outward(i).wait()


def hops(lists, counts, tiles, pool, fixed, bunch=4):
    steps = counts.shape[1]
    slots = lists.shape[1] // steps
    chunks = steps // math.gcd(bunch, steps // 2)
    rows, vectors = pool.shape[1:]
    block = pl.BlockSpec(memory_space=VMEM)
    return pl.pallas_call(
        functools.partial(hops_kernel, slots, fixed),
        out_shape=HBM((steps, rows, vectors), F32),
        in_specs=[pl.BlockSpec(memory_space=SMEM)] * 2 + [block] * 2,
        out_specs=pl.BlockSpec(memory_space=HBM),
        scratch_shapes=[VMEM((steps, rows, vectors), F32), pltpu.SemaphoreType.DMA((chunks,))],
        compiler_params=pltpu.CompilerParams(
            vmem_limit_bytes=ROOM + 4 * steps * rows * vectors + 2 * pool.size
        ),
        cost_estimate=pl.CostEstimate(flops=8 * 10**9, bytes_accessed=40 * 2**20, transcendentals=0),
        name="hops",
    )(lists, counts, tiles, pool)


def adjoint_kernel(phase, slots, count, lists_ref, counts_ref, tiles_ref, left_ref, *rest):
    outs, sum_ref = rest[:-1], rest[-1]
    local, rows = left_ref.shape[:2]
    for s in range(2 * count):
        sum_ref[s] = jnp.zeros_like(sum_ref[s])

    def one_block(block, carry):
        d = block // local
        tiles = tiles_ref.at[d]

        def two(j, carry):
            e0 = lists_ref[phase, block * slots + 2 * j]
            e1 = lists_ref[phase, block * slots + 2 * j + 1]
            value = lax.dot_general(
                jnp.concatenate([tiles[e0 // SHIFT], tiles[e1 // SHIFT]], axis=1),
                left_ref[block % local], (((0,), (0,)), ((), ())), preferred_element_type=F32,
            )
            sum_ref[d * count + e0 % SHIFT] += value[:rows]
            sum_ref[d * count + e1 % SHIFT] += value[rows:]
            return carry

        return lax.fori_loop(0, (counts_ref[phase, block] + 1) // 2, two, carry)

    lax.fori_loop(0, 2 * local, one_block, 0)
    first = 0
    for out_ref in outs:
        size = out_ref.shape[2] // rows
        for d in range(2):
            for s in range(size):
                value = sum_ref[d * count + first + s]
                out_ref[d, :, s * rows:(s + 1) * rows] = value.astype(BF16).T
        first += size


def adjoint(phase, lists, counts, tiles, left, sizes):
    count = sum(sizes)
    slots = lists.shape[1] // counts.shape[1]
    rows, vectors = left.shape[1:]
    block = pl.BlockSpec(memory_space=VMEM)
    size = 2 * count * rows * vectors
    return pl.pallas_call(
        functools.partial(adjoint_kernel, phase, slots, count),
        out_shape=[jax.ShapeDtypeStruct((2, vectors, n * rows), BF16) for n in sizes],
        in_specs=[pl.BlockSpec(memory_space=SMEM)] * 2 + [block] * 2,
        out_specs=[block] * len(sizes),
        scratch_shapes=[VMEM((2 * count, rows, vectors), F32)],
        compiler_params=pltpu.CompilerParams(vmem_limit_bytes=ROOM + 6 * size + 2 * left.size),
        cost_estimate=pl.CostEstimate(flops=8 * 10**9, bytes_accessed=16 * 2**20, transcendentals=0),
        name="adjoint",
    )(lists, counts, tiles, left)


def gram_kernel(
    phase, count, slots, fixed, more, final, lists_ref, counts_ref, tiles_ref, in_ref, left_ref, *rest
):
    whole_sum = not more and phase + 1 == final
    arrivals, (sum_ref, pool_ref, held_ref, high_ref, low_ref, in_sems, sems) = rest[:count], rest[count:]
    steps, rows, vectors = held_ref.shape
    per = steps // 2
    chunks = in_sems.shape[0] // 2
    bunch = per // chunks
    inward = None if more else in_chunks(in_ref, held_ref, in_sems)
    loads = pool_loads(arrivals, pool_ref, sems)
    for copy in loads:
        copy.start()
    ahead = min(2, chunks)
    if more:
        sum_ref[...] = in_ref[...]
    else:
        for i in range(ahead):
            for d in range(2):
                inward(d * chunks + i).start()
        sum_ref[...] = jnp.zeros_like(sum_ref)
    for copy in loads:
        copy.wait()

    def some(step, carry):
        spots = [(d, g, d * per + step * bunch + g) for d in range(2) for g in range(bunch)]

        if not more:
            @pl.when(step + ahead < chunks)
            def _():
                for d in range(2):
                    inward(d * chunks + step + ahead).start()

            for d in range(2):
                inward(d * chunks + step).wait()
        for d, g, block in spots:
            entry = lambda j, block=block: lists_ref[phase, block * slots + j]
            if more:
                held_ref[block] = jnp.zeros_like(held_ref[block])
            for j in range(fixed):
                held_ref[block] += pair(entry, j, tiles_ref.at[d], pool_ref)
        for d, g, block in spots:
            entry = lambda j, block=block: lists_ref[phase, block * slots + j]
            add_rest(
                held_ref.at[block], fixed, counts_ref[phase, block], entry, tiles_ref.at[d], pool_ref
            )
        for d, g, block in spots:
            value = held_ref[block]
            high = value.astype(BF16)
            spot = (pl.ds(g * rows, rows), pl.ds(d * vectors, vectors))
            high_ref[spot] = high
            low = (value - high.astype(F32)).astype(BF16)
            open_block = counts_ref[final, block] > 0 if whole_sum else True
            low_ref[spot] = jnp.where(open_block, low, jnp.zeros_like(low))
        sum_ref[...] += jnp.dot(left_ref[step], high_ref[...], preferred_element_type=F32)
        sum_ref[...] += jnp.dot(left_ref[step], low_ref[...], preferred_element_type=F32)
        return carry

    lax.fori_loop(0, chunks, some, 0)


def gram(phase, lists, counts, tiles, current, left_t, arrivals, fixed):
    steps = counts.shape[1]
    more = current.ndim == 2
    rows, vectors = arrivals[0].shape[1:]
    slots = lists.shape[1] // steps
    chunks, columns, depth = left_t.shape
    cap = arrivals[0].shape[0]
    block = pl.BlockSpec(memory_space=VMEM)
    dma = pltpu.SemaphoreType.DMA
    room = 2 * ROOM + 4 * steps * rows * vectors + sum(2 * a.size for a in arrivals)
    return pl.pallas_call(
        functools.partial(gram_kernel, phase, len(arrivals), slots, fixed, more, counts.shape[0] - 1),
        out_shape=jax.ShapeDtypeStruct((columns, 2 * vectors), F32),
        in_specs=[pl.BlockSpec(memory_space=SMEM)] * 2
        + [block, block if more else pl.BlockSpec(memory_space=HBM), block]
        + [pl.BlockSpec(memory_space=HBM)] * len(arrivals),
        out_specs=block,
        scratch_shapes=[
            VMEM((len(arrivals) * cap, rows, vectors), BF16),
            VMEM((steps, rows, vectors), F32),
            VMEM((depth, 2 * vectors), BF16),
            VMEM((depth, 2 * vectors), BF16),
            dma((2 * chunks,)),
            dma((len(arrivals),)),
        ],
        compiler_params=pltpu.CompilerParams(vmem_limit_bytes=room),
        cost_estimate=pl.CostEstimate(flops=12 * 10**9, bytes_accessed=24 * 2**20, transcendentals=0),
        name="gram",
    )(lists, counts, tiles, current if more else in_hbm(current), in_vmem(left_t), *map(in_hbm, arrivals))


def late_kernel(count, rank_ref, in_ref, adjoint_ref, *rest):
    arrivals, rest = rest[:count], rest[count:]
    outs, sum_ref = rest[:-1], rest[-1]
    vectors = arrivals[0].shape[2]
    pool = jnp.concatenate([ref[...].reshape(-1, vectors) for ref in arrivals], axis=0)
    for d in range(2):
        side = (slice(None), slice(d * vectors, (d + 1) * vectors))
        sum_ref[side] = in_ref[side] + jnp.dot(adjoint_ref[d], pool, preferred_element_type=F32)
    if len(outs) == 1:
        outs[0][...] = sum_ref[...]
        return
    send_ref, keep_ref = outs
    core = rank_ref[0] % 2
    outer, inner, own = send_ref.shape[:3]
    for n in range(outer * inner):
        keep_ref[n // inner, n % inner] = sum_ref[pl.ds(pl.multiple_of((2 * n + core) * own, own), own), :]
        send_ref[n // inner, n % inner] = sum_ref[
            pl.ds(pl.multiple_of((2 * n + 1 - core) * own, own), own), :
        ].astype(send_ref.dtype)


def late(rank, sums, adjoint, arrivals, devices, sent, last):
    columns, both = sums.shape
    own = columns // devices
    block = pl.BlockSpec(memory_space=VMEM)
    if not last or own % 8:
        halves = [VMEM(sums.shape, F32)]
    else:
        half = (devices // 8, 4, own, both)
        halves = [VMEM(half, sent), VMEM(half, F32)]
    return pl.pallas_call(
        functools.partial(late_kernel, len(arrivals)),
        out_shape=halves,
        in_specs=[pl.BlockSpec(memory_space=SMEM)] + [block] * (2 + len(arrivals)),
        out_specs=[block] * len(halves),
        scratch_shapes=[VMEM(sums.shape, F32)],
        compiler_params=pltpu.CompilerParams(vmem_limit_bytes=2 * ROOM),
        cost_estimate=pl.CostEstimate(flops=4 * 10**9, bytes_accessed=12 * 2**20, transcendentals=0),
        name="late",
    )(rank, *map(in_vmem, (sums, adjoint, *arrivals)))


def split_kernel(width, shift, count, final, scale, rank_ref, keep_ref, *rest):
    arrived, outs = rest[:count], rest[count:]
    mine = (rank_ref[0] >> shift) % width
    if final:
        vectors = outs[0].shape[-1]
        total = keep_ref[...]
        for ref in arrived:
            total = total + ref[...].astype(F32)
        total = total * scale
        for d in range(2):
            outs[0][d] = total[:, d * vectors:(d + 1) * vectors]
        return
    for mask in range(width):
        where = mine ^ mask
        if len(keep_ref.shape) == 4:
            part = keep_ref[:, where]
            for ref in arrived:
                part = part + ref[:, where].astype(F32)
        else:
            part = keep_ref[where]
            for ref in arrived:
                part = part + ref[where].astype(F32)
        outs[mask][...] = part.astype(outs[mask].dtype)


def split(rank, keep, arrived, width, shift, sent):
    part = keep.shape[:-3] + keep.shape[-2:]
    return pl.pallas_call(
        functools.partial(split_kernel, width, shift, len(arrived), False, None),
        out_shape=[VMEM(part, sent if n else F32) for n in range(width)],
        in_specs=[pl.BlockSpec(memory_space=SMEM)] + [pl.BlockSpec(memory_space=VMEM)] * (1 + len(arrived)),
        out_specs=[pl.BlockSpec(memory_space=VMEM)] * width,
        compiler_params=pltpu.CompilerParams(vmem_limit_bytes=ROOM),
    )(rank, *map(in_vmem, (keep, *arrived)))


def finish(rank, keep, arrived, scale):
    own, both = keep.shape
    return pl.pallas_call(
        functools.partial(split_kernel, 1, 0, len(arrived), True, scale),
        out_shape=jax.ShapeDtypeStruct((2, own, both // 2), F32),
        in_specs=[pl.BlockSpec(memory_space=SMEM)] + [pl.BlockSpec(memory_space=VMEM)] * (1 + len(arrived)),
        out_specs=pl.BlockSpec(memory_space=VMEM),
        compiler_params=pltpu.CompilerParams(vmem_limit_bytes=ROOM),
        name="finish",
    )(rank, *map(in_vmem, (keep, *arrived)))


def swap(value, mask, devices):
    return lax.ppermute(value, "rows", [(i, i ^ mask) for i in range(devices)])


def body(left, right, tiles, source_blocks, tile_index, send_blocks):
    block_rows = tiles.shape[-1]
    vectors = right.shape[1]
    local = right.shape[0] // block_rows
    devices = lax.axis_size("rows")
    slots = source_blocks.shape[-1]
    scale = 1.0 / math.sqrt(local * block_rows * devices)
    rank = lax.axis_index("rows").astype(jnp.int32).reshape(1)
    blocks = right.reshape(local, block_rows, vectors)
    order = exchange_order(devices)
    groups = exchange_groups(len(order))
    send = send_blocks.T

    early = min(EARLY, len(order))
    packed = first_pack(rank, send, blocks, order[:early])
    packed += pack(rank, send, blocks, order[early:])
    arrived = []
    for n, mask in enumerate(order):
        arrived.append(swap(packed[n], mask, devices))

    lists, counts = slot_lists(
        rank, send, source_blocks.reshape(2 * local, slots), tile_index.reshape(2 * local, slots),
        local, order, [start for start, _ in groups], tiles.shape[1],
    )
    tiles = jnp.concatenate([tiles, jnp.zeros((2, 1) + tiles.shape[2:], tiles.dtype)], axis=1)
    bunch = math.gcd(local, 8) * block_rows
    left_t = left.reshape(-1, bunch, vectors).transpose(0, 2, 1)
    tiles = in_vmem(tiles)
    sums = hops(lists, counts, tiles, blocks, 4)
    start, stop = groups[-1]
    cut = stop - (stop - start) * 2 // 5
    cap = send.shape[0]
    met = adjoint(
        len(groups), lists, counts, tiles, left.reshape(blocks.shape),
        [(cut - start) * cap, (stop - cut) * cap],
    )
    for n, (first, last) in enumerate(groups[:-1]):
        sums = gram(n + 1, lists, counts, tiles, sums, left_t, arrived[first:last], 3)
    sums, = late(rank, sums, met[0], arrived[start:cut], devices, F32, False)
    sums = late(rank, sums, met[1], arrived[cut:stop], devices, F32, True)
    if len(sums) == 1:
        mine = lax.psum_scatter(sums[0] * scale, "rows", scatter_dimension=0, tiled=True)
        return mine.reshape(mine.shape[0], 2, vectors).transpose(1, 0, 2)
    send, keep = sums
    outer = devices // 8
    got = swap(send, 1, devices)
    parts = split(rank, keep, [got], 4, 1, BF16)
    got = [swap(parts[n], n << 1, devices) for n in (3, 1, 2)]
    parts = split(rank, parts[0], got, outer, 3, F32)
    far_first = sorted(range(1, outer), key=lambda n: (n < outer // 2, n))
    got = [swap(parts[n], n << 3, devices) for n in far_first]
    return finish(rank, parts[0], got, scale)


def solution(mesh):
    placed = (
        P("rows", None),
        P("rows", None),
        P(),
        P(None, "rows", None),
        P(None, "rows", None),
        P("rows", None),
    )

    return jax.shard_map(body, mesh=mesh, in_specs=placed, out_specs=P(None, "rows", None), check_vma=False)
```

```python
import functools
import math

import jax
import jax.numpy as jnp
from jax import lax
from jax.experimental import pallas as pl
from jax.experimental.pallas import tpu as pltpu
from jax.sharding import PartitionSpec as P


F32 = jnp.float32
BF16 = jnp.bfloat16
SHIFT = 1024
ROOM = 8 * 2**20
LATE = 13
MOST = 40
EARLY = 3
SMEM = pltpu.SMEM
VMEM = pltpu.VMEM
HBM = pltpu.HBM


def exchange_order(devices):
    half = devices // 2
    far, near = list(range(half, devices)), list(range(1, half))
    order, far = far[:EARLY], far[EARLY:]
    while far or near:
        order += near[:1] + far[:1]
        near, far = near[1:], far[1:]
    return order


def exchange_groups(count):
    early = count - min(LATE, count // 2)
    parts = -(-early // MOST)
    cuts = [early * n // parts for n in range(parts + 1)]
    return list(zip(cuts, cuts[1:] + [count]))


def in_hbm(value):
    return pltpu.with_memory_space_constraint(value, HBM)


def in_vmem(value):
    return pltpu.with_memory_space_constraint(value, VMEM)


def whole(shape, space=VMEM):
    return pl.BlockSpec(shape, lambda *_: (0,) * len(shape), memory_space=space)


def first_kernel(masks, rank_ref, send_ref, blocks_ref, *rest):
    outs, sems = rest[: len(masks)], rest[len(masks)]
    cap = send_ref.shape[0]
    copies = []
    for n, mask in enumerate(masks):
        for c in range(cap):
            block = jnp.maximum(send_ref[c, rank_ref[0] ^ mask], 0)
            copy = pltpu.make_async_copy(blocks_ref.at[block], outs[n].at[c], sems.at[n * cap + c])
            copy.start()
            copies.append(copy)
    for copy in copies:
        copy.wait()


def first_pack(rank, send, blocks, masks):
    cap = send.shape[0]
    return pl.pallas_call(
        functools.partial(first_kernel, masks),
        out_shape=[VMEM((cap,) + blocks.shape[1:], BF16)] * len(masks),
        in_specs=[pl.BlockSpec(memory_space=SMEM)] * 2 + [pl.BlockSpec(memory_space=HBM)],
        out_specs=[pl.BlockSpec(memory_space=VMEM)] * len(masks),
        scratch_shapes=[pltpu.SemaphoreType.DMA((len(masks) * cap,))],
        compiler_params=pltpu.CompilerParams(vmem_limit_bytes=ROOM),
        name="first_pack",
    )(rank, in_hbm(send), in_hbm(blocks))


def pack_kernel(masks, after, rank_ref, send_ref, blocks_ref, *rest):
    rest = rest[after:]
    outs, (held_ref, in_sems, out_sems) = rest[: len(masks)], rest[len(masks):]
    cap = send_ref.shape[0]
    rank = rank_ref[0]
    inward, outward = [], []
    for n, mask in enumerate(masks):
        for c in range(cap):
            i = n * cap + c
            block = jnp.maximum(send_ref[c, rank ^ mask], 0)
            copy = pltpu.make_async_copy(blocks_ref.at[block], held_ref.at[i], in_sems.at[i])
            copy.start()
            inward.append(copy)
            outward.append(pltpu.make_async_copy(held_ref.at[i], outs[n].at[c], out_sems.at[i]))
    for one, two in zip(inward, outward):
        one.wait()
        two.start()
    for copy in outward:
        copy.wait()


def pack(rank, send, blocks, masks, after=()):
    cap = send.shape[0]
    count = len(masks) * cap
    return pl.pallas_call(
        functools.partial(pack_kernel, masks, len(after)),
        out_shape=[jax.ShapeDtypeStruct((cap,) + blocks.shape[1:], BF16)] * len(masks),
        in_specs=[whole((1,), SMEM), whole(send.shape, SMEM)]
        + [pl.BlockSpec(memory_space=HBM)] * (1 + len(after)),
        out_specs=[pl.BlockSpec(memory_space=HBM)] * len(masks),
        scratch_shapes=[
            VMEM((count,) + blocks.shape[1:], BF16),
            pltpu.SemaphoreType.DMA((count,)),
            pltpu.SemaphoreType.DMA((count,)),
        ],
        compiler_params=pltpu.CompilerParams(vmem_limit_bytes=ROOM + 2 * count * blocks[0].size),
        name="pack",
    )(rank, send, in_hbm(blocks), *after)


def slot_lists(rank, send, source, tile, local, order, starts, spare):
    cap = send.shape[0]
    slots = source.shape[1]
    mine = lax.dynamic_index_in_dim(send, rank[0], 1, keepdims=False)
    away = source >= local
    r = jnp.maximum(source - local, 0)
    c = r % cap
    mask = (r // cap) ^ rank[0]
    spot = jnp.where(
        mask[..., None] == jnp.array(order, jnp.int32), jnp.arange(len(order), dtype=jnp.int32), 0
    ).sum(-1)
    own = source
    for n in range(cap):
        own = jnp.where(away & (c == n), jnp.maximum(mine[n], 0), own)
    phase = jnp.zeros_like(source)
    first = jnp.zeros_like(source)
    far = away & (mask != 0)
    for n, start in enumerate(starts):
        phase = jnp.where(far & (spot >= start), n + 1, phase)
        first = jnp.where(far & (spot >= start), start, first)
    value = tile * SHIFT + jnp.where(far, (spot - first) * cap + c, own)
    phases = jnp.arange(len(starts) + 1, dtype=jnp.int32)[:, None, None]
    hit = (tile >= 0)[None] & (phase[None] == phases)
    k = jnp.arange(slots, dtype=jnp.int32)
    before = (hit[:, :, None, :] & (k[None, :] < k[:, None])).astype(jnp.int32).sum(-1)
    there = hit[:, :, None, :] & (before[:, :, None, :] == k[:, None])
    empty = spare * SHIFT
    lists = jnp.where(there, value[None, :, None, :] - empty, 0).sum(-1) + empty
    return lists.reshape(len(starts) + 1, -1), hit.astype(jnp.int32).sum(-1)


def pair(entry, j, tiles_ref, pool_ref):
    e0, e1 = entry(2 * j), entry(2 * j + 1)
    return jnp.dot(
        jnp.concatenate([tiles_ref[e0 // SHIFT], tiles_ref[e1 // SHIFT]], axis=1),
        jnp.concatenate([pool_ref[e0 % SHIFT], pool_ref[e1 % SHIFT]], axis=0),
        preferred_element_type=F32,
    )


def add_rest(acc_ref, done, count, entry, tiles_ref, pool_ref):
    def one(j, carry):
        acc_ref[...] += pair(entry, j, tiles_ref, pool_ref)
        return carry

    lax.fori_loop(done, (count + 1) // 2, one, 0)


def pool_loads(arrivals, pool_ref, sems):
    cap = arrivals[0].shape[0]
    return [
        pltpu.make_async_copy(ref, pool_ref.at[pl.ds(n * cap, cap)], sems.at[n])
        for n, ref in enumerate(arrivals)
    ]


def in_chunks(from_ref, to_ref, sems):
    size = from_ref.shape[0] // sems.shape[0]
    return lambda i: pltpu.make_async_copy(
        from_ref.at[pl.ds(i * size, size)], to_ref.at[pl.ds(i * size, size)], sems.at[i]
    )


def hops_kernel(slots, fixed, lists_ref, counts_ref, tiles_ref, pool_ref, out_ref, held_ref, out_sems):
    chunks = out_sems.shape[0]
    bunch = held_ref.shape[0] // chunks
    outward = in_chunks(held_ref, out_ref, out_sems)

    def some(step, carry):
        tiles = tiles_ref.at[2 * step // chunks]
        for g in range(bunch):
            block = step * bunch + g
            entry = lambda j, block=block: lists_ref[0, block * slots + j]
            for j in range(fixed):
                value = pair(entry, j, tiles, pool_ref)
                if j:
                    held_ref[block] += value
                else:
                    held_ref[block] = value
        for g in range(bunch):
            block = step * bunch + g
            entry = lambda j, block=block: lists_ref[0, block * slots + j]
            add_rest(held_ref.at[block], fixed, counts_ref[0, block], entry, tiles, pool_ref)
        outward(step).start()
        return carry

    lax.fori_loop(0, chunks, some, 0)
    for i in range(chunks):
        outward(i).wait()


def hops(lists, counts, tiles, pool, fixed, bunch=4):
    steps = counts.shape[1]
    slots = lists.shape[1] // steps
    chunks = steps // math.gcd(bunch, steps // 2)
    rows, vectors = pool.shape[1:]
    block = pl.BlockSpec(memory_space=VMEM)
    return pl.pallas_call(
        functools.partial(hops_kernel, slots, fixed),
        out_shape=HBM((steps, rows, vectors), F32),
        in_specs=[pl.BlockSpec(memory_space=SMEM)] * 2 + [block] * 2,
        out_specs=pl.BlockSpec(memory_space=HBM),
        scratch_shapes=[VMEM((steps, rows, vectors), F32), pltpu.SemaphoreType.DMA((chunks,))],
        compiler_params=pltpu.CompilerParams(
            vmem_limit_bytes=ROOM + 4 * steps * rows * vectors + 2 * pool.size
        ),
        cost_estimate=pl.CostEstimate(flops=8 * 10**9, bytes_accessed=40 * 2**20, transcendentals=0),
        name="hops",
    )(lists, counts, tiles, pool)


def adjoint_kernel(phase, slots, count, own, lists_ref, counts_ref, tiles_ref, left_ref, *rest):
    outs, sum_ref = rest[:-1], rest[-1]
    local, rows = left_ref.shape[:2]
    for s in range(2 * count):
        sum_ref[s] = jnp.zeros_like(sum_ref[s])

    def one_block(block, carry):
        d = block // local
        tiles = tiles_ref.at[d]

        def two(j, carry):
            e0 = lists_ref[phase, block * slots + 2 * j]
            e1 = lists_ref[phase, block * slots + 2 * j + 1]
            value = lax.dot_general(
                jnp.concatenate([tiles[e0 // SHIFT], tiles[e1 // SHIFT]], axis=1),
                left_ref[block % local], (((0,), (0,)), ((), ())), preferred_element_type=F32,
            )
            sum_ref[d * count + e0 % SHIFT] += value[:rows]
            sum_ref[d * count + e1 % SHIFT] += value[rows:]
            return carry

        return lax.fori_loop(0, (counts_ref[phase, block] + 1) // 2, two, carry)

    lax.fori_loop(0, 2 * local, one_block, 0)
    first = 0
    for out_ref in outs:
        size = out_ref.shape[2] // rows
        for d in range(2):
            for s in range(size):
                value = sum_ref[d * count + first + s]
                turned = value.astype(BF16).T
                if not own:
                    out_ref[d, :, s * rows:(s + 1) * rows] = turned
                    continue
                half = turned.shape[0] // 2
                for n in range(half // own):
                    for core in range(2):
                        row, place = (2 * n + core) * own, core * half + n * own
                        out_ref[d, place:place + own, s * rows:(s + 1) * rows] = turned[row:row + own]
        first += size


def adjoint(phase, lists, counts, tiles, left, sizes, own):
    count = sum(sizes)
    slots = lists.shape[1] // counts.shape[1]
    rows, vectors = left.shape[1:]
    block = pl.BlockSpec(memory_space=VMEM)
    size = 2 * count * rows * vectors
    return pl.pallas_call(
        functools.partial(adjoint_kernel, phase, slots, count, own),
        out_shape=[jax.ShapeDtypeStruct((2, vectors, n * rows), BF16) for n in sizes],
        in_specs=[pl.BlockSpec(memory_space=SMEM)] * 2 + [block] * 2,
        out_specs=[block] * len(sizes),
        scratch_shapes=[VMEM((2 * count, rows, vectors), F32)],
        compiler_params=pltpu.CompilerParams(vmem_limit_bytes=ROOM + 6 * size + 2 * left.size),
        cost_estimate=pl.CostEstimate(flops=8 * 10**9, bytes_accessed=16 * 2**20, transcendentals=0),
        name="adjoint",
    )(lists, counts, tiles, left)


def gram_kernel(
    phase, count, slots, fixed, more, final, lists_ref, counts_ref, tiles_ref, in_ref, left_ref, *rest
):
    whole_sum = not more and phase + 1 == final
    arrivals, (sum_ref, pool_ref, held_ref, high_ref, low_ref, in_sems, sems) = rest[:count], rest[count:]
    steps, rows, vectors = held_ref.shape
    per = steps // 2
    chunks = in_sems.shape[0] // 2
    bunch = per // chunks
    inward = None if more else in_chunks(in_ref, held_ref, in_sems)
    loads = pool_loads(arrivals, pool_ref, sems)
    for copy in loads:
        copy.start()
    ahead = min(2, chunks)
    if more:
        sum_ref[...] = in_ref[...]
    else:
        for i in range(ahead):
            for d in range(2):
                inward(d * chunks + i).start()
        sum_ref[...] = jnp.zeros_like(sum_ref)
    for copy in loads:
        copy.wait()

    def some(step, carry):
        spots = [(d, g, d * per + step * bunch + g) for d in range(2) for g in range(bunch)]

        if not more:
            @pl.when(step + ahead < chunks)
            def _():
                for d in range(2):
                    inward(d * chunks + step + ahead).start()

            for d in range(2):
                inward(d * chunks + step).wait()
        for d, g, block in spots:
            entry = lambda j, block=block: lists_ref[phase, block * slots + j]
            if more:
                held_ref[block] = jnp.zeros_like(held_ref[block])
            for j in range(fixed):
                held_ref[block] += pair(entry, j, tiles_ref.at[d], pool_ref)
        for d, g, block in spots:
            entry = lambda j, block=block: lists_ref[phase, block * slots + j]
            add_rest(
                held_ref.at[block], fixed, counts_ref[phase, block], entry, tiles_ref.at[d], pool_ref
            )
        for d, g, block in spots:
            value = held_ref[block]
            high = value.astype(BF16)
            spot = (pl.ds(g * rows, rows), pl.ds(d * vectors, vectors))
            high_ref[spot] = high
            low = (value - high.astype(F32)).astype(BF16)
            open_block = counts_ref[final, block] > 0 if whole_sum else True
            low_ref[spot] = jnp.where(open_block, low, jnp.zeros_like(low))
        sum_ref[...] += jnp.dot(left_ref[step], high_ref[...], preferred_element_type=F32)
        sum_ref[...] += jnp.dot(left_ref[step], low_ref[...], preferred_element_type=F32)
        return carry

    lax.fori_loop(0, chunks, some, 0)


def gram(phase, lists, counts, tiles, current, left_t, arrivals, fixed):
    steps = counts.shape[1]
    more = current.ndim == 2
    rows, vectors = arrivals[0].shape[1:]
    slots = lists.shape[1] // steps
    chunks, columns, depth = left_t.shape
    cap = arrivals[0].shape[0]
    block = pl.BlockSpec(memory_space=VMEM)
    dma = pltpu.SemaphoreType.DMA
    room = 2 * ROOM + 4 * steps * rows * vectors + sum(2 * a.size for a in arrivals)
    return pl.pallas_call(
        functools.partial(gram_kernel, phase, len(arrivals), slots, fixed, more, counts.shape[0] - 1),
        out_shape=jax.ShapeDtypeStruct((columns, 2 * vectors), F32),
        in_specs=[pl.BlockSpec(memory_space=SMEM)] * 2
        + [block, block if more else pl.BlockSpec(memory_space=HBM), block]
        + [pl.BlockSpec(memory_space=HBM)] * len(arrivals),
        out_specs=block,
        scratch_shapes=[
            VMEM((len(arrivals) * cap, rows, vectors), BF16),
            VMEM((steps, rows, vectors), F32),
            VMEM((depth, 2 * vectors), BF16),
            VMEM((depth, 2 * vectors), BF16),
            dma((2 * chunks,)),
            dma((len(arrivals),)),
        ],
        compiler_params=pltpu.CompilerParams(vmem_limit_bytes=room),
        cost_estimate=pl.CostEstimate(flops=12 * 10**9, bytes_accessed=24 * 2**20, transcendentals=0),
        name="gram",
    )(lists, counts, tiles, current if more else in_hbm(current), in_vmem(left_t), *map(in_hbm, arrivals))


def late_kernel(other, rank_ref, in_ref, adjoint_ref, *rest):
    arrivals, out_ref = rest[:-1], rest[-1]
    vectors = arrivals[0].shape[2]
    pool = jnp.concatenate([ref[...].reshape(-1, vectors) for ref in arrivals], axis=0)
    if other is None:
        rows = slice(None)
    else:
        half = in_ref.shape[0] // 2
        rows = pl.ds(pl.multiple_of(((rank_ref[0] + other) % 2) * half, half), half)
    for d in range(2):
        side = slice(d * vectors, (d + 1) * vectors)
        value = in_ref[rows, side] + jnp.dot(adjoint_ref[d, rows], pool, preferred_element_type=F32)
        out_ref[..., side] = value.reshape(out_ref.shape[:-1] + (vectors,))


def late(rank, sums, adjoint, arrivals, shape, other=None):
    block = pl.BlockSpec(memory_space=VMEM)
    return pl.pallas_call(
        functools.partial(late_kernel, other),
        out_shape=VMEM(shape, F32),
        in_specs=[pl.BlockSpec(memory_space=SMEM)] + [block] * (2 + len(arrivals)),
        out_specs=block,
        compiler_params=pltpu.CompilerParams(vmem_limit_bytes=2 * ROOM),
        cost_estimate=pl.CostEstimate(flops=2 * 10**9, bytes_accessed=12 * 2**20, transcendentals=0),
        name="late",
    )(rank, *map(in_vmem, (sums, adjoint, *arrivals)))


def split_kernel(width, shift, count, final, scale, rank_ref, keep_ref, *rest):
    arrived, outs = rest[:count], rest[count:]
    mine = (rank_ref[0] >> shift) % width
    if final:
        vectors = outs[0].shape[-1]
        total = keep_ref[...]
        for ref in arrived:
            total = total + ref[...].astype(F32)
        total = total * scale
        for d in range(2):
            outs[0][d] = total[:, d * vectors:(d + 1) * vectors]
        return
    for mask in range(width):
        where = mine ^ mask
        if len(keep_ref.shape) == 4:
            part = keep_ref[:, where]
            for ref in arrived:
                part = part + ref[:, where].astype(F32)
        else:
            part = keep_ref[where]
            for ref in arrived:
                part = part + ref[where].astype(F32)
        outs[mask][...] = part.astype(outs[mask].dtype)


def split(rank, keep, arrived, width, shift, sent):
    part = keep.shape[:-3] + keep.shape[-2:]
    return pl.pallas_call(
        functools.partial(split_kernel, width, shift, len(arrived), False, None),
        out_shape=[VMEM(part, sent if n else F32) for n in range(width)],
        in_specs=[pl.BlockSpec(memory_space=SMEM)] + [pl.BlockSpec(memory_space=VMEM)] * (1 + len(arrived)),
        out_specs=[pl.BlockSpec(memory_space=VMEM)] * width,
        compiler_params=pltpu.CompilerParams(vmem_limit_bytes=ROOM),
    )(rank, *map(in_vmem, (keep, *arrived)))


def finish(rank, keep, arrived, scale):
    own, both = keep.shape
    return pl.pallas_call(
        functools.partial(split_kernel, 1, 0, len(arrived), True, scale),
        out_shape=jax.ShapeDtypeStruct((2, own, both // 2), F32),
        in_specs=[pl.BlockSpec(memory_space=SMEM)] + [pl.BlockSpec(memory_space=VMEM)] * (1 + len(arrived)),
        out_specs=pl.BlockSpec(memory_space=VMEM),
        compiler_params=pltpu.CompilerParams(vmem_limit_bytes=ROOM),
        name="finish",
    )(rank, *map(in_vmem, (keep, *arrived)))


def swap(value, mask, devices):
    return lax.ppermute(value, "rows", [(i, i ^ mask) for i in range(devices)])


def body(left, right, tiles, source_blocks, tile_index, send_blocks):
    block_rows = tiles.shape[-1]
    vectors = right.shape[1]
    local = right.shape[0] // block_rows
    devices = lax.axis_size("rows")
    slots = source_blocks.shape[-1]
    scale = 1.0 / math.sqrt(local * block_rows * devices)
    rank = lax.axis_index("rows").astype(jnp.int32).reshape(1)
    blocks = right.reshape(local, block_rows, vectors)
    order = exchange_order(devices)
    groups = exchange_groups(len(order))
    send = send_blocks.T

    early = min(EARLY, len(order))
    packed = first_pack(rank, send, blocks, order[:early])
    packed += pack(rank, send, blocks, order[early:])
    arrived = []
    for n, mask in enumerate(order):
        arrived.append(swap(packed[n], mask, devices))

    lists, counts = slot_lists(
        rank, send, source_blocks.reshape(2 * local, slots), tile_index.reshape(2 * local, slots),
        local, order, [start for start, _ in groups], tiles.shape[1],
    )
    tiles = jnp.concatenate([tiles, jnp.zeros((2, 1) + tiles.shape[2:], tiles.dtype)], axis=1)
    bunch = math.gcd(local, 8) * block_rows
    left_t = left.reshape(-1, bunch, vectors).transpose(0, 2, 1)
    own = 0 if vectors % (8 * devices) else vectors // devices
    if own:
        left_t = left_t.reshape(-1, devices // 2, 2, own, bunch).swapaxes(1, 2).reshape(left_t.shape)
    tiles = in_vmem(tiles)
    sums = hops(lists, counts, tiles, blocks, 4)
    start, stop = groups[-1]
    cut = stop - (stop - start) * 2 // 5
    cap = send.shape[0]
    met = adjoint(
        len(groups), lists, counts, tiles, left.reshape(blocks.shape),
        [(cut - start) * cap, (stop - cut) * cap], own,
    )
    for n, (first, last) in enumerate(groups[:-1]):
        sums = gram(n + 1, lists, counts, tiles, sums, left_t, arrived[first:last], 3)
    sums = late(rank, sums, met[0], arrived[start:cut], sums.shape)
    if not own:
        sums = late(rank, sums, met[1], arrived[cut:stop], sums.shape)
        mine = lax.psum_scatter(sums * scale, "rows", scatter_dimension=0, tiled=True)
        return mine.reshape(mine.shape[0], 2, vectors).transpose(1, 0, 2)
    outer = devices // 8
    half = (outer, 4, own, 2 * vectors)
    send = late(rank, sums, met[1], arrived[cut:stop], half, 1)
    got = swap(send, 1, devices)
    keep = late(rank, sums, met[1], arrived[cut:stop], half, 0)
    parts = split(rank, keep, [got], 4, 1, BF16)
    got = [swap(parts[n], n << 1, devices) for n in (3, 1, 2)]
    parts = split(rank, parts[0], got, outer, 3, F32)
    far_first = sorted(range(1, outer), key=lambda n: (n < outer // 2, n))
    got = [swap(parts[n], n << 3, devices) for n in far_first]
    return finish(rank, parts[0], got, scale)


def solution(mesh):
    placed = (
        P("rows", None),
        P("rows", None),
        P(),
        P(None, "rows", None),
        P(None, "rows", None),
        P("rows", None),
    )

    return jax.shard_map(body, mesh=mesh, in_specs=placed, out_specs=P(None, "rows", None), check_vma=False)
```

```python
import functools
import math

import jax
import jax.numpy as jnp
from jax import lax
from jax.experimental import pallas as pl
from jax.experimental.pallas import tpu as pltpu
from jax.sharding import PartitionSpec as P


F32 = jnp.float32
BF16 = jnp.bfloat16
SHIFT = 1024
ROOM = 8 * 2**20
LATE = 13
MOST = 40
EARLY = 3
SMEM = pltpu.SMEM
VMEM = pltpu.VMEM
HBM = pltpu.HBM


def exchange_order(devices):
    half = devices // 2
    far, near = list(range(half, devices)), list(range(1, half))
    order, far = far[:EARLY], far[EARLY:]
    while far or near:
        order += near[:1] + far[:1]
        near, far = near[1:], far[1:]
    return order


def exchange_groups(count):
    early = count - min(LATE, count // 2)
    parts = -(-early // MOST)
    cuts = [early * n // parts for n in range(parts + 1)]
    return list(zip(cuts, cuts[1:] + [count]))


def in_hbm(value):
    return pltpu.with_memory_space_constraint(value, HBM)


def in_vmem(value):
    return pltpu.with_memory_space_constraint(value, VMEM)


def whole(shape, space=VMEM):
    return pl.BlockSpec(shape, lambda *_: (0,) * len(shape), memory_space=space)


def first_kernel(masks, rank_ref, send_ref, blocks_ref, *rest):
    outs, sems = rest[: len(masks)], rest[len(masks)]
    cap = send_ref.shape[0]
    copies = []
    for n, mask in enumerate(masks):
        for c in range(cap):
            block = jnp.maximum(send_ref[c, rank_ref[0] ^ mask], 0)
            copy = pltpu.make_async_copy(blocks_ref.at[block], outs[n].at[c], sems.at[n * cap + c])
            copy.start()
            copies.append(copy)
    for copy in copies:
        copy.wait()


def first_pack(rank, send, blocks, masks):
    cap = send.shape[0]
    return pl.pallas_call(
        functools.partial(first_kernel, masks),
        out_shape=[VMEM((cap,) + blocks.shape[1:], BF16)] * len(masks),
        in_specs=[pl.BlockSpec(memory_space=SMEM)] * 2 + [pl.BlockSpec(memory_space=HBM)],
        out_specs=[pl.BlockSpec(memory_space=VMEM)] * len(masks),
        scratch_shapes=[pltpu.SemaphoreType.DMA((len(masks) * cap,))],
        compiler_params=pltpu.CompilerParams(vmem_limit_bytes=ROOM),
        name="first_pack",
    )(rank, in_hbm(send), in_hbm(blocks))


def pack_kernel(masks, after, rank_ref, send_ref, blocks_ref, *rest):
    rest = rest[after:]
    outs, (held_ref, in_sems, out_sems) = rest[: len(masks)], rest[len(masks):]
    cap = send_ref.shape[0]
    rank = rank_ref[0]
    inward, outward = [], []
    for n, mask in enumerate(masks):
        for c in range(cap):
            i = n * cap + c
            block = jnp.maximum(send_ref[c, rank ^ mask], 0)
            copy = pltpu.make_async_copy(blocks_ref.at[block], held_ref.at[i], in_sems.at[i])
            copy.start()
            inward.append(copy)
            outward.append(pltpu.make_async_copy(held_ref.at[i], outs[n].at[c], out_sems.at[i]))
    for one, two in zip(inward, outward):
        one.wait()
        two.start()
    for copy in outward:
        copy.wait()


def pack(rank, send, blocks, masks, after=()):
    cap = send.shape[0]
    count = len(masks) * cap
    return pl.pallas_call(
        functools.partial(pack_kernel, masks, len(after)),
        out_shape=[jax.ShapeDtypeStruct((cap,) + blocks.shape[1:], BF16)] * len(masks),
        in_specs=[whole((1,), SMEM), whole(send.shape, SMEM)]
        + [pl.BlockSpec(memory_space=HBM)] * (1 + len(after)),
        out_specs=[pl.BlockSpec(memory_space=HBM)] * len(masks),
        scratch_shapes=[
            VMEM((count,) + blocks.shape[1:], BF16),
            pltpu.SemaphoreType.DMA((count,)),
            pltpu.SemaphoreType.DMA((count,)),
        ],
        compiler_params=pltpu.CompilerParams(vmem_limit_bytes=ROOM + 2 * count * blocks[0].size),
        name="pack",
    )(rank, send, in_hbm(blocks), *after)


def slot_lists(rank, send, source, tile, local, order, starts, spare):
    cap = send.shape[0]
    slots = source.shape[1]
    mine = lax.dynamic_index_in_dim(send, rank[0], 1, keepdims=False)
    away = source >= local
    r = jnp.maximum(source - local, 0)
    c = r % cap
    mask = (r // cap) ^ rank[0]
    spot = jnp.where(
        mask[..., None] == jnp.array(order, jnp.int32), jnp.arange(len(order), dtype=jnp.int32), 0
    ).sum(-1)
    own = source
    for n in range(cap):
        own = jnp.where(away & (c == n), jnp.maximum(mine[n], 0), own)
    phase = jnp.zeros_like(source)
    first = jnp.zeros_like(source)
    far = away & (mask != 0)
    for n, start in enumerate(starts):
        phase = jnp.where(far & (spot >= start), n + 1, phase)
        first = jnp.where(far & (spot >= start), start, first)
    value = tile * SHIFT + jnp.where(far, (spot - first) * cap + c, own)
    phases = jnp.arange(len(starts) + 1, dtype=jnp.int32)[:, None, None]
    hit = (tile >= 0)[None] & (phase[None] == phases)
    k = jnp.arange(slots, dtype=jnp.int32)
    before = (hit[:, :, None, :] & (k[None, :] < k[:, None])).astype(jnp.int32).sum(-1)
    there = hit[:, :, None, :] & (before[:, :, None, :] == k[:, None])
    empty = spare * SHIFT
    lists = jnp.where(there, value[None, :, None, :] - empty, 0).sum(-1) + empty
    return lists.reshape(len(starts) + 1, -1), hit.astype(jnp.int32).sum(-1)


def pair(entry, j, tiles_ref, pool_ref):
    e0, e1 = entry(2 * j), entry(2 * j + 1)
    return jnp.dot(
        jnp.concatenate([tiles_ref[e0 // SHIFT], tiles_ref[e1 // SHIFT]], axis=1),
        jnp.concatenate([pool_ref[e0 % SHIFT], pool_ref[e1 % SHIFT]], axis=0),
        preferred_element_type=F32,
    )


def add_rest(acc_ref, done, count, entry, tiles_ref, pool_ref):
    def one(j, carry):
        acc_ref[...] += pair(entry, j, tiles_ref, pool_ref)
        return carry

    lax.fori_loop(done, (count + 1) // 2, one, 0)


def pool_loads(arrivals, pool_ref, sems):
    cap = arrivals[0].shape[0]
    return [
        pltpu.make_async_copy(ref, pool_ref.at[pl.ds(n * cap, cap)], sems.at[n])
        for n, ref in enumerate(arrivals)
    ]


def in_chunks(from_ref, to_ref, sems):
    size = from_ref.shape[0] // sems.shape[0]
    return lambda i: pltpu.make_async_copy(
        from_ref.at[pl.ds(i * size, size)], to_ref.at[pl.ds(i * size, size)], sems.at[i]
    )


def hops_kernel(slots, fixed, lists_ref, counts_ref, tiles_ref, pool_ref, out_ref, held_ref, out_sems):
    chunks = out_sems.shape[0]
    bunch = held_ref.shape[0] // chunks
    outward = in_chunks(held_ref, out_ref, out_sems)

    def some(step, carry):
        tiles = tiles_ref.at[2 * step // chunks]
        for g in range(bunch):
            block = step * bunch + g
            entry = lambda j, block=block: lists_ref[0, block * slots + j]
            for j in range(fixed):
                value = pair(entry, j, tiles, pool_ref)
                if j:
                    held_ref[block] += value
                else:
                    held_ref[block] = value
        for g in range(bunch):
            block = step * bunch + g
            entry = lambda j, block=block: lists_ref[0, block * slots + j]
            add_rest(held_ref.at[block], fixed, counts_ref[0, block], entry, tiles, pool_ref)
        outward(step).start()
        return carry

    lax.fori_loop(0, chunks, some, 0)
    for i in range(chunks):
        outward(i).wait()


def hops(lists, counts, tiles, pool, fixed, bunch=4):
    steps = counts.shape[1]
    slots = lists.shape[1] // steps
    chunks = steps // math.gcd(bunch, steps // 2)
    rows, vectors = pool.shape[1:]
    block = pl.BlockSpec(memory_space=VMEM)
    return pl.pallas_call(
        functools.partial(hops_kernel, slots, fixed),
        out_shape=HBM((steps, rows, vectors), F32),
        in_specs=[pl.BlockSpec(memory_space=SMEM)] * 2 + [block] * 2,
        out_specs=pl.BlockSpec(memory_space=HBM),
        scratch_shapes=[VMEM((steps, rows, vectors), F32), pltpu.SemaphoreType.DMA((chunks,))],
        compiler_params=pltpu.CompilerParams(
            vmem_limit_bytes=ROOM + 4 * steps * rows * vectors + 2 * pool.size
        ),
        cost_estimate=pl.CostEstimate(flops=8 * 10**9, bytes_accessed=40 * 2**20, transcendentals=0),
        name="hops",
    )(lists, counts, tiles, pool)


def adjoint_kernel(phase, slots, count, own, lists_ref, counts_ref, tiles_ref, left_ref, *rest):
    outs, sum_ref = rest[:-1], rest[-1]
    local, rows = left_ref.shape[:2]
    for s in range(2 * count):
        sum_ref[s] = jnp.zeros_like(sum_ref[s])

    def one_block(block, carry):
        d = block // local
        tiles = tiles_ref.at[d]

        def two(j, carry):
            e0 = lists_ref[phase, block * slots + 2 * j]
            e1 = lists_ref[phase, block * slots + 2 * j + 1]
            value = lax.dot_general(
                jnp.concatenate([tiles[e0 // SHIFT], tiles[e1 // SHIFT]], axis=1),
                left_ref[block % local], (((0,), (0,)), ((), ())), preferred_element_type=F32,
            )
            sum_ref[d * count + e0 % SHIFT] += value[:rows]
            sum_ref[d * count + e1 % SHIFT] += value[rows:]
            return carry

        return lax.fori_loop(0, (counts_ref[phase, block] + 1) // 2, two, carry)

    lax.fori_loop(0, 2 * local, one_block, 0)
    first = 0
    for out_ref in outs:
        size = out_ref.shape[2] // rows
        for d in range(2):
            for s in range(size):
                value = sum_ref[d * count + first + s]
                turned = value.astype(BF16).T
                if not own:
                    out_ref[d, :, s * rows:(s + 1) * rows] = turned
                    continue
                half = turned.shape[0] // 2
                for n in range(half // own):
                    for core in range(2):
                        row, place = (2 * n + core) * own, core * half + n * own
                        out_ref[d, place:place + own, s * rows:(s + 1) * rows] = turned[row:row + own]
        first += size


def adjoint(phase, lists, counts, tiles, left, sizes, own):
    count = sum(sizes)
    slots = lists.shape[1] // counts.shape[1]
    rows, vectors = left.shape[1:]
    block = pl.BlockSpec(memory_space=VMEM)
    size = 2 * count * rows * vectors
    return pl.pallas_call(
        functools.partial(adjoint_kernel, phase, slots, count, own),
        out_shape=[jax.ShapeDtypeStruct((2, vectors, n * rows), BF16) for n in sizes],
        in_specs=[pl.BlockSpec(memory_space=SMEM)] * 2 + [block] * 2,
        out_specs=[block] * len(sizes),
        scratch_shapes=[VMEM((2 * count, rows, vectors), F32)],
        compiler_params=pltpu.CompilerParams(vmem_limit_bytes=ROOM + 6 * size + 2 * left.size),
        cost_estimate=pl.CostEstimate(flops=8 * 10**9, bytes_accessed=16 * 2**20, transcendentals=0),
        name="adjoint",
    )(lists, counts, tiles, left)


def gram_kernel(
    phase, count, slots, fixed, more, final, lists_ref, counts_ref, tiles_ref, in_ref, left_ref, *rest
):
    whole_sum = not more and phase + 1 == final
    arrivals, (sum_ref, pool_ref, held_ref, high_ref, low_ref, in_sems, sems) = rest[:count], rest[count:]
    steps, rows, vectors = held_ref.shape
    per = steps // 2
    chunks = in_sems.shape[0] // 2
    bunch = per // chunks
    inward = None if more else in_chunks(in_ref, held_ref, in_sems)
    loads = pool_loads(arrivals, pool_ref, sems)
    for copy in loads:
        copy.start()
    ahead = min(2, chunks)
    if more:
        sum_ref[...] = in_ref[...]
    else:
        for i in range(ahead):
            for d in range(2):
                inward(d * chunks + i).start()
        sum_ref[...] = jnp.zeros_like(sum_ref)
    for copy in loads:
        copy.wait()

    def some(step, carry):
        spots = [(d, g, d * per + step * bunch + g) for d in range(2) for g in range(bunch)]

        if not more:
            @pl.when(step + ahead < chunks)
            def _():
                for d in range(2):
                    inward(d * chunks + step + ahead).start()

            for d in range(2):
                inward(d * chunks + step).wait()
        for d, g, block in spots:
            entry = lambda j, block=block: lists_ref[phase, block * slots + j]
            if more:
                held_ref[block] = jnp.zeros_like(held_ref[block])
            for j in range(fixed):
                held_ref[block] += pair(entry, j, tiles_ref.at[d], pool_ref)
        for d, g, block in spots:
            entry = lambda j, block=block: lists_ref[phase, block * slots + j]
            add_rest(
                held_ref.at[block], fixed, counts_ref[phase, block], entry, tiles_ref.at[d], pool_ref
            )
        for d, g, block in spots:
            value = held_ref[block]
            high = value.astype(BF16)
            spot = (pl.ds(g * rows, rows), pl.ds(d * vectors, vectors))
            high_ref[spot] = high
            low = (value - high.astype(F32)).astype(BF16)
            open_block = counts_ref[final, block] > 0 if whole_sum else True
            low_ref[spot] = jnp.where(open_block, low, jnp.zeros_like(low))
        sum_ref[...] += jnp.dot(left_ref[step], high_ref[...], preferred_element_type=F32)
        sum_ref[...] += jnp.dot(left_ref[step], low_ref[...], preferred_element_type=F32)
        return carry

    lax.fori_loop(0, chunks, some, 0)


def gram(phase, lists, counts, tiles, current, left_t, arrivals, fixed):
    steps = counts.shape[1]
    more = current.ndim == 2
    rows, vectors = arrivals[0].shape[1:]
    slots = lists.shape[1] // steps
    chunks, columns, depth = left_t.shape
    cap = arrivals[0].shape[0]
    block = pl.BlockSpec(memory_space=VMEM)
    dma = pltpu.SemaphoreType.DMA
    room = 2 * ROOM + 4 * steps * rows * vectors + sum(2 * a.size for a in arrivals)
    return pl.pallas_call(
        functools.partial(gram_kernel, phase, len(arrivals), slots, fixed, more, counts.shape[0] - 1),
        out_shape=jax.ShapeDtypeStruct((columns, 2 * vectors), F32),
        in_specs=[pl.BlockSpec(memory_space=SMEM)] * 2
        + [block, block if more else pl.BlockSpec(memory_space=HBM), block]
        + [pl.BlockSpec(memory_space=HBM)] * len(arrivals),
        out_specs=block,
        scratch_shapes=[
            VMEM((len(arrivals) * cap, rows, vectors), BF16),
            VMEM((steps, rows, vectors), F32),
            VMEM((depth, 2 * vectors), BF16),
            VMEM((depth, 2 * vectors), BF16),
            dma((2 * chunks,)),
            dma((len(arrivals),)),
        ],
        compiler_params=pltpu.CompilerParams(vmem_limit_bytes=room),
        cost_estimate=pl.CostEstimate(flops=12 * 10**9, bytes_accessed=24 * 2**20, transcendentals=0),
        name="gram",
    )(lists, counts, tiles, current if more else in_hbm(current), in_vmem(left_t), *map(in_hbm, arrivals))


def late_kernel(other, rank_ref, in_ref, adjoint_ref, *rest):
    arrivals, out_ref = rest[:-1], rest[-1]
    vectors = arrivals[0].shape[2]
    pool = jnp.concatenate([ref[...].reshape(-1, vectors) for ref in arrivals], axis=0)
    if other is None:
        rows = slice(None)
    else:
        half = in_ref.shape[0] // 2
        rows = pl.ds(pl.multiple_of(((rank_ref[0] + other) % 2) * half, half), half)
    for d in range(2):
        side = slice(d * vectors, (d + 1) * vectors)
        value = in_ref[rows, side] + jnp.dot(adjoint_ref[d, rows], pool, preferred_element_type=F32)
        out_ref[..., side] = value.reshape(out_ref.shape[:-1] + (vectors,))


def late(rank, sums, adjoint, arrivals, shape, other=None):
    block = pl.BlockSpec(memory_space=VMEM)
    return pl.pallas_call(
        functools.partial(late_kernel, other),
        out_shape=VMEM(shape, F32),
        in_specs=[pl.BlockSpec(memory_space=SMEM)] + [block] * (2 + len(arrivals)),
        out_specs=block,
        compiler_params=pltpu.CompilerParams(vmem_limit_bytes=2 * ROOM),
        cost_estimate=pl.CostEstimate(flops=2 * 10**9, bytes_accessed=12 * 2**20, transcendentals=0),
        name="late",
    )(rank, *map(in_vmem, (sums, adjoint, *arrivals)))


def split_kernel(width, shift, count, final, scale, rank_ref, keep_ref, *rest):
    arrived, outs = rest[:count], rest[count:]
    mine = (rank_ref[0] >> shift) % width
    if final:
        vectors = outs[0].shape[-1]
        total = keep_ref[...]
        for ref in arrived:
            total = total + ref[...].astype(F32)
        total = total * scale
        for d in range(2):
            outs[0][d] = total[:, d * vectors:(d + 1) * vectors]
        return
    for mask in range(width):
        where = mine ^ mask
        if len(keep_ref.shape) == 4:
            part = keep_ref[:, where]
            for ref in arrived:
                part = part + ref[:, where].astype(F32)
        else:
            part = keep_ref[where]
            for ref in arrived:
                part = part + ref[where].astype(F32)
        outs[mask][...] = part.astype(outs[mask].dtype)


def split(rank, keep, arrived, width, shift, sent):
    part = keep.shape[:-3] + keep.shape[-2:]
    return pl.pallas_call(
        functools.partial(split_kernel, width, shift, len(arrived), False, None),
        out_shape=[VMEM(part, sent if n else F32) for n in range(width)],
        in_specs=[pl.BlockSpec(memory_space=SMEM)] + [pl.BlockSpec(memory_space=VMEM)] * (1 + len(arrived)),
        out_specs=[pl.BlockSpec(memory_space=VMEM)] * width,
        compiler_params=pltpu.CompilerParams(vmem_limit_bytes=ROOM),
    )(rank, *map(in_vmem, (keep, *arrived)))


def finish(rank, keep, arrived, scale):
    own, both = keep.shape
    return pl.pallas_call(
        functools.partial(split_kernel, 1, 0, len(arrived), True, scale),
        out_shape=jax.ShapeDtypeStruct((2, own, both // 2), F32),
        in_specs=[pl.BlockSpec(memory_space=SMEM)] + [pl.BlockSpec(memory_space=VMEM)] * (1 + len(arrived)),
        out_specs=pl.BlockSpec(memory_space=VMEM),
        compiler_params=pltpu.CompilerParams(vmem_limit_bytes=ROOM),
        name="finish",
    )(rank, *map(in_vmem, (keep, *arrived)))


def swap(value, mask, devices):
    return lax.ppermute(value, "rows", [(i, i ^ mask) for i in range(devices)])


def body(left, right, tiles, source_blocks, tile_index, send_blocks):
    block_rows = tiles.shape[-1]
    vectors = right.shape[1]
    local = right.shape[0] // block_rows
    devices = lax.axis_size("rows")
    slots = source_blocks.shape[-1]
    scale = 1.0 / math.sqrt(local * block_rows * devices)
    rank = lax.axis_index("rows").astype(jnp.int32).reshape(1)
    blocks = right.reshape(local, block_rows, vectors)
    order = exchange_order(devices)
    groups = exchange_groups(len(order))
    send = send_blocks.T

    early = min(EARLY, len(order))
    packed = first_pack(rank, send, blocks, order[:early])
    packed += pack(rank, send, blocks, order[early:])
    arrived = []
    for n, mask in enumerate(order):
        arrived.append(swap(packed[n], mask, devices))

    lists, counts = slot_lists(
        rank, send, source_blocks.reshape(2 * local, slots), tile_index.reshape(2 * local, slots),
        local, order, [start for start, _ in groups], tiles.shape[1],
    )
    tiles = jnp.concatenate([tiles, jnp.zeros((2, 1) + tiles.shape[2:], tiles.dtype)], axis=1)
    bunch = math.gcd(local, 8) * block_rows
    left_t = left.reshape(-1, bunch, vectors).transpose(0, 2, 1)
    own = 0 if vectors % (8 * devices) else vectors // devices
    if own:
        left_t = left_t.reshape(-1, devices // 2, 2, own, bunch).swapaxes(1, 2).reshape(left_t.shape)
    tiles = in_vmem(tiles)
    sums = hops(lists, counts, tiles, blocks, 4)
    start, stop = groups[-1]
    size = stop - start
    cuts = [start, stop - size * 2 // 5, stop - size // 4, stop]
    spans = [slice(a, b) for a, b in zip(cuts, cuts[1:]) if a < b]
    cap = send.shape[0]
    met = adjoint(
        len(groups), lists, counts, tiles, left.reshape(blocks.shape),
        [(span.stop - span.start) * cap for span in spans], own,
    )
    for n, (first, last) in enumerate(groups[:-1]):
        sums = gram(n + 1, lists, counts, tiles, sums, left_t, arrived[first:last], 3)
    for part, span in zip(met[:-1], spans):
        sums = late(rank, sums, part, arrived[span], sums.shape)
    if not own:
        sums = late(rank, sums, met[-1], arrived[spans[-1]], sums.shape)
        mine = lax.psum_scatter(sums * scale, "rows", scatter_dimension=0, tiled=True)
        return mine.reshape(mine.shape[0], 2, vectors).transpose(1, 0, 2)
    outer = devices // 8
    half = (outer, 4, own, 2 * vectors)
    send = late(rank, sums, met[-1], arrived[spans[-1]], half, 1)
    got = swap(send, 1, devices)
    keep = late(rank, sums, met[-1], arrived[spans[-1]], half, 0)
    parts = split(rank, keep, [got], 4, 1, BF16)
    got = [swap(parts[n], n << 1, devices) for n in (3, 1, 2)]
    parts = split(rank, parts[0], got, outer, 3, F32)
    far_first = sorted(range(1, outer), key=lambda n: (n < outer // 2, n))
    got = [swap(parts[n], n << 3, devices) for n in far_first]
    return finish(rank, parts[0], got, scale)


def solution(mesh):
    placed = (
        P("rows", None),
        P("rows", None),
        P(),
        P(None, "rows", None),
        P(None, "rows", None),
        P("rows", None),
    )

    return jax.shard_map(body, mesh=mesh, in_specs=placed, out_specs=P(None, "rows", None), check_vma=False)
```
